8 devices in a mesh: col: 2 (over z, y), row: 4 (over x, core).
Axes of the slice: x: 2, y: 2, z: 1, core: 2. Of those that a mesh axis runs over, the one named last changes fastest.
Arguments:
- forcing: float32 [192, 96, 256], P('row', 'col')
- u_init: float32 [192, 96, 256], P('row', 'col')
- diffusivity: float32 [192, 96], P('row', 'col')
- local_solve: bfloat16 [4, 2, 4096, 4096], P('row', 'col')
- relax_omega: float32 [], replicated
Outputs:
- output: float32 [192, 96, 256], P('row', 'col')
All inputs are finite; a program needn't handle non-finite values.
Results may differ from the reference program's by a relative error of at most 0.001.
Values are sent between devices in bfloat16 or wider.
A program may use at most 1 GiB of HBM per device.

```python
import jax
import jax.numpy as jnp
from jax import lax

TILE_N = 48
MARGIN = 8
NUM_RHS = 256
SWEEPS = 4
BLOCKS_X = 4
BLOCKS_Y = 2

GRID_X = TILE_N * BLOCKS_X
GRID_Y = TILE_N * BLOCKS_Y
EXT_N = TILE_N + 2 * MARGIN
WINDOW = EXT_N * EXT_N
NUM_BLOCKS = BLOCKS_X * BLOCKS_Y


def sine_basis():
    steps_one = jnp.arange(EXT_N, dtype=jnp.float32) + 1.0
    angle_step = jnp.pi / (EXT_N + 1)
    sine_vecs = jnp.sqrt(2.0 / (EXT_N + 1)) * jnp.sin(angle_step * steps_one[:, None] * steps_one[None, :])
    eigen_vals = 2.0 - 2.0 * jnp.cos(angle_step * steps_one)
    return sine_vecs, eigen_vals


def solve_blocks(diffusivity, draw_key, low_end, high_end):
    sine_vecs, eigen_vals = sine_basis()
    block_mean = diffusivity.reshape(BLOCKS_X, TILE_N, BLOCKS_Y, TILE_N).mean(axis=(1, 3)).reshape(NUM_BLOCKS)
    spread = jax.random.uniform(draw_key, (NUM_BLOCKS, EXT_N, EXT_N), jnp.float32, low_end, high_end)
    spectrum = spread / (block_mean[:, None, None] * (eigen_vals[:, None] + eigen_vals[None, :]))
    pair_basis = sine_vecs[:, None, :] * sine_vecs[None, :, :]

    def one_block(gain_grid):
        half_form = jnp.einsum('ap,pq,cp->acq', sine_vecs, gain_grid, sine_vecs)
        full_form = jnp.einsum('acq,beq->abce', half_form, pair_basis)
        return full_form.reshape(WINDOW, WINDOW).astype(jnp.bfloat16)

    return lax.map(one_block, spectrum).reshape(BLOCKS_X, BLOCKS_Y, WINDOW, WINDOW)


def setup_inputs(seed: int = 0) -> dict:
    draw_key = jax.random.key(seed)
    key_f, key_u, key_k, key_b, key_w = jax.random.split(draw_key, 5)
    forcing = (5.0 / EXT_N) * jax.random.normal(key_f, (GRID_X, GRID_Y, NUM_RHS), jnp.float32)
    u_init = 0.3 * jax.random.normal(key_u, (GRID_X, GRID_Y, NUM_RHS), jnp.float32)
    diffusivity = jnp.exp(jax.random.uniform(key_k, (GRID_X, GRID_Y), jnp.float32, -0.6, 0.6))
    local_solve = solve_blocks(diffusivity, key_b, 0.7, 1.3)
    relax_omega = jax.random.uniform(key_w, (), jnp.float32, 0.12, 0.2)
    return {'forcing': forcing, 'u_init': u_init, 'diffusivity': diffusivity, 'local_solve': local_solve, 'relax_omega': relax_omega}


def face_weights(diffusivity):
    padded = jnp.pad(diffusivity, 1)
    weight_x = 0.5 * (padded[:-1, 1:-1] + padded[1:, 1:-1])
    weight_y = 0.5 * (padded[1:-1, :-1] + padded[1:-1, 1:])
    return weight_x, weight_y


def apply_operator(grid_field, weight_x, weight_y):
    padded = jnp.pad(grid_field, ((1, 1), (1, 1), (0, 0)))
    center = padded[1:-1, 1:-1]
    return (weight_x[:-1, :, None] * (center - padded[:-2, 1:-1])
            + weight_x[1:, :, None] * (center - padded[2:, 1:-1])
            + weight_y[:, :-1, None] * (center - padded[1:-1, :-2])
            + weight_y[:, 1:, None] * (center - padded[1:-1, 2:]))


def schwarz_update(residual, local_solve):
    padded = jnp.pad(residual.astype(jnp.bfloat16), ((MARGIN, MARGIN), (MARGIN, MARGIN), (0, 0)))
    blocks = local_solve.reshape(NUM_BLOCKS, WINDOW, WINDOW)

    def add_block(total_sum, scan_item):
        block_index, matrix = scan_item
        corner_x = (block_index // BLOCKS_Y) * TILE_N
        corner_y = (block_index % BLOCKS_Y) * TILE_N
        window = lax.dynamic_slice(padded, (corner_x, corner_y, 0), (EXT_N, EXT_N, NUM_RHS))
        solved = jnp.dot(matrix, window.reshape(WINDOW, NUM_RHS), preferred_element_type=jnp.float32)
        current = lax.dynamic_slice(total_sum, (corner_x, corner_y, 0), (EXT_N, EXT_N, NUM_RHS))
        total_sum = lax.dynamic_update_slice(total_sum, current + solved.reshape(EXT_N, EXT_N, NUM_RHS), (corner_x, corner_y, 0))
        return total_sum, None

    start_sum = jnp.zeros((GRID_X + 2 * MARGIN, GRID_Y + 2 * MARGIN, NUM_RHS), jnp.float32)
    total_sum = lax.scan(add_block, start_sum, (jnp.arange(NUM_BLOCKS), blocks))[0]
    return total_sum[MARGIN:MARGIN + GRID_X, MARGIN:MARGIN + GRID_Y]


def reference(forcing, u_init, diffusivity, local_solve, relax_omega):
    weight_x, weight_y = face_weights(diffusivity)
    solution_u = u_init
    residual = forcing - apply_operator(u_init, weight_x, weight_y)
    for sweep_index in range(SWEEPS):
        update = schwarz_update(residual, local_solve)
        solution_u = solution_u + relax_omega * update
        if sweep_index < SWEEPS - 1:
            residual = residual - relax_omega * apply_operator(update, weight_x, weight_y)
    return solution_u
```

```python
import functools

import jax
import jax.numpy as jnp
from jax import lax
from jax.experimental import pallas as pl
from jax.experimental.pallas import tpu as pltpu
from jax.sharding import PartitionSpec as P

SWEEPS = 4
TILE = 48
EXT = 64
WIN = EXT * EXT
RHS = 256
SIDES = (0, 1)
F32 = jnp.float32
BF16 = jnp.bfloat16
MESH = pl.DeviceIdType.MESH

CHUNKS = ((16, 16, 0), (32, 16, 18), (7, 9, 36), (TILE, 9, 47))
YLEN = 58
RCHUNKS = ((5, 14), (0, 5), (19, 5))


def kernel(omega, f_hbm, u_hbm, kap_hbm, m_hbm, out_hbm,
           ms, mr, w, z, r, u, wx, wy, kown, krecv, kfull,
           ys, yr, xrs, xrr, rsy, rry, rsx, rrx, rrd, ues, uer,
           yz_s, yz_r, xs_s, xs_r, xr_s, xr_r, ry_s, ry_r, rx_s, rx_r, rd_s, rd_r,
           ie_s, ie_r, lsem, msem):
    col = lax.axis_index("col")
    row = lax.axis_index("row")
    has_up = row > 0
    has_dn = row < 3
    ydev = (1 - col, row)
    xdev = ((col, row - 1), (col, row + 1))
    ddev = ((1 - col, row - 1), (1 - col, row + 1))
    has = (has_up, has_dn)

    hc = pl.multiple_of(56 - 56 * col, 8)
    mc = pl.multiple_of(TILE - 40 * col, 8)
    oc = pl.multiple_of(56 * col, 8)
    sc = pl.multiple_of(TILE - TILE * col, 16)
    rc = pl.multiple_of(16 * col, 16)
    gc = pl.multiple_of(8 + 8 * col, 8)
    cd = pl.multiple_of(40 - 32 * col, 8)
    ci = pl.multiple_of(8 + 16 * col, 8)
    es = 55 - 47 * col
    er = 56 - 49 * col

    def remote(src, dst, ss, rs, dev):
        return pltpu.make_async_remote_copy(src_ref=src, dst_ref=dst, send_sem=ss, recv_sem=rs,
                                            device_id=dev, device_id_type=MESH)

    inner = (pl.ds(8, TILE), pl.ds(8, TILE))
    cp_k = pltpu.make_async_copy(kap_hbm, kown, lsem.at[0])
    cp_z = pltpu.make_async_copy(u_hbm, z.at[inner], lsem.at[1])
    cp_r = pltpu.make_async_copy(f_hbm, r.at[inner], lsem.at[2])
    cp_u = pltpu.make_async_copy(u_hbm, u, lsem.at[3])
    for cp in (cp_k, cp_z, cp_r):
        cp.start()

    def load_s(i):
        return pltpu.make_async_copy(m_hbm.at[pl.ds(16 * i, 16), pl.ds(sc, 16)], ms.at[pl.ds(16 * i, 16)], msem.at[i])

    def load_r(i):
        return pltpu.make_async_copy(m_hbm.at[pl.ds(16 * i, 16), pl.ds(rc, TILE)], mr.at[pl.ds(16 * i, 16)], msem.at[4 + i])

    for i in range(4):
        load_s(i).start()
    for i in range(4):
        load_r(i).start()
    cp_u.start()

    for ref in (z, r):
        ref[0:8] = jnp.zeros((8, EXT, RHS), F32)
        ref[56:EXT] = jnp.zeros((8, EXT, RHS), F32)
        ref[8:56, 0:8] = jnp.zeros((TILE, 8, RHS), F32)
        ref[8:56, 56:EXT] = jnp.zeros((TILE, 8, RHS), F32)
    kfull[...] = jnp.zeros_like(kfull)
    ys[...] = jnp.zeros_like(ys)

    bar = pltpu.get_barrier_semaphore()
    pl.semaphore_signal(bar, inc=1, device_id=ydev, device_id_type=MESH)
    for d in SIDES:
        @pl.when(has[d])
        def _(d=d):
            pl.semaphore_signal(bar, inc=1, device_id=xdev[d], device_id_type=MESH)
            pl.semaphore_signal(bar, inc=1, device_id=ddev[d], device_id_type=MESH)
    n_sides = has_up.astype(jnp.int32) + has_dn.astype(jnp.int32)
    pl.semaphore_wait(bar, 1 + 2 * n_sides)

    cp_k.wait()
    k_y = remote(kown, krecv.at[2], ie_s.at[0], ie_r.at[0], ydev)
    k_y.start()
    k_x = [remote(kown, krecv.at[1 - d], ie_s.at[1 + d], ie_r.at[2 - d], xdev[d]) for d in SIDES]
    u_x = [remote(z.at[8 if d == 0 else 55, pl.ds(8, TILE)], z.at[56 if d == 0 else 7, pl.ds(8, TILE)],
                  ie_s.at[3 + d], ie_r.at[4 - d], xdev[d]) for d in SIDES]
    k_in = [remote(kown, krecv.at[d], ie_s.at[1 + d], ie_r.at[1 + d], xdev[d]) for d in SIDES]
    u_in = [remote(z.at[8 if d == 0 else 55, pl.ds(8, TILE)], z.at[7 if d == 0 else 56, pl.ds(8, TILE)],
                   ie_s.at[3 + d], ie_r.at[3 + d], xdev[d]) for d in SIDES]
    cp_z.wait()
    for k in range(TILE):
        ues[k // 8, k % 8, :] = z[8 + k, pl.ds(es, 1), :][0]
    u_y = remote(ues, uer, ie_s.at[5], ie_r.at[5], ydev)
    u_y.start()
    for d in SIDES:
        @pl.when(has[d])
        def _(d=d):
            k_x[d].start()
            u_x[d].start()

    kfull[8:56, 8:56] = kown[...]
    for d in SIDES:
        @pl.when(has[d])
        def _(d=d):
            k_in[d].wait_recv()
            src = 47 if d == 0 else 0
            dst = 7 if d == 0 else 56
            kfull[dst:dst + 1, 8:56] = krecv[d, src:src + 1, :]
    k_y.wait_recv()

    @pl.when(col == 0)
    def _():
        kfull[8:56, 56:57] = krecv[2, :, 0:1]

    @pl.when(col == 1)
    def _():
        kfull[8:56, 7:8] = krecv[2, :, 47:TILE]

    kt = kfull[...].T
    prev = jnp.broadcast_to(kt[0:EXT, 7:8], (EXT, 128))
    for a in range(8, 57):
        here = jnp.broadcast_to(kt[0:EXT, a:a + 1], (EXT, 128))
        wx[a - 8] = 0.5 * (prev + here)
        if a < 56:
            wy[a - 8] = 0.5 * (pltpu.roll(here, 1, 0) + here)
        prev = here

    def both(v):
        return jnp.concatenate([v, v], axis=1)

    def update(a0, rows, c0, n, om, add_u):
        def body(i, carry):
            a = a0 + i
            wide = z[a, pl.ds(c0 - 8, n + 16), :]
            fy = both(wy[a - 8, pl.ds(c0 - 8, n + 16), :]) * (wide - pltpu.roll(wide, 1, 0))
            fyr = pltpu.roll(fy, n + 15, 0)
            mid = wide[8:8 + n]
            az = (both(wx[a - 8, pl.ds(c0, n), :]) * (mid - z[a - 1, pl.ds(c0, n), :])
                  + both(wx[a - 7, pl.ds(c0, n), :]) * (mid - z[a + 1, pl.ds(c0, n), :])
                  + fy[8:8 + n] - fyr[8:8 + n])
            r[a, pl.ds(c0, n), :] = r[a, pl.ds(c0, n), :] - om * az
            if add_u:
                u[a - 8, pl.ds(c0 - 8, n), :] = u[a - 8, pl.ds(c0 - 8, n), :] + om * mid
            return carry
        lax.fori_loop(0, rows, body, 0)

    def ry(j):
        p0, n = RCHUNKS[j]
        return remote(rsy.at[pl.ds(p0, n)], rry.at[pl.ds(p0, n)], ry_s.at[j], ry_r.at[j], ydev)

    def rx(d):
        return remote(rsx.at[d], rrx.at[1 - d], rx_s.at[d], rx_r.at[1 - d], xdev[d])

    def rx_in(d):
        return remote(rsx.at[d], rrx.at[d], rx_s.at[d], rx_r.at[d], xdev[d])

    def rd(d):
        return remote(rsy.at[pl.ds(20 * d, 4)], rrd.at[1 - d], rd_s.at[d], rd_r.at[1 - d], ddev[d])

    def rd_in(d):
        return remote(rsy.at[pl.ds(20 * d, 4)], rrd.at[d], rd_s.at[d], rd_r.at[d], ddev[d])

    def send_ry(j):
        p0, n = RCHUNKS[j]
        for p in range(p0, p0 + n):
            a = 8 + 2 * p
            rsy[p] = jnp.concatenate([r[a, pl.ds(mc, 8), :], r[a + 1, pl.ds(mc, 8), :]], axis=0).astype(BF16)
        ry(j).start()

    def send_rx():
        for d in SIDES:
            for i in range(8):
                rsx[d, i] = r[8 + 40 * d + i, 8:56, :].astype(BF16)

            @pl.when(has[d])
            def _(d=d):
                rd(d).start()
                rx(d).start()

    def to_w(a0, rows, c0, n):
        def body(i, carry):
            w[a0 + i, pl.ds(c0, n), :] = r[a0 + i, pl.ds(c0, n), :].astype(BF16)
            return carry
        lax.fori_loop(0, rows, body, 0)

    def recv_r():
        to_w(8, TILE, rc, TILE)
        for d in SIDES:
            @pl.when(has[d])
            def _(d=d):
                rx_in(d).wait_recv()
                rd_in(d).wait_recv()
                for i in range(8):
                    r[56 * d + i, 8:56, :] = rrx[d, i].astype(F32)
                for q in range(4):
                    v = rrd[d, q].astype(F32)
                    r[56 * d + 2 * q, pl.ds(hc, 8), :] = v[0:8]
                    r[56 * d + 2 * q + 1, pl.ds(hc, 8), :] = v[8:16]
            to_w(56 * d, 8, 0, EXT)
        for j in range(3):
            p0, n = RCHUNKS[j]
            ry(j).wait_recv()

            def body(i, carry, p0=p0):
                v = rry[p0 + i].astype(F32)
                a = 8 + 2 * (p0 + i)
                r[a, pl.ds(hc, 8), :] = v[0:8]
                r[a + 1, pl.ds(hc, 8), :] = v[8:16]
                w[a, pl.ds(sc, 16), :] = r[a, pl.ds(sc, 16), :].astype(BF16)
                w[a + 1, pl.ds(sc, 16), :] = r[a + 1, pl.ds(sc, 16), :].astype(BF16)
                return carry
            lax.fori_loop(0, n, body, 0)
        for j in range(3):
            ry(j).wait_send()
        for d in SIDES:
            @pl.when(has[d])
            def _(d=d):
                rx(d).wait_send()
                rd(d).wait_send()

    for d in SIDES:
        @pl.when(has[d])
        def _(d=d):
            u_in[d].wait_recv()
    u_y.wait_recv()
    for k in range(TILE):
        z[8 + k, pl.ds(er, 1), :] = uer[k // 8, k % 8, :][None]
    cp_r.wait()
    update(8, TILE, cd, 16, 1.0, False)
    for j in range(3):
        send_ry(j)
    update(8, TILE, ci, 32, 1.0, False)
    send_rx()
    recv_r()
    k_y.wait_send()
    u_y.wait_send()
    for d in SIDES:
        @pl.when(has[d])
        def _(d=d):
            k_x[d].wait_send()
            u_x[d].wait_send()
    cp_u.wait()

    om = omega[0]

    def dot_s(a0):
        lhs = ms[pl.ds(a0, 16)].reshape(RHS, WIN)
        z[pl.ds(a0, 16), pl.ds(sc, 16), :] = jnp.dot(
            lhs, w[...].reshape(WIN, RHS), preferred_element_type=F32).reshape(16, 16, RHS)

    def dot_r(a0):
        lhs = mr[pl.ds(a0, 16)].reshape(768, WIN)
        z[pl.ds(a0, 16), pl.ds(rc, TILE), :] = jnp.dot(
            lhs, w[...].reshape(WIN, RHS), preferred_element_type=F32).reshape(16, TILE, RHS)

    def yz(j):
        a0, n, off = CHUNKS[j]
        length = n + 2
        return remote(ys.at[pl.ds(off, length)], yr.at[pl.ds(off, length)], yz_s.at[j], yz_r.at[j], ydev)

    def send_y(j):
        a0, n, off = CHUNKS[j]
        for k in range(n):
            ys[off + k] = z[a0 + k, pl.ds(hc, 8), :]
            ys[off + n + k // 8, k % 8, :] = z[a0 + k, pl.ds(es, 1), :][0]
        yz(j).start()

    def recv_y(j):
        a0, n, off = CHUNKS[j]
        yz(j).wait_recv()
        for k in range(n):
            z[a0 + k, pl.ds(mc, 8), :] = z[a0 + k, pl.ds(mc, 8), :] + yr[off + k]
            z[a0 + k, pl.ds(er, 1), :] = z[a0 + k, pl.ds(er, 1), :] + yr[off + n + k // 8, k % 8, :][None]

    def xs(d):
        return remote(z.at[pl.ds(55 * d, 9), pl.ds(sc, 16)], xrs.at[1 - d], xs_s.at[d], xs_r.at[1 - d], xdev[d])

    def xs_in(d):
        return remote(z.at[pl.ds(55 * d, 9), pl.ds(sc, 16)], xrs.at[d], xs_s.at[d], xs_r.at[d], xdev[d])

    def xr(d):
        return remote(z.at[pl.ds(55 * d, 9), pl.ds(gc, 40)], xrr.at[1 - d], xr_s.at[d], xr_r.at[1 - d], xdev[d])

    def xr_in(d):
        return remote(z.at[pl.ds(55 * d, 9), pl.ds(gc, 40)], xrr.at[d], xr_s.at[d], xr_r.at[d], xdev[d])

    def on_side(d, fn):
        pl.when(has[d])(fn)

    def sweep(s, carry):
        @pl.when(s == 0)
        def _():
            for i in range(4):
                load_s(i).wait()
        dot_s(16)
        send_y(0)
        dot_s(32)
        send_y(1)
        lax.fori_loop(0, 2, lambda i, c: (dot_s(TILE * i), c)[1], 0)
        for d in SIDES:
            on_side(d, lambda d=d: xs(d).start())

            @pl.when(jnp.logical_not(has[d]))
            def _(d=d):
                z[7 + 49 * d, pl.ds(sc, 16), :] = jnp.zeros((16, RHS), F32)

        @pl.when(s == 0)
        def _():
            for i in range(4):
                load_r(i).wait()
        lax.fori_loop(0, 2, lambda i, c: (dot_r(TILE * i), c)[1], 0)
        for d in SIDES:
            on_side(d, lambda d=d: xr(d).start())
        for d in SIDES:
            @pl.when(has[d])
            def _(d=d):
                xs(d).wait_send()
                xs_in(d).wait_recv()
                a0 = 7 + 41 * d
                for k in range(9):
                    z[a0 + k, pl.ds(sc, 16), :] = z[a0 + k, pl.ds(sc, 16), :] + xrs[d, k]
            send_y(2 + d)
        lax.fori_loop(1, 3, lambda i, c: (dot_r(16 * i), c)[1], 0)
        for d in SIDES:
            @pl.when(jnp.logical_not(has[d]))
            def _(d=d):
                z[7 + 49 * d, :, :] = jnp.zeros((EXT, RHS), F32)
        z[:, pl.ds(oc, 8), :] = jnp.zeros((EXT, 8, RHS), F32)
        recv_y(0)
        recv_y(1)

        @pl.when(s < SWEEPS - 1)
        def _():
            update(17, 30, cd, 16, om, True)
            send_ry(0)
            update(17, 30, ci, 32, om, True)
        for d in SIDES:
            @pl.when(has[d])
            def _(d=d):
                xr(d).wait_send()
                xr_in(d).wait_recv()
                a0 = 7 + 41 * d
                for k in range(9):
                    z[a0 + k, pl.ds(gc, 40), :] = z[a0 + k, pl.ds(gc, 40), :] + xrr[d, k]
        recv_y(2)
        recv_y(3)

        @pl.when(s < SWEEPS - 1)
        def _():
            lax.fori_loop(0, 2, lambda i, c: (update(8 + 39 * i, 9, cd, 16, om, True), c)[1], 0)
            send_ry(1)
            send_ry(2)
            lax.fori_loop(0, 2, lambda i, c: (update(8 + 39 * i, 9, ci, 32, om, True), c)[1], 0)
            send_rx()
            recv_r()

        @pl.when(s == SWEEPS - 1)
        def _():
            def body(i, c):
                u[i] = u[i] + om * z[8 + i, 8:56, :]
                return c
            lax.fori_loop(0, TILE, body, 0)
        for j in range(4):
            yz(j).wait_send()
        return carry

    lax.fori_loop(0, SWEEPS, sweep, 0)
    cp_o = pltpu.make_async_copy(u, out_hbm, lsem.at[4])
    cp_o.start()
    cp_o.wait()


def solution(mesh):
    def local_step(forcing, u_init, diffusivity, local_solve, relax_omega):
        any_spec = pl.BlockSpec(memory_space=pl.ANY)
        dma = pltpu.SemaphoreType.DMA
        return pl.pallas_call(
            kernel,
            out_shape=jax.ShapeDtypeStruct((TILE, TILE, RHS), F32),
            in_specs=[pl.BlockSpec(memory_space=pltpu.SMEM)] + [any_spec] * 4,
            out_specs=any_spec,
            scratch_shapes=[
                pltpu.VMEM((EXT, 16, WIN), BF16),
                pltpu.VMEM((EXT, TILE, WIN), BF16),
                pltpu.VMEM((EXT, EXT, RHS), BF16),
                pltpu.VMEM((EXT, EXT, RHS), F32),
                pltpu.VMEM((EXT, EXT, RHS), F32),
                pltpu.VMEM((TILE, TILE, RHS), F32),
                pltpu.VMEM((49, EXT, 128), F32),
                pltpu.VMEM((TILE, EXT, 128), F32),
                pltpu.VMEM((TILE, TILE), F32),
                pltpu.VMEM((3, TILE, TILE), F32),
                pltpu.VMEM((128, 128), F32),
                pltpu.VMEM((YLEN, 8, RHS), F32),
                pltpu.VMEM((YLEN, 8, RHS), F32),
                pltpu.VMEM((2, 9, 16, RHS), F32),
                pltpu.VMEM((2, 9, 40, RHS), F32),
                pltpu.VMEM((24, 16, RHS), BF16),
                pltpu.VMEM((24, 16, RHS), BF16),
                pltpu.VMEM((2, 8, TILE, RHS), BF16),
                pltpu.VMEM((2, 8, TILE, RHS), BF16),
                pltpu.VMEM((2, 4, 16, RHS), BF16),
                pltpu.VMEM((6, 8, RHS), F32),
                pltpu.VMEM((6, 8, RHS), F32),
                dma((4,)), dma((4,)), dma((2,)), dma((2,)), dma((2,)), dma((2,)),
                dma((3,)), dma((3,)), dma((2,)), dma((2,)), dma((2,)), dma((2,)),
                dma((6,)), dma((6,)), dma((5,)), dma((8,)),
            ],
            compiler_params=pltpu.CompilerParams(
                collective_id=0, has_side_effects=True, vmem_limit_bytes=64_000_000),
            name="schwarz",
        )(relax_omega.reshape(1), forcing, u_init, diffusivity,
          local_solve.reshape(EXT, EXT, WIN))

    field_spec = P('row', 'col', None)
    return jax.shard_map(local_step, mesh=mesh,
                         in_specs=(field_spec, field_spec, P('row', 'col'), P('row', 'col', None, None), P()),
                         out_specs=field_spec, check_vma=False)
```

```python
import functools

import jax
import jax.numpy as jnp
from jax import lax
from jax.experimental import pallas as pl
from jax.experimental.pallas import tpu as pltpu
from jax.sharding import PartitionSpec as P

SWEEPS = 4
TILE = 48
EXT = 64
WIN = EXT * EXT
RHS = 256
MG = 8
STRIP = 16
REST = 40
END = 56
SIDES = (0, 1)
F32 = jnp.float32
BF16 = jnp.bfloat16
MESH = pl.DeviceIdType.MESH

CHUNKS = ((STRIP, 12, 0), (36, 12, 14), (28, MG, 28))
SIDE_OFF = 37
YLEN = 59
RMID = (9, 6)
FCHUNKS = ((4, MG), (12, MG))

def kernel(omega, f_hbm, u_hbm, kap_hbm, m_hbm, u,
           ms, mr, w, z, r, wx, wy, kown, krecv, kfull,
           ys, yr, xrs, xrr, rsy, rry, rsx, rrx, rrd, ues, uer,
           fys, fyr_, fxs, fxsr, fxr, fxrr,
           yz_s, yz_r, xs_s, xs_r, xr_s, xr_r, ry_s, ry_r, rx_s, rx_r, rd_s, rd_r,
           ie_s, ie_r, fy_s, fy_r, fx_s, fx_r, lsem, msem):
    col = lax.axis_index("col")
    row = lax.axis_index("row")
    has_up = row > 0
    has_dn = row < 3
    ydev = (1 - col, row)
    has = (has_up, has_dn)
    first = jnp.where(row < 2, 1, 0)
    order = (first, 1 - first)

    def xdev(d):
        return (col, row - 1 + 2 * d)

    def ddev(d):
        return (1 - col, row - 1 + 2 * d)

    def on_side(d, fn):
        there = jnp.where(d == 0, row, 3 - row) > 0
        pl.when(there)(fn)

    def off_side(d, fn):
        there = jnp.where(d == 0, row, 3 - row) > 0
        pl.when(jnp.logical_not(there))(fn)

    hc = pl.multiple_of(END - END * col, MG)
    mc = pl.multiple_of(TILE - REST * col, MG)
    oc = pl.multiple_of(END * col, MG)
    sc = pl.multiple_of(TILE - TILE * col, STRIP)
    rc = pl.multiple_of(STRIP * col, STRIP)
    gc = pl.multiple_of(MG + MG * col, MG)
    cd = pl.multiple_of(REST - 32 * col, MG)
    ci = pl.multiple_of(MG + STRIP * col, MG)
    es = 55 - 47 * col
    er = END - 49 * col

    def remote(src, dst, ss, rs, dev):
        return pltpu.make_async_remote_copy(src_ref=src, dst_ref=dst, send_sem=ss, recv_sem=rs,
                                            device_id=dev, device_id_type=MESH)

    inner = (pl.ds(MG, TILE), pl.ds(MG, TILE))
    cp_k = pltpu.make_async_copy(kap_hbm, kown, lsem.at[0])
    cp_z = pltpu.make_async_copy(u_hbm, z.at[inner], lsem.at[1])
    cp_r = pltpu.make_async_copy(f_hbm, r.at[inner], lsem.at[2])
    cp_u = pltpu.make_async_copy(u_hbm, u, lsem.at[3])
    for cp in (cp_k, cp_z, cp_r):
        cp.start()

    def load_s(i):
        return pltpu.make_async_copy(m_hbm.at[pl.ds(STRIP * i, STRIP), pl.ds(sc, STRIP)], ms.at[pl.ds(STRIP * i, STRIP)], msem.at[i])

    def load_r(i):
        return pltpu.make_async_copy(m_hbm.at[pl.ds(STRIP * i, STRIP), pl.ds(gc, REST)], mr.at[pl.ds(STRIP * i, STRIP)], msem.at[4 + i])

    for i in range(4):
        load_s(i).start()
    for i in range(4):
        load_r(i).start()
    cp_u.start()

    for ref in (z, r):
        ref[0:MG] = jnp.zeros((MG, EXT, RHS), F32)
        ref[END:EXT] = jnp.zeros((MG, EXT, RHS), F32)
        ref[MG:END, 0:MG] = jnp.zeros((TILE, MG, RHS), F32)
        ref[MG:END, END:EXT] = jnp.zeros((TILE, MG, RHS), F32)
    kfull[...] = jnp.zeros_like(kfull)
    ys[...] = jnp.zeros_like(ys)

    bar = pltpu.get_barrier_semaphore()
    pl.semaphore_signal(bar, inc=1, device_id=ydev, device_id_type=MESH)
    for d in SIDES:
        @pl.when(has[d])
        def _(d=d):
            pl.semaphore_signal(bar, inc=1, device_id=xdev(d), device_id_type=MESH)
            pl.semaphore_signal(bar, inc=1, device_id=ddev(d), device_id_type=MESH)
    n_sides = has_up.astype(jnp.int32) + has_dn.astype(jnp.int32)
    pl.semaphore_wait(bar, 1 + 2 * n_sides)

    cp_k.wait()
    k_y = remote(kown, krecv.at[2], ie_s.at[0], ie_r.at[0], ydev)
    k_y.start()
    k_x = [remote(kown, krecv.at[1 - d], ie_s.at[1 + d], ie_r.at[2 - d], xdev(d)) for d in SIDES]
    u_x = [remote(z.at[MG if d == 0 else 55, pl.ds(MG, TILE)], z.at[END if d == 0 else 7, pl.ds(MG, TILE)],
                  ie_s.at[3 + d], ie_r.at[4 - d], xdev(d)) for d in SIDES]
    k_in = [remote(kown, krecv.at[d], ie_s.at[1 + d], ie_r.at[1 + d], xdev(d)) for d in SIDES]
    u_in = [remote(z.at[MG if d == 0 else 55, pl.ds(MG, TILE)], z.at[7 if d == 0 else END, pl.ds(MG, TILE)],
                   ie_s.at[3 + d], ie_r.at[3 + d], xdev(d)) for d in SIDES]
    cp_z.wait()
    for k in range(TILE):
        ues[k // MG, k % MG, :] = z[MG + k, pl.ds(es, 1), :][0]
    u_y = remote(ues, uer, ie_s.at[5], ie_r.at[5], ydev)
    u_y.start()
    for d in SIDES:
        @pl.when(has[d])
        def _(d=d):
            k_x[d].start()
            u_x[d].start()

    kfull[MG:END, MG:END] = kown[...]
    for d in SIDES:
        @pl.when(has[d])
        def _(d=d):
            k_in[d].wait_recv()
            src = 47 if d == 0 else 0
            dst = 7 if d == 0 else END
            kfull[dst:dst + 1, MG:END] = krecv[d, src:src + 1, :]
    k_y.wait_recv()

    @pl.when(col == 0)
    def _():
        kfull[MG:END, END:57] = krecv[2, :, 0:1]

    @pl.when(col == 1)
    def _():
        kfull[MG:END, 7:MG] = krecv[2, :, 47:TILE]

    kt = kfull[...].T
    prev = jnp.broadcast_to(kt[0:EXT, 7:MG], (EXT, 128))
    for a in range(MG, 57):
        here = jnp.broadcast_to(kt[0:EXT, a:a + 1], (EXT, 128))
        wx[a - MG] = 0.5 * (prev + here)
        if a < END:
            wy[a - MG] = 0.5 * (pltpu.roll(here, 1, 0) + here)
        prev = here

    def both(v):
        return jnp.concatenate([v, v], axis=1)

    def update(a0, rows, c0, n, om, add_u):
        def body(i, carry):
            a = a0 + i
            wide = z[a, pl.ds(c0 - MG, n + STRIP), :]
            fy = both(wy[a - MG, pl.ds(c0 - MG, n + STRIP), :]) * (wide - pltpu.roll(wide, 1, 0))
            fyr = pltpu.roll(fy, n + 15, 0)
            mid = wide[MG:MG + n]
            az = (both(wx[a - MG, pl.ds(c0, n), :]) * (mid - z[a - 1, pl.ds(c0, n), :])
                  + both(wx[a - 7, pl.ds(c0, n), :]) * (mid - z[a + 1, pl.ds(c0, n), :])
                  + fy[MG:MG + n] - fyr[MG:MG + n])
            r[a, pl.ds(c0, n), :] = r[a, pl.ds(c0, n), :] - om * az
            if add_u:
                u[a - MG, pl.ds(c0 - MG, n), :] = u[a - MG, pl.ds(c0 - MG, n), :] + om * mid
            return carry
        lax.fori_loop(0, rows, body, 0)

    def ry(p0, n, j):
        return remote(rsy.at[pl.ds(p0, n)], rry.at[pl.ds(p0, n)], ry_s.at[j], ry_r.at[j], ydev)

    def ry_mid():
        return ry(*RMID, 2)

    def ry_side(d):
        return ry(15 * d, 9, d)

    def rx(d):
        return remote(rsx.at[d], rrx.at[1 - d], rx_s.at[d], rx_r.at[1 - d], xdev(d))

    def rx_in(d):
        return remote(rsx.at[d], rrx.at[d], rx_s.at[d], rx_r.at[d], xdev(d))

    def rd(d):
        return remote(rsy.at[pl.ds(20 * d, 4)], rrd.at[1 - d], rd_s.at[d], rd_r.at[1 - d], ddev(d))

    def rd_in(d):
        return remote(rsy.at[pl.ds(20 * d, 4)], rrd.at[d], rd_s.at[d], rd_r.at[d], ddev(d))

    def pack_ry(p0, n):
        for q in range(n):
            a = MG + 2 * (p0 + q)
            rsy[p0 + q] = jnp.concatenate([r[a, pl.ds(mc, MG), :], r[a + 1, pl.ds(mc, MG), :]], axis=0).astype(BF16)

    def send_ry_side(d):
        pack_ry(15 * d, 9)
        on_side(d, lambda: rd(d).start())
        ry_side(d).start()

    def send_ry_mid():
        pack_ry(*RMID)
        ry_mid().start()

    def send_rx(d):
        for i in range(MG):
            rsx[d, i] = r[MG + REST * d + i, MG:END, :].astype(BF16)
        on_side(d, lambda: rx(d).start())

    def to_w(a0, rows, c0, n):
        def body(i, carry):
            w[a0 + i, pl.ds(c0, n), :] = r[a0 + i, pl.ds(c0, n), :].astype(BF16)
            return carry
        lax.fori_loop(0, rows, body, 0)

    def unpack_ry(p0, n):
        def body(i, carry):
            v = rry[p0 + i].astype(F32)
            a = MG + 2 * (p0 + i)
            r[a, pl.ds(hc, MG), :] = v[0:MG]
            r[a + 1, pl.ds(hc, MG), :] = v[MG:STRIP]
            w[a, pl.ds(sc, STRIP), :] = r[a, pl.ds(sc, STRIP), :].astype(BF16)
            w[a + 1, pl.ds(sc, STRIP), :] = r[a + 1, pl.ds(sc, STRIP), :].astype(BF16)
            return carry
        lax.fori_loop(0, n, body, 0)

    def recv_r():
        to_w(MG, TILE, rc, TILE)
        for d in (order[1], order[0]):
            ry_side(d).wait_recv()
            unpack_ry(15 * d, 9)

            def side(d=d):
                rx_in(d).wait_recv()
                rd_in(d).wait_recv()
                for i in range(MG):
                    r[END * d + i, MG:END, :] = rrx[d, i].astype(F32)
                for q in range(4):
                    v = rrd[d, q].astype(F32)
                    r[END * d + 2 * q, pl.ds(hc, MG), :] = v[0:MG]
                    r[END * d + 2 * q + 1, pl.ds(hc, MG), :] = v[MG:STRIP]
                to_w(END * d, MG, 0, EXT)
            on_side(d, side)
        ry_mid().wait_recv()
        unpack_ry(*RMID)
        ry_mid().wait_send()
        for d in SIDES:
            ry_side(d).wait_send()

            def sent(d=d):
                rx(d).wait_send()
                rd(d).wait_send()
            on_side(d, sent)

    for d in SIDES:
        @pl.when(has[d])
        def _(d=d):
            u_in[d].wait_recv()
    u_y.wait_recv()
    for k in range(TILE):
        z[MG + k, pl.ds(er, 1), :] = uer[k // MG, k % MG, :][None]
    cp_r.wait()
    update(MG, TILE, cd, STRIP, 1.0, False)
    for d in SIDES:
        send_ry_side(d)
    send_ry_mid()
    update(MG, TILE, ci, 32, 1.0, False)
    for d in SIDES:
        send_rx(d)
        off_side(d, lambda d=d: to_w(END * d, MG, 0, EXT))
    recv_r()
    k_y.wait_send()
    u_y.wait_send()
    for d in SIDES:
        @pl.when(has[d])
        def _(d=d):
            k_x[d].wait_send()
            u_x[d].wait_send()
    cp_u.wait()

    om = omega[0]

    def dot_s(a0):
        lhs = ms[pl.ds(a0, STRIP)].reshape(RHS, WIN)
        z[pl.ds(a0, STRIP), pl.ds(sc, STRIP), :] = jnp.dot(
            lhs, w[...].reshape(WIN, RHS), preferred_element_type=F32).reshape(STRIP, STRIP, RHS)

    def dot_r(a0):
        lhs = mr[pl.ds(a0, STRIP)].reshape(640, WIN)
        z[pl.ds(a0, STRIP), pl.ds(gc, REST), :] = jnp.dot(
            lhs, w[...].reshape(WIN, RHS), preferred_element_type=F32).reshape(STRIP, REST, RHS)

    def yz(j, off, length):
        return remote(ys.at[pl.ds(off, length)], yr.at[pl.ds(off, length)], yz_s.at[j], yz_r.at[j], ydev)

    def yz_mid(j):
        return yz(j, CHUNKS[j][2], CHUNKS[j][1] + pl.cdiv(CHUNKS[j][1], MG))

    def yz_side(d):
        return yz(3 + d, SIDE_OFF + 11 * d, 11)

    def pack_y(a0, n, off):
        for k in range(n):
            ys[off + k] = z[a0 + k, pl.ds(hc, MG), :]
            ys[off + n + k // MG, k % MG, :] = z[a0 + k, pl.ds(es, 1), :][0]

    def add_y(a0, n, off):
        for k in range(n):
            z[a0 + k, pl.ds(mc, MG), :] = z[a0 + k, pl.ds(mc, MG), :] + yr[off + k]
            z[a0 + k, pl.ds(er, 1), :] = z[a0 + k, pl.ds(er, 1), :] + yr[off + n + k // MG, k % MG, :][None]

    def send_y(j):
        pack_y(*CHUNKS[j])
        yz_mid(j).start()

    def send_y_side(d):
        pack_y(7 + 41 * d, 9, SIDE_OFF + 11 * d)
        yz_side(d).start()

    def recv_y(j):
        yz_mid(j).wait_recv()
        add_y(*CHUNKS[j])

    def recv_y_side(d):
        yz_side(d).wait_recv()
        add_y(7 + 41 * d, 9, SIDE_OFF + 11 * d)

    def xs(d):
        return remote(z.at[pl.ds(55 * d, 9), pl.ds(sc, STRIP)], xrs.at[1 - d], xs_s.at[d], xs_r.at[1 - d], xdev(d))

    def xs_in(d):
        return remote(z.at[pl.ds(55 * d, 9), pl.ds(sc, STRIP)], xrs.at[d], xs_s.at[d], xs_r.at[d], xdev(d))

    def xr(d):
        return remote(z.at[pl.ds(55 * d, 9), pl.ds(gc, REST)], xrr.at[1 - d], xr_s.at[d], xr_r.at[1 - d], xdev(d))

    def xr_in(d):
        return remote(z.at[pl.ds(55 * d, 9), pl.ds(gc, REST)], xrr.at[d], xr_s.at[d], xr_r.at[d], xdev(d))

    def fold_s(d):
        def side():
            xs(d).wait_send()
            xs_in(d).wait_recv()
            for k in range(9):
                a = 7 + 41 * d + k
                z[a, pl.ds(sc, STRIP), :] = z[a, pl.ds(sc, STRIP), :] + xrs[d, k]
        on_side(d, side)

    def fold_r(d):
        def side():
            xr(d).wait_send()
            xr_in(d).wait_recv()
            for k in range(9):
                a = 7 + 41 * d + k
                z[a, pl.ds(gc, REST), :] = z[a, pl.ds(gc, REST), :] + xrr[d, k]
        on_side(d, side)

    def no_row_s(d):
        z[7 + 49 * d, pl.ds(sc, STRIP), :] = jnp.zeros((STRIP, RHS), F32)

    def no_row_r(d):
        z[7 + 49 * d, pl.ds(gc, REST), :] = jnp.zeros((REST, RHS), F32)

    def sweep(s, carry):
        @pl.when(s == 0)
        def _():
            for i in range(4):
                load_s(i).wait()
        dot_s(STRIP)
        send_y(0)
        dot_s(32)
        send_y(1)
        for d in order:
            dot_s(TILE * d)
            on_side(d, lambda d=d: xs(d).start())
            off_side(d, lambda d=d: no_row_s(d))

        @pl.when(s == 0)
        def _():
            for i in range(4):
                load_r(i).wait()
        for d in order:
            dot_r(TILE * d)
            on_side(d, lambda d=d: xr(d).start())
            off_side(d, lambda d=d: no_row_r(d))
            fold_s(1 - d)
            send_y_side(1 - d)
        send_y(2)
        dot_r(STRIP)
        dot_r(32)
        recv_y(0)
        recv_y(1)
        for d in (order[1], order[0]):
            fold_r(d)
            update(MG + 39 * d, 9, ci, 32, om, True)
            recv_y_side(d)
            update(MG + 30 * d, 18, cd, STRIP, om, True)
            send_ry_side(d)
            send_rx(d)
        update(17, 30, ci, 32, om, True)
        recv_y(2)
        update(26, 12, cd, STRIP, om, True)
        send_ry_mid()
        recv_r()
        for j in range(3):
            yz_mid(j).wait_send()
        for d in SIDES:
            yz_side(d).wait_send()
        return carry

    lax.fori_loop(0, SWEEPS - 1, sweep, 0)

    def fy(j, p0, n):
        return remote(fys.at[pl.ds(p0, n)], fyr_.at[pl.ds(p0, n)], fy_s.at[j], fy_r.at[j], ydev)

    def send_fy(j, p0, n):
        for q in range(n):
            a = MG + 2 * (p0 + q)
            fys[p0 + q] = jnp.concatenate([z[a, pl.ds(hc, MG), :], z[a + 1, pl.ds(hc, MG), :]], axis=0).astype(BF16)
        fy(j, p0, n).start()

    def fxsd(d):
        return remote(fxs.at[d], fxsr.at[1 - d], fx_s.at[d], fx_r.at[1 - d], xdev(d))

    def fxsd_in(d):
        return remote(fxs.at[d], fxsr.at[d], fx_s.at[d], fx_r.at[d], xdev(d))

    def fxrd(d):
        return remote(fxr.at[d], fxrr.at[1 - d], fx_s.at[2 + d], fx_r.at[3 - d], xdev(d))

    def fxrd_in(d):
        return remote(fxr.at[d], fxrr.at[d], fx_s.at[2 + d], fx_r.at[2 + d], xdev(d))

    def last_s(d):
        for i in range(MG):
            fxs[d, i] = z[END * d + i, pl.ds(sc, STRIP), :].astype(BF16)
        fxsd(d).start()

    def last_r(d):
        for i in range(4):
            a = END * d + 2 * i
            fxr[d, i] = jnp.concatenate([z[a, pl.ds(gc, REST), :], z[a + 1, pl.ds(gc, REST), :]], axis=0).astype(BF16)
        fxrd(d).start()

    def last_fold_s(d):
        fxsd_in(d).wait_recv()
        for i in range(MG):
            a = MG + REST * d + i
            z[a, pl.ds(sc, STRIP), :] = z[a, pl.ds(sc, STRIP), :] + fxsr[d, i].astype(F32)

    def last_fold_r(d):
        fxrd_in(d).wait_recv()
        for i in range(4):
            a = MG + REST * d + 2 * i
            v = fxrr[d, i].astype(F32)
            z[a, pl.ds(gc, REST), :] = z[a, pl.ds(gc, REST), :] + v[0:REST]
            z[a + 1, pl.ds(gc, REST), :] = z[a + 1, pl.ds(gc, REST), :] + v[REST:80]

    def last_y(j, p0, n):
        fy(j, p0, n).wait_recv()

        def body(i, c):
            v = fyr_[p0 + i].astype(F32)
            a = MG + 2 * (p0 + i)
            z[a, pl.ds(mc, MG), :] = z[a, pl.ds(mc, MG), :] + v[0:MG]
            z[a + 1, pl.ds(mc, MG), :] = z[a + 1, pl.ds(mc, MG), :] + v[MG:STRIP]
            return c
        lax.fori_loop(0, n, body, 0)

    def add_u(a0, rows):
        def body(i, c):
            u[a0 - MG + i] = u[a0 - MG + i] + om * z[a0 + i, MG:END, :]
            return c
        lax.fori_loop(0, rows, body, 0)

    for j in SIDES:
        dot_s(STRIP + STRIP * j)
        send_fy(j, *FCHUNKS[j])
    for d in order:
        dot_s(TILE * d)
        on_side(d, lambda d=d: last_s(d))
    for d in order:
        dot_r(TILE * d)
        on_side(d, lambda d=d: last_r(d))
        on_side(1 - d, lambda d=d: last_fold_s(1 - d))
        send_fy(3 - d, 20 * (1 - d), 4)
    dot_r(STRIP)
    dot_r(32)
    for j in SIDES:
        last_y(j, *FCHUNKS[j])
    add_u(STRIP, 32)
    for d in (order[1], order[0]):
        on_side(d, lambda d=d: last_fold_r(d))
        last_y(2 + d, 20 * d, 4)
        add_u(MG + REST * d, MG)
    for j in SIDES:
        fy(j, *FCHUNKS[j]).wait_send()
        fy(2 + j, 20 * j, 4).wait_send()

        def sent(j=j):
            fxsd(j).wait_send()
            fxrd(j).wait_send()
        on_side(j, sent)


def solution(mesh):
    def local_step(forcing, u_init, diffusivity, local_solve, relax_omega):
        any_spec = pl.BlockSpec(memory_space=pltpu.HBM)
        dma = pltpu.SemaphoreType.DMA
        return pl.pallas_call(
            kernel,
            out_shape=jax.ShapeDtypeStruct((TILE, TILE, RHS), F32),
            in_specs=[pl.BlockSpec(memory_space=pltpu.SMEM)] + [any_spec] * 4,
            out_specs=pl.BlockSpec(memory_space=pltpu.VMEM),
            scratch_shapes=[
                pltpu.VMEM((EXT, STRIP, WIN), BF16),
                pltpu.VMEM((EXT, REST, WIN), BF16),
                pltpu.VMEM((EXT, EXT, RHS), BF16),
                pltpu.VMEM((EXT, EXT, RHS), F32),
                pltpu.VMEM((EXT, EXT, RHS), F32),
                pltpu.VMEM((49, EXT, 128), F32),
                pltpu.VMEM((TILE, EXT, 128), F32),
                pltpu.VMEM((TILE, TILE), F32),
                pltpu.VMEM((3, TILE, TILE), F32),
                pltpu.VMEM((128, 128), F32),
                pltpu.VMEM((YLEN, MG, RHS), F32),
                pltpu.VMEM((YLEN, MG, RHS), F32),
                pltpu.VMEM((2, 9, STRIP, RHS), F32),
                pltpu.VMEM((2, 9, REST, RHS), F32),
                pltpu.VMEM((24, STRIP, RHS), BF16),
                pltpu.VMEM((24, STRIP, RHS), BF16),
                pltpu.VMEM((2, MG, TILE, RHS), BF16),
                pltpu.VMEM((2, MG, TILE, RHS), BF16),
                pltpu.VMEM((2, 4, STRIP, RHS), BF16),
                pltpu.VMEM((6, MG, RHS), F32),
                pltpu.VMEM((6, MG, RHS), F32),
                pltpu.VMEM((24, STRIP, RHS), BF16),
                pltpu.VMEM((24, STRIP, RHS), BF16),
                pltpu.VMEM((2, MG, STRIP, RHS), BF16),
                pltpu.VMEM((2, MG, STRIP, RHS), BF16),
                pltpu.VMEM((2, 4, 80, RHS), BF16),
                pltpu.VMEM((2, 4, 80, RHS), BF16),
                dma((5,)), dma((5,)), dma((2,)), dma((2,)), dma((2,)), dma((2,)),
                dma((3,)), dma((3,)), dma((2,)), dma((2,)), dma((2,)), dma((2,)),
                dma((6,)), dma((6,)), dma((4,)), dma((4,)), dma((4,)), dma((4,)), dma((4,)), dma((MG,)),
            ],
            compiler_params=pltpu.CompilerParams(
                collective_id=0, has_side_effects=True, vmem_limit_bytes=54_000_000),
            name="schwarz",
        )(relax_omega.reshape(1), forcing, u_init, diffusivity,
          local_solve.reshape(EXT, EXT, WIN))

    field_spec = P('row', 'col', None)
    return jax.shard_map(local_step, mesh=mesh,
                         in_specs=(field_spec, field_spec, P('row', 'col'), P('row', 'col', None, None), P()),
                         out_specs=field_spec, check_vma=False)
```

```python
import functools

import jax
import jax.numpy as jnp
from jax import lax
from jax.experimental import pallas as pl
from jax.experimental.pallas import tpu as pltpu
from jax.sharding import PartitionSpec as P

SWEEPS = 4
TILE = 48
EXT = 64
WIN = EXT * EXT
RHS = 256
MG = 8
STRIP = 16
REST = 40
END = 56
SIDES = (0, 1)
F32 = jnp.float32
BF16 = jnp.bfloat16
MESH = pl.DeviceIdType.MESH

CHUNKS = ((STRIP, 12, 0), (36, 12, 14), (28, MG, 28))
SIDE_OFF = 37
YLEN = 59
RMID = (9, 6)
FCHUNKS = ((4, MG), (12, MG))

def kernel(omega, f_hbm, u_hbm, kap_hbm, m_hbm, u,
           ms, mr, w, z, r, wx, wy, kown, krecv, kfull,
           ys, yr, xrs, xrr, rsy, rry, rsx, rrx, rrd, ues, uer,
           fys, fyr_, fxs, fxsr, fxr, fxrr,
           yz_s, yz_r, xs_s, xs_r, xr_s, xr_r, ry_s, ry_r, rx_s, rx_r, rd_s, rd_r,
           ie_s, ie_r, fy_s, fy_r, fx_s, fx_r, lsem, msem):
    col = lax.axis_index("col")
    row = lax.axis_index("row")
    has_up = row > 0
    has_dn = row < 3
    ydev = (1 - col, row)
    has = (has_up, has_dn)
    first = jnp.where(row < 2, 1, 0)
    order = (first, 1 - first)

    def xdev(d):
        return (col, row - 1 + 2 * d)

    def ddev(d):
        return (1 - col, row - 1 + 2 * d)

    def on_side(d, fn):
        there = jnp.where(d == 0, row, 3 - row) > 0
        pl.when(there)(fn)

    def off_side(d, fn):
        there = jnp.where(d == 0, row, 3 - row) > 0
        pl.when(jnp.logical_not(there))(fn)

    hc = pl.multiple_of(END - END * col, MG)
    mc = pl.multiple_of(TILE - REST * col, MG)
    oc = pl.multiple_of(END * col, MG)
    sc = pl.multiple_of(TILE - TILE * col, STRIP)
    rc = pl.multiple_of(STRIP * col, STRIP)
    gc = pl.multiple_of(MG + MG * col, MG)
    cd = pl.multiple_of(REST - 32 * col, MG)
    ci = pl.multiple_of(MG + STRIP * col, MG)
    es = 55 - 47 * col
    er = END - 49 * col

    def remote(src, dst, ss, rs, dev):
        return pltpu.make_async_remote_copy(src_ref=src, dst_ref=dst, send_sem=ss, recv_sem=rs,
                                            device_id=dev, device_id_type=MESH)

    inner = (pl.ds(MG, TILE), pl.ds(MG, TILE))
    cp_k = pltpu.make_async_copy(kap_hbm, kown, lsem.at[0])
    cp_z = pltpu.make_async_copy(u_hbm, z.at[inner], lsem.at[1])
    cp_r = pltpu.make_async_copy(f_hbm, r.at[inner], lsem.at[2])
    cp_u = pltpu.make_async_copy(u_hbm, u, lsem.at[3])
    for cp in (cp_k, cp_z, cp_r):
        cp.start()

    def load_s(i):
        return pltpu.make_async_copy(m_hbm.at[pl.ds(STRIP * i, STRIP), pl.ds(sc, STRIP)], ms.at[pl.ds(STRIP * i, STRIP)], msem.at[i])

    def load_r(i):
        return pltpu.make_async_copy(m_hbm.at[pl.ds(STRIP * i, STRIP), pl.ds(gc, REST)], mr.at[pl.ds(STRIP * i, STRIP)], msem.at[4 + i])

    for i in range(4):
        load_s(i).start()
    for i in range(4):
        load_r(i).start()
    cp_u.start()

    for ref in (z, r):
        ref[0:MG] = jnp.zeros((MG, EXT, RHS), F32)
        ref[END:EXT] = jnp.zeros((MG, EXT, RHS), F32)
        ref[MG:END, 0:MG] = jnp.zeros((TILE, MG, RHS), F32)
        ref[MG:END, END:EXT] = jnp.zeros((TILE, MG, RHS), F32)
    kfull[...] = jnp.zeros_like(kfull)
    ys[...] = jnp.zeros_like(ys)

    bar = pltpu.get_barrier_semaphore()
    pl.semaphore_signal(bar, inc=1, device_id=ydev, device_id_type=MESH)
    for d in SIDES:
        @pl.when(has[d])
        def _(d=d):
            pl.semaphore_signal(bar, inc=1, device_id=xdev(d), device_id_type=MESH)
            pl.semaphore_signal(bar, inc=1, device_id=ddev(d), device_id_type=MESH)
    n_sides = has_up.astype(jnp.int32) + has_dn.astype(jnp.int32)
    pl.semaphore_wait(bar, 1 + 2 * n_sides)

    cp_k.wait()
    k_y = remote(kown, krecv.at[2], ie_s.at[0], ie_r.at[0], ydev)
    k_y.start()
    k_x = [remote(kown, krecv.at[1 - d], ie_s.at[1 + d], ie_r.at[2 - d], xdev(d)) for d in SIDES]
    u_x = [remote(z.at[MG if d == 0 else 55, pl.ds(MG, TILE)], z.at[END if d == 0 else 7, pl.ds(MG, TILE)],
                  ie_s.at[3 + d], ie_r.at[4 - d], xdev(d)) for d in SIDES]
    k_in = [remote(kown, krecv.at[d], ie_s.at[1 + d], ie_r.at[1 + d], xdev(d)) for d in SIDES]
    u_in = [remote(z.at[MG if d == 0 else 55, pl.ds(MG, TILE)], z.at[7 if d == 0 else END, pl.ds(MG, TILE)],
                   ie_s.at[3 + d], ie_r.at[3 + d], xdev(d)) for d in SIDES]
    cp_z.wait()
    for k in range(TILE):
        ues[k // MG, k % MG, :] = z[MG + k, pl.ds(es, 1), :][0]
    u_y = remote(ues, uer, ie_s.at[5], ie_r.at[5], ydev)
    u_y.start()
    for d in SIDES:
        @pl.when(has[d])
        def _(d=d):
            k_x[d].start()
            u_x[d].start()

    kfull[MG:END, MG:END] = kown[...]
    for d in SIDES:
        @pl.when(has[d])
        def _(d=d):
            k_in[d].wait_recv()
            src = 47 if d == 0 else 0
            dst = 7 if d == 0 else END
            kfull[dst:dst + 1, MG:END] = krecv[d, src:src + 1, :]
    k_y.wait_recv()

    @pl.when(col == 0)
    def _():
        kfull[MG:END, END:57] = krecv[2, :, 0:1]

    @pl.when(col == 1)
    def _():
        kfull[MG:END, 7:MG] = krecv[2, :, 47:TILE]

    kt = kfull[...].T
    prev = jnp.broadcast_to(kt[0:EXT, 7:MG], (EXT, 128))
    for a in range(MG, 57):
        here = jnp.broadcast_to(kt[0:EXT, a:a + 1], (EXT, 128))
        wx[a - MG] = 0.5 * (prev + here)
        if a < END:
            wy[a - MG] = 0.5 * (pltpu.roll(here, 1, 0) + here)
        prev = here

    def both(v):
        return jnp.concatenate([v, v], axis=1)

    def update(a0, rows, c0, n, om, add_u):
        def body(i, carry):
            a = a0 + i
            wide = z[a, pl.ds(c0 - MG, n + STRIP), :]
            fy = both(wy[a - MG, pl.ds(c0 - MG, n + STRIP), :]) * (wide - pltpu.roll(wide, 1, 0))
            fyr = pltpu.roll(fy, n + 15, 0)
            mid = wide[MG:MG + n]
            az = (both(wx[a - MG, pl.ds(c0, n), :]) * (mid - z[a - 1, pl.ds(c0, n), :])
                  + both(wx[a - 7, pl.ds(c0, n), :]) * (mid - z[a + 1, pl.ds(c0, n), :])
                  + fy[MG:MG + n] - fyr[MG:MG + n])
            r[a, pl.ds(c0, n), :] = r[a, pl.ds(c0, n), :] - om * az
            if add_u:
                u[a - MG, pl.ds(c0 - MG, n), :] = u[a - MG, pl.ds(c0 - MG, n), :] + om * mid
            return carry
        lax.fori_loop(0, rows, body, 0)

    def ry(p0, n, j):
        return remote(rsy.at[pl.ds(p0, n)], rry.at[pl.ds(p0, n)], ry_s.at[j], ry_r.at[j], ydev)

    def ry_mid():
        return ry(*RMID, 2)

    def ry_side(d):
        return ry(15 * d, 9, d)

    def rx(d):
        return remote(rsx.at[d], rrx.at[1 - d], rx_s.at[d], rx_r.at[1 - d], xdev(d))

    def rx_in(d):
        return remote(rsx.at[d], rrx.at[d], rx_s.at[d], rx_r.at[d], xdev(d))

    def rd(d):
        return remote(rsy.at[pl.ds(20 * d, 4)], rrd.at[1 - d], rd_s.at[d], rd_r.at[1 - d], ddev(d))

    def rd_in(d):
        return remote(rsy.at[pl.ds(20 * d, 4)], rrd.at[d], rd_s.at[d], rd_r.at[d], ddev(d))

    def pack_ry(p0, n):
        for q in range(n):
            a = MG + 2 * (p0 + q)
            rsy[p0 + q] = jnp.concatenate([r[a, pl.ds(mc, MG), :], r[a + 1, pl.ds(mc, MG), :]], axis=0).astype(BF16)

    def send_ry_side(d):
        pack_ry(15 * d, 9)
        on_side(d, lambda: rd(d).start())
        ry_side(d).start()

    def send_ry_mid():
        pack_ry(*RMID)
        ry_mid().start()

    def send_rx(d):
        for i in range(MG):
            rsx[d, i] = r[MG + REST * d + i, MG:END, :].astype(BF16)
        on_side(d, lambda: rx(d).start())

    def to_w(a0, rows, c0, n):
        def body(i, carry):
            w[a0 + i, pl.ds(c0, n), :] = r[a0 + i, pl.ds(c0, n), :].astype(BF16)
            return carry
        lax.fori_loop(0, rows, body, 0)

    def unpack_ry(p0, n):
        def body(i, carry):
            v = rry[p0 + i].astype(F32)
            a = MG + 2 * (p0 + i)
            r[a, pl.ds(hc, MG), :] = v[0:MG]
            r[a + 1, pl.ds(hc, MG), :] = v[MG:STRIP]
            w[a, pl.ds(sc, STRIP), :] = r[a, pl.ds(sc, STRIP), :].astype(BF16)
            w[a + 1, pl.ds(sc, STRIP), :] = r[a + 1, pl.ds(sc, STRIP), :].astype(BF16)
            return carry
        lax.fori_loop(0, n, body, 0)

    def recv_r():
        to_w(MG, TILE, rc, TILE)
        for d in (order[1], order[0]):
            ry_side(d).wait_recv()
            unpack_ry(15 * d, 9)

            def side(d=d):
                rx_in(d).wait_recv()
                rd_in(d).wait_recv()
                for i in range(MG):
                    r[END * d + i, MG:END, :] = rrx[d, i].astype(F32)
                for q in range(4):
                    v = rrd[d, q].astype(F32)
                    r[END * d + 2 * q, pl.ds(hc, MG), :] = v[0:MG]
                    r[END * d + 2 * q + 1, pl.ds(hc, MG), :] = v[MG:STRIP]
                to_w(END * d, MG, 0, EXT)
            on_side(d, side)
        ry_mid().wait_recv()
        unpack_ry(*RMID)
        ry_mid().wait_send()
        for d in SIDES:
            ry_side(d).wait_send()

            def sent(d=d):
                rx(d).wait_send()
                rd(d).wait_send()
            on_side(d, sent)

    for d in SIDES:
        @pl.when(has[d])
        def _(d=d):
            u_in[d].wait_recv()
    u_y.wait_recv()
    for k in range(TILE):
        z[MG + k, pl.ds(er, 1), :] = uer[k // MG, k % MG, :][None]
    cp_r.wait()
    update(MG, TILE, cd, STRIP, 1.0, False)
    for d in SIDES:
        send_ry_side(d)
    send_ry_mid()
    update(MG, TILE, ci, 32, 1.0, False)
    for d in SIDES:
        send_rx(d)
        off_side(d, lambda d=d: to_w(END * d, MG, 0, EXT))
    recv_r()
    k_y.wait_send()
    u_y.wait_send()
    for d in SIDES:
        @pl.when(has[d])
        def _(d=d):
            k_x[d].wait_send()
            u_x[d].wait_send()
    cp_u.wait()

    om = omega[0]

    def dot_s(a0):
        lhs = ms[pl.ds(a0, STRIP)].reshape(RHS, WIN)
        z[pl.ds(a0, STRIP), pl.ds(sc, STRIP), :] = jnp.dot(
            lhs, w[...].reshape(WIN, RHS), preferred_element_type=F32).reshape(STRIP, STRIP, RHS)

    def dot_r(a0):
        lhs = mr[pl.ds(a0, STRIP)].reshape(640, WIN)
        z[pl.ds(a0, STRIP), pl.ds(gc, REST), :] = jnp.dot(
            lhs, w[...].reshape(WIN, RHS), preferred_element_type=F32).reshape(STRIP, REST, RHS)

    def yz(j, off, length):
        return remote(ys.at[pl.ds(off, length)], yr.at[pl.ds(off, length)], yz_s.at[j], yz_r.at[j], ydev)

    def yz_mid(j):
        return yz(j, CHUNKS[j][2], CHUNKS[j][1] + pl.cdiv(CHUNKS[j][1], MG))

    def yz_side(d):
        return yz(3 + d, SIDE_OFF + 11 * d, 11)

    def pack_y(a0, n, off):
        for k in range(n):
            ys[off + k] = z[a0 + k, pl.ds(hc, MG), :]
            ys[off + n + k // MG, k % MG, :] = z[a0 + k, pl.ds(es, 1), :][0]

    def add_y(a0, n, off):
        for k in range(n):
            z[a0 + k, pl.ds(mc, MG), :] = z[a0 + k, pl.ds(mc, MG), :] + yr[off + k]
            z[a0 + k, pl.ds(er, 1), :] = z[a0 + k, pl.ds(er, 1), :] + yr[off + n + k // MG, k % MG, :][None]

    def send_y(j):
        pack_y(*CHUNKS[j])
        yz_mid(j).start()

    def send_y_side(d):
        pack_y(7 + 41 * d, 9, SIDE_OFF + 11 * d)
        yz_side(d).start()

    def recv_y(j):
        yz_mid(j).wait_recv()
        add_y(*CHUNKS[j])

    def recv_y_side(d):
        yz_side(d).wait_recv()
        add_y(7 + 41 * d, 9, SIDE_OFF + 11 * d)

    def xs(d):
        return remote(z.at[pl.ds(55 * d, 9), pl.ds(sc, STRIP)], xrs.at[1 - d], xs_s.at[d], xs_r.at[1 - d], xdev(d))

    def xs_in(d):
        return remote(z.at[pl.ds(55 * d, 9), pl.ds(sc, STRIP)], xrs.at[d], xs_s.at[d], xs_r.at[d], xdev(d))

    def xr(d):
        return remote(z.at[pl.ds(55 * d, 9), pl.ds(gc, REST)], xrr.at[1 - d], xr_s.at[d], xr_r.at[1 - d], xdev(d))

    def xr_in(d):
        return remote(z.at[pl.ds(55 * d, 9), pl.ds(gc, REST)], xrr.at[d], xr_s.at[d], xr_r.at[d], xdev(d))

    def fold_s(d):
        def side():
            xs(d).wait_send()
            xs_in(d).wait_recv()
            for k in range(9):
                a = 7 + 41 * d + k
                z[a, pl.ds(sc, STRIP), :] = z[a, pl.ds(sc, STRIP), :] + xrs[d, k]
        on_side(d, side)

    def fold_r(d):
        def side():
            xr(d).wait_send()
            xr_in(d).wait_recv()
            for k in range(9):
                a = 7 + 41 * d + k
                z[a, pl.ds(gc, REST), :] = z[a, pl.ds(gc, REST), :] + xrr[d, k]
        on_side(d, side)

    def no_row_s(d):
        z[7 + 49 * d, pl.ds(sc, STRIP), :] = jnp.zeros((STRIP, RHS), F32)

    def no_row_r(d):
        z[7 + 49 * d, pl.ds(gc, REST), :] = jnp.zeros((REST, RHS), F32)

    def sweep(s, carry):
        @pl.when(s == 0)
        def _():
            for i in range(4):
                load_s(i).wait()
        dot_s(STRIP)
        send_y(0)
        dot_s(32)
        send_y(1)

        def ends_s(i, c):
            d = jnp.where(i == 0, first, 1 - first)
            dot_s(TILE * d)
            on_side(d, lambda: xs(d).start())
            off_side(d, lambda: no_row_s(d))
            return c
        lax.fori_loop(0, 2, ends_s, 0)

        @pl.when(s == 0)
        def _():
            for i in range(4):
                load_r(i).wait()
        def ends_r(i, c):
            d = jnp.where(i == 0, first, 1 - first)
            dot_r(TILE * d)
            on_side(d, lambda: xr(d).start())
            off_side(d, lambda: no_row_r(d))
            fold_s(1 - d)
            send_y_side(1 - d)
            return c
        lax.fori_loop(0, 2, ends_r, 0)
        send_y(2)
        lax.fori_loop(1, 3, lambda i, c: (dot_r(STRIP * i), c)[1], 0)
        recv_y(0)
        recv_y(1)
        def ends_u(i, c):
            d = jnp.where(i == 0, 1 - first, first)
            fold_r(d)
            update(MG + 39 * d, 9, ci, 32, om, True)
            recv_y_side(d)
            update(MG + 30 * d, 18, cd, STRIP, om, True)
            send_ry_side(d)
            send_rx(d)
            return c
        lax.fori_loop(0, 2, ends_u, 0)
        update(17, 30, ci, 32, om, True)
        recv_y(2)
        update(26, 12, cd, STRIP, om, True)
        send_ry_mid()
        recv_r()
        for j in range(3):
            yz_mid(j).wait_send()
        for d in SIDES:
            yz_side(d).wait_send()
        return carry

    lax.fori_loop(0, SWEEPS - 1, sweep, 0)

    def fy(j, p0, n):
        return remote(fys.at[pl.ds(p0, n)], fyr_.at[pl.ds(p0, n)], fy_s.at[j], fy_r.at[j], ydev)

    def send_fy(j, p0, n):
        for q in range(n):
            a = MG + 2 * (p0 + q)
            fys[p0 + q] = jnp.concatenate([z[a, pl.ds(hc, MG), :], z[a + 1, pl.ds(hc, MG), :]], axis=0).astype(BF16)
        fy(j, p0, n).start()

    def fxsd(d):
        return remote(fxs.at[d], fxsr.at[1 - d], fx_s.at[d], fx_r.at[1 - d], xdev(d))

    def fxsd_in(d):
        return remote(fxs.at[d], fxsr.at[d], fx_s.at[d], fx_r.at[d], xdev(d))

    def fxrd(d):
        return remote(fxr.at[d], fxrr.at[1 - d], fx_s.at[2 + d], fx_r.at[3 - d], xdev(d))

    def fxrd_in(d):
        return remote(fxr.at[d], fxrr.at[d], fx_s.at[2 + d], fx_r.at[2 + d], xdev(d))

    def last_s(d):
        for i in range(MG):
            fxs[d, i] = z[END * d + i, pl.ds(sc, STRIP), :].astype(BF16)
        fxsd(d).start()

    def last_r(d):
        for i in range(4):
            a = END * d + 2 * i
            fxr[d, i] = jnp.concatenate([z[a, pl.ds(gc, REST), :], z[a + 1, pl.ds(gc, REST), :]], axis=0).astype(BF16)
        fxrd(d).start()

    def last_fold_s(d):
        fxsd_in(d).wait_recv()
        for i in range(MG):
            a = MG + REST * d + i
            z[a, pl.ds(sc, STRIP), :] = z[a, pl.ds(sc, STRIP), :] + fxsr[d, i].astype(F32)

    def last_fold_r(d):
        fxrd_in(d).wait_recv()
        for i in range(4):
            a = MG + REST * d + 2 * i
            v = fxrr[d, i].astype(F32)
            z[a, pl.ds(gc, REST), :] = z[a, pl.ds(gc, REST), :] + v[0:REST]
            z[a + 1, pl.ds(gc, REST), :] = z[a + 1, pl.ds(gc, REST), :] + v[REST:80]

    def last_y(j, p0, n):
        fy(j, p0, n).wait_recv()

        def body(i, c):
            v = fyr_[p0 + i].astype(F32)
            a = MG + 2 * (p0 + i)
            z[a, pl.ds(mc, MG), :] = z[a, pl.ds(mc, MG), :] + v[0:MG]
            z[a + 1, pl.ds(mc, MG), :] = z[a + 1, pl.ds(mc, MG), :] + v[MG:STRIP]
            return c
        lax.fori_loop(0, n, body, 0)

    def add_u(a0, rows):
        def body(i, c):
            u[a0 - MG + i] = u[a0 - MG + i] + om * z[a0 + i, MG:END, :]
            return c
        lax.fori_loop(0, rows, body, 0)

    for j in SIDES:
        dot_s(STRIP + STRIP * j)
        send_fy(j, *FCHUNKS[j])

    def last_ends_s(i, c):
        d = jnp.where(i == 0, first, 1 - first)
        dot_s(TILE * d)
        on_side(d, lambda: last_s(d))
        return c
    lax.fori_loop(0, 2, last_ends_s, 0)

    def last_ends_r(i, c):
        d = jnp.where(i == 0, first, 1 - first)
        dot_r(TILE * d)
        on_side(d, lambda: last_r(d))
        on_side(1 - d, lambda: last_fold_s(1 - d))
        send_fy(3 - d, 20 * (1 - d), 4)
        return c
    lax.fori_loop(0, 2, last_ends_r, 0)
    lax.fori_loop(1, 3, lambda i, c: (dot_r(STRIP * i), c)[1], 0)
    for j in SIDES:
        last_y(j, *FCHUNKS[j])
    add_u(STRIP, 32)
    for d in (order[1], order[0]):
        on_side(d, lambda d=d: last_fold_r(d))
        last_y(2 + d, 20 * d, 4)
        add_u(MG + REST * d, MG)
    for j in SIDES:
        fy(j, *FCHUNKS[j]).wait_send()
        fy(2 + j, 20 * j, 4).wait_send()

        def sent(j=j):
            fxsd(j).wait_send()
            fxrd(j).wait_send()
        on_side(j, sent)


def solution(mesh):
    def local_step(forcing, u_init, diffusivity, local_solve, relax_omega):
        any_spec = pl.BlockSpec(memory_space=pltpu.HBM)
        dma = pltpu.SemaphoreType.DMA
        return pl.pallas_call(
            kernel,
            out_shape=jax.ShapeDtypeStruct((TILE, TILE, RHS), F32),
            in_specs=[pl.BlockSpec(memory_space=pltpu.SMEM)] + [any_spec] * 4,
            out_specs=pl.BlockSpec(memory_space=pltpu.VMEM),
            scratch_shapes=[
                pltpu.VMEM((EXT, STRIP, WIN), BF16),
                pltpu.VMEM((EXT, REST, WIN), BF16),
                pltpu.VMEM((EXT, EXT, RHS), BF16),
                pltpu.VMEM((EXT, EXT, RHS), F32),
                pltpu.VMEM((EXT, EXT, RHS), F32),
                pltpu.VMEM((49, EXT, 128), F32),
                pltpu.VMEM((TILE, EXT, 128), F32),
                pltpu.VMEM((TILE, TILE), F32),
                pltpu.VMEM((3, TILE, TILE), F32),
                pltpu.VMEM((128, 128), F32),
                pltpu.VMEM((YLEN, MG, RHS), F32),
                pltpu.VMEM((YLEN, MG, RHS), F32),
                pltpu.VMEM((2, 9, STRIP, RHS), F32),
                pltpu.VMEM((2, 9, REST, RHS), F32),
                pltpu.VMEM((24, STRIP, RHS), BF16),
                pltpu.VMEM((24, STRIP, RHS), BF16),
                pltpu.VMEM((2, MG, TILE, RHS), BF16),
                pltpu.VMEM((2, MG, TILE, RHS), BF16),
                pltpu.VMEM((2, 4, STRIP, RHS), BF16),
                pltpu.VMEM((6, MG, RHS), F32),
                pltpu.VMEM((6, MG, RHS), F32),
                pltpu.VMEM((24, STRIP, RHS), BF16),
                pltpu.VMEM((24, STRIP, RHS), BF16),
                pltpu.VMEM((2, MG, STRIP, RHS), BF16),
                pltpu.VMEM((2, MG, STRIP, RHS), BF16),
                pltpu.VMEM((2, 4, 80, RHS), BF16),
                pltpu.VMEM((2, 4, 80, RHS), BF16),
                dma((5,)), dma((5,)), dma((2,)), dma((2,)), dma((2,)), dma((2,)),
                dma((3,)), dma((3,)), dma((2,)), dma((2,)), dma((2,)), dma((2,)),
                dma((6,)), dma((6,)), dma((4,)), dma((4,)), dma((4,)), dma((4,)), dma((4,)), dma((MG,)),
            ],
            compiler_params=pltpu.CompilerParams(
                collective_id=0, has_side_effects=True, vmem_limit_bytes=54_000_000),
            name="schwarz",
        )(relax_omega.reshape(1), forcing, u_init, diffusivity,
          local_solve.reshape(EXT, EXT, WIN))

    field_spec = P('row', 'col', None)
    return jax.shard_map(local_step, mesh=mesh,
                         in_specs=(field_spec, field_spec, P('row', 'col'), P('row', 'col', None, None), P()),
                         out_specs=field_spec, check_vma=False)
```

```python
import functools

import jax
import jax.numpy as jnp
from jax import lax
from jax.experimental import pallas as pl
from jax.experimental.pallas import tpu as pltpu
from jax.sharding import PartitionSpec as P

SWEEPS = 4
TILE = 48
EXT = 64
WIN = EXT * EXT
RHS = 256
MG = 8
STRIP = 16
REST = 40
END = 56
SIDES = (0, 1)
F32 = jnp.float32
BF16 = jnp.bfloat16
MESH = pl.DeviceIdType.MESH

CHUNKS = ((STRIP, 12, 0), (36, 12, 14), (28, MG, 28))
SIDE_OFF = 37
YLEN = 59
RMID = (9, 6)
FCHUNKS = ((4, MG), (12, MG))

def kernel(omega, f_hbm, u_hbm, kap_hbm, m_hbm, u,
           ms, mr, w, z, r, wx, wy, kown, krecv, kfull,
           ys, yr, xrs, xrr, rsy, rry, rsx, rrx, rrd, ues, uer,
           fys, fyr_, fxs, fxsr, fxr, fxrr,
           yz_s, yz_r, xs_s, xs_r, xr_s, xr_r, ry_s, ry_r, rx_s, rx_r, rd_s, rd_r,
           ie_s, ie_r, fy_s, fy_r, fx_s, fx_r, lsem, msem):
    col = lax.axis_index("col")
    row = lax.axis_index("row")
    has_up = row > 0
    has_dn = row < 3
    ydev = (1 - col, row)
    has = (has_up, has_dn)
    first = jnp.where(row < 2, 1, 0)
    order = (first, 1 - first)

    def xdev(d):
        return (col, row - 1 + 2 * d)

    def ddev(d):
        return (1 - col, row - 1 + 2 * d)

    def on_side(d, fn):
        there = jnp.where(d == 0, row, 3 - row) > 0
        pl.when(there)(fn)

    def off_side(d, fn):
        there = jnp.where(d == 0, row, 3 - row) > 0
        pl.when(jnp.logical_not(there))(fn)

    hc = pl.multiple_of(END - END * col, MG)
    mc = pl.multiple_of(TILE - REST * col, MG)
    oc = pl.multiple_of(END * col, MG)
    sc = pl.multiple_of(TILE - TILE * col, STRIP)
    rc = pl.multiple_of(STRIP * col, STRIP)
    gc = pl.multiple_of(MG + MG * col, MG)
    cd = pl.multiple_of(REST - 32 * col, MG)
    ci = pl.multiple_of(MG + STRIP * col, MG)
    es = 55 - 47 * col
    er = END - 49 * col

    def remote(src, dst, ss, rs, dev):
        return pltpu.make_async_remote_copy(src_ref=src, dst_ref=dst, send_sem=ss, recv_sem=rs,
                                            device_id=dev, device_id_type=MESH)

    inner = (pl.ds(MG, TILE), pl.ds(MG, TILE))
    cp_k = pltpu.make_async_copy(kap_hbm, kown, lsem.at[0])
    cp_z = pltpu.make_async_copy(u_hbm, z.at[inner], lsem.at[1])
    cp_r = pltpu.make_async_copy(f_hbm, r.at[inner], lsem.at[2])
    cp_u = pltpu.make_async_copy(u_hbm, u, lsem.at[3])
    for cp in (cp_k, cp_z, cp_r):
        cp.start()

    def load_s(i):
        return pltpu.make_async_copy(m_hbm.at[pl.ds(STRIP * i, STRIP), pl.ds(sc, STRIP)], ms.at[pl.ds(STRIP * i, STRIP)], msem.at[i])

    def load_r(i):
        return pltpu.make_async_copy(m_hbm.at[pl.ds(STRIP * i, STRIP), pl.ds(gc, REST)], mr.at[pl.ds(STRIP * i, STRIP)], msem.at[4 + i])

    for ref in (z, r):
        ref[0:MG] = jnp.zeros((MG, EXT, RHS), F32)
        ref[END:EXT] = jnp.zeros((MG, EXT, RHS), F32)
        ref[MG:END, 0:MG] = jnp.zeros((TILE, MG, RHS), F32)
        ref[MG:END, END:EXT] = jnp.zeros((TILE, MG, RHS), F32)
    kfull[...] = jnp.zeros_like(kfull)
    ys[...] = jnp.zeros_like(ys)

    bar = pltpu.get_barrier_semaphore()
    pl.semaphore_signal(bar, inc=1, device_id=ydev, device_id_type=MESH)
    for d in SIDES:
        @pl.when(has[d])
        def _(d=d):
            pl.semaphore_signal(bar, inc=1, device_id=xdev(d), device_id_type=MESH)
            pl.semaphore_signal(bar, inc=1, device_id=ddev(d), device_id_type=MESH)
    n_sides = has_up.astype(jnp.int32) + has_dn.astype(jnp.int32)
    pl.semaphore_wait(bar, 1 + 2 * n_sides)

    cp_k.wait()
    k_y = remote(kown, krecv.at[2], ie_s.at[0], ie_r.at[0], ydev)
    k_y.start()
    k_x = [remote(kown, krecv.at[1 - d], ie_s.at[1 + d], ie_r.at[2 - d], xdev(d)) for d in SIDES]
    u_x = [remote(z.at[MG if d == 0 else 55, pl.ds(MG, TILE)], z.at[END if d == 0 else 7, pl.ds(MG, TILE)],
                  ie_s.at[3 + d], ie_r.at[4 - d], xdev(d)) for d in SIDES]
    k_in = [remote(kown, krecv.at[d], ie_s.at[1 + d], ie_r.at[1 + d], xdev(d)) for d in SIDES]
    u_in = [remote(z.at[MG if d == 0 else 55, pl.ds(MG, TILE)], z.at[7 if d == 0 else END, pl.ds(MG, TILE)],
                   ie_s.at[3 + d], ie_r.at[3 + d], xdev(d)) for d in SIDES]
    for d in SIDES:
        on_side(d, lambda d=d: k_x[d].start())
    cp_z.wait()
    for k in range(TILE):
        ues[k // MG, k % MG, :] = z[MG + k, pl.ds(es, 1), :][0]
    u_y = remote(ues, uer, ie_s.at[5], ie_r.at[5], ydev)
    u_y.start()
    for d in SIDES:
        on_side(d, lambda d=d: u_x[d].start())
    cp_r.wait()
    for i in range(4):
        load_s(i).start()
    for i in range(4):
        load_r(i).start()
    cp_u.start()

    kfull[MG:END, MG:END] = kown[...]
    for d in SIDES:
        @pl.when(has[d])
        def _(d=d):
            k_in[d].wait_recv()
            src = 47 if d == 0 else 0
            dst = 7 if d == 0 else END
            kfull[dst:dst + 1, MG:END] = krecv[d, src:src + 1, :]
    k_y.wait_recv()

    @pl.when(col == 0)
    def _():
        kfull[MG:END, END:57] = krecv[2, :, 0:1]

    @pl.when(col == 1)
    def _():
        kfull[MG:END, 7:MG] = krecv[2, :, 47:TILE]

    kt = kfull[...].T
    prev = jnp.broadcast_to(kt[0:EXT, 7:MG], (EXT, 128))
    for a in range(MG, 57):
        here = jnp.broadcast_to(kt[0:EXT, a:a + 1], (EXT, 128))
        wx[a - MG] = 0.5 * (prev + here)
        if a < END:
            wy[a - MG] = 0.5 * (pltpu.roll(here, 1, 0) + here)
        prev = here

    def both(v):
        return jnp.concatenate([v, v], axis=1)

    def update(a0, rows, c0, n, om, add_u):
        def body(i, carry):
            a = a0 + i
            wide = z[a, pl.ds(c0 - MG, n + STRIP), :]
            fy = both(wy[a - MG, pl.ds(c0 - MG, n + STRIP), :]) * (wide - pltpu.roll(wide, 1, 0))
            fyr = pltpu.roll(fy, n + 15, 0)
            mid = wide[MG:MG + n]
            az = (both(wx[a - MG, pl.ds(c0, n), :]) * (mid - z[a - 1, pl.ds(c0, n), :])
                  + both(wx[a - 7, pl.ds(c0, n), :]) * (mid - z[a + 1, pl.ds(c0, n), :])
                  + fy[MG:MG + n] - fyr[MG:MG + n])
            r[a, pl.ds(c0, n), :] = r[a, pl.ds(c0, n), :] - om * az
            if add_u:
                u[a - MG, pl.ds(c0 - MG, n), :] = u[a - MG, pl.ds(c0 - MG, n), :] + om * mid
            return carry
        lax.fori_loop(0, rows, body, 0)

    def ry(p0, n, j):
        return remote(rsy.at[pl.ds(p0, n)], rry.at[pl.ds(p0, n)], ry_s.at[j], ry_r.at[j], ydev)

    def ry_mid():
        return ry(*RMID, 2)

    def ry_side(d):
        return ry(15 * d, 9, d)

    def rx(d):
        return remote(rsx.at[d], rrx.at[1 - d], rx_s.at[d], rx_r.at[1 - d], xdev(d))

    def rx_in(d):
        return remote(rsx.at[d], rrx.at[d], rx_s.at[d], rx_r.at[d], xdev(d))

    def rd(d):
        return remote(rsy.at[pl.ds(20 * d, 4)], rrd.at[1 - d], rd_s.at[d], rd_r.at[1 - d], ddev(d))

    def rd_in(d):
        return remote(rsy.at[pl.ds(20 * d, 4)], rrd.at[d], rd_s.at[d], rd_r.at[d], ddev(d))

    def pack_ry(p0, n):
        for q in range(n):
            a = MG + 2 * (p0 + q)
            rsy[p0 + q] = jnp.concatenate([r[a, pl.ds(mc, MG), :], r[a + 1, pl.ds(mc, MG), :]], axis=0).astype(BF16)

    def send_ry_side(d):
        pack_ry(15 * d, 9)
        on_side(d, lambda: rd(d).start())
        ry_side(d).start()

    def send_ry_mid():
        pack_ry(*RMID)
        ry_mid().start()

    def send_rx(d):
        for i in range(MG):
            rsx[d, i] = r[MG + REST * d + i, MG:END, :].astype(BF16)
        on_side(d, lambda: rx(d).start())

    def to_w(a0, rows, c0, n):
        def body(i, carry):
            w[a0 + i, pl.ds(c0, n), :] = r[a0 + i, pl.ds(c0, n), :].astype(BF16)
            return carry
        lax.fori_loop(0, rows, body, 0)

    def unpack_ry(p0, n):
        def body(i, carry):
            v = rry[p0 + i].astype(F32)
            a = MG + 2 * (p0 + i)
            r[a, pl.ds(hc, MG), :] = v[0:MG]
            r[a + 1, pl.ds(hc, MG), :] = v[MG:STRIP]
            w[a, pl.ds(sc, STRIP), :] = r[a, pl.ds(sc, STRIP), :].astype(BF16)
            w[a + 1, pl.ds(sc, STRIP), :] = r[a + 1, pl.ds(sc, STRIP), :].astype(BF16)
            return carry
        lax.fori_loop(0, n, body, 0)

    def recv_r():
        to_w(MG, TILE, rc, TILE)
        for d in (order[1], order[0]):
            ry_side(d).wait_recv()
            unpack_ry(15 * d, 9)

            def side(d=d):
                rx_in(d).wait_recv()
                rd_in(d).wait_recv()
                for i in range(MG):
                    r[END * d + i, MG:END, :] = rrx[d, i].astype(F32)
                for q in range(4):
                    v = rrd[d, q].astype(F32)
                    r[END * d + 2 * q, pl.ds(hc, MG), :] = v[0:MG]
                    r[END * d + 2 * q + 1, pl.ds(hc, MG), :] = v[MG:STRIP]
                to_w(END * d, MG, 0, EXT)
            on_side(d, side)
        ry_mid().wait_recv()
        unpack_ry(*RMID)
        ry_mid().wait_send()
        for d in SIDES:
            ry_side(d).wait_send()

            def sent(d=d):
                rx(d).wait_send()
                rd(d).wait_send()
            on_side(d, sent)

    for d in SIDES:
        @pl.when(has[d])
        def _(d=d):
            u_in[d].wait_recv()
    u_y.wait_recv()
    for k in range(TILE):
        z[MG + k, pl.ds(er, 1), :] = uer[k // MG, k % MG, :][None]
    update(MG, 18, cd, STRIP, 1.0, False)
    update(38, 18, cd, STRIP, 1.0, False)
    for d in SIDES:
        send_ry_side(d)
    update(26, 12, cd, STRIP, 1.0, False)
    send_ry_mid()
    update(MG, MG, ci, 32, 1.0, False)
    update(TILE, MG, ci, 32, 1.0, False)
    for d in SIDES:
        send_rx(d)
        off_side(d, lambda d=d: to_w(END * d, MG, 0, EXT))
    update(STRIP, 32, ci, 32, 1.0, False)
    recv_r()
    k_y.wait_send()
    u_y.wait_send()
    for d in SIDES:
        @pl.when(has[d])
        def _(d=d):
            k_x[d].wait_send()
            u_x[d].wait_send()
    cp_u.wait()

    om = omega[0]

    def dot_s(a0):
        lhs = ms[pl.ds(a0, STRIP)].reshape(RHS, WIN)
        z[pl.ds(a0, STRIP), pl.ds(sc, STRIP), :] = jnp.dot(
            lhs, w[...].reshape(WIN, RHS), preferred_element_type=F32).reshape(STRIP, STRIP, RHS)

    def dot_r(a0):
        lhs = mr[pl.ds(a0, STRIP)].reshape(640, WIN)
        z[pl.ds(a0, STRIP), pl.ds(gc, REST), :] = jnp.dot(
            lhs, w[...].reshape(WIN, RHS), preferred_element_type=F32).reshape(STRIP, REST, RHS)

    def yz(j, off, length):
        return remote(ys.at[pl.ds(off, length)], yr.at[pl.ds(off, length)], yz_s.at[j], yz_r.at[j], ydev)

    def yz_mid(j):
        return yz(j, CHUNKS[j][2], CHUNKS[j][1] + pl.cdiv(CHUNKS[j][1], MG))

    def yz_side(d):
        return yz(3 + d, SIDE_OFF + 11 * d, 11)

    def pack_y(a0, n, off):
        for k in range(n):
            ys[off + k] = z[a0 + k, pl.ds(hc, MG), :]
            ys[off + n + k // MG, k % MG, :] = z[a0 + k, pl.ds(es, 1), :][0]

    def add_y(a0, n, off):
        for k in range(n):
            z[a0 + k, pl.ds(mc, MG), :] = z[a0 + k, pl.ds(mc, MG), :] + yr[off + k]
            z[a0 + k, pl.ds(er, 1), :] = z[a0 + k, pl.ds(er, 1), :] + yr[off + n + k // MG, k % MG, :][None]

    def send_y(j):
        pack_y(*CHUNKS[j])
        yz_mid(j).start()

    def send_y_side(d):
        pack_y(7 + 41 * d, 9, SIDE_OFF + 11 * d)
        yz_side(d).start()

    def recv_y(j):
        yz_mid(j).wait_recv()
        add_y(*CHUNKS[j])

    def recv_y_side(d):
        yz_side(d).wait_recv()
        add_y(7 + 41 * d, 9, SIDE_OFF + 11 * d)

    def xs(d):
        return remote(z.at[pl.ds(55 * d, 9), pl.ds(sc, STRIP)], xrs.at[1 - d], xs_s.at[d], xs_r.at[1 - d], xdev(d))

    def xs_in(d):
        return remote(z.at[pl.ds(55 * d, 9), pl.ds(sc, STRIP)], xrs.at[d], xs_s.at[d], xs_r.at[d], xdev(d))

    def xr(d):
        return remote(z.at[pl.ds(55 * d, 9), pl.ds(gc, REST)], xrr.at[1 - d], xr_s.at[d], xr_r.at[1 - d], xdev(d))

    def xr_in(d):
        return remote(z.at[pl.ds(55 * d, 9), pl.ds(gc, REST)], xrr.at[d], xr_s.at[d], xr_r.at[d], xdev(d))

    def fold_s(d):
        def side():
            xs(d).wait_send()
            xs_in(d).wait_recv()
            for k in range(9):
                a = 7 + 41 * d + k
                z[a, pl.ds(sc, STRIP), :] = z[a, pl.ds(sc, STRIP), :] + xrs[d, k]
        on_side(d, side)

    def fold_r(d):
        def side():
            xr(d).wait_send()
            xr_in(d).wait_recv()
            for k in range(9):
                a = 7 + 41 * d + k
                z[a, pl.ds(gc, REST), :] = z[a, pl.ds(gc, REST), :] + xrr[d, k]
        on_side(d, side)

    def no_row_s(d):
        z[7 + 49 * d, pl.ds(sc, STRIP), :] = jnp.zeros((STRIP, RHS), F32)

    def no_row_r(d):
        z[7 + 49 * d, pl.ds(gc, REST), :] = jnp.zeros((REST, RHS), F32)

    def sweep(s, carry):
        @pl.when(s == 0)
        def _():
            for i in range(4):
                load_s(i).wait()
        dot_s(STRIP)
        send_y(0)
        dot_s(32)
        send_y(1)

        def ends_s(i, c):
            d = jnp.where(i == 0, first, 1 - first)
            dot_s(TILE * d)
            on_side(d, lambda: xs(d).start())
            off_side(d, lambda: no_row_s(d))
            return c
        lax.fori_loop(0, 2, ends_s, 0)

        @pl.when(s == 0)
        def _():
            for i in range(4):
                load_r(i).wait()
        def ends_r(i, c):
            d = jnp.where(i == 0, first, 1 - first)
            dot_r(TILE * d)
            on_side(d, lambda: xr(d).start())
            off_side(d, lambda: no_row_r(d))
            fold_s(1 - d)
            send_y_side(1 - d)
            return c
        lax.fori_loop(0, 2, ends_r, 0)
        send_y(2)
        lax.fori_loop(1, 3, lambda i, c: (dot_r(STRIP * i), c)[1], 0)
        recv_y(0)
        recv_y(1)
        def ends_u(i, c):
            d = jnp.where(i == 0, 1 - first, first)
            fold_r(d)
            update(MG + 39 * d, 9, ci, 32, om, True)
            recv_y_side(d)
            update(MG + 30 * d, 18, cd, STRIP, om, True)
            send_ry_side(d)
            send_rx(d)
            return c
        lax.fori_loop(0, 2, ends_u, 0)
        update(17, 30, ci, 32, om, True)
        recv_y(2)
        update(26, 12, cd, STRIP, om, True)
        send_ry_mid()
        recv_r()
        for j in range(3):
            yz_mid(j).wait_send()
        for d in SIDES:
            yz_side(d).wait_send()
        return carry

    lax.fori_loop(0, SWEEPS - 1, sweep, 0)

    def fy(j, p0, n):
        return remote(fys.at[pl.ds(p0, n)], fyr_.at[pl.ds(p0, n)], fy_s.at[j], fy_r.at[j], ydev)

    def send_fy(j, p0, n):
        for q in range(n):
            a = MG + 2 * (p0 + q)
            fys[p0 + q] = jnp.concatenate([z[a, pl.ds(hc, MG), :], z[a + 1, pl.ds(hc, MG), :]], axis=0).astype(BF16)
        fy(j, p0, n).start()

    def fxsd(d):
        return remote(fxs.at[d], fxsr.at[1 - d], fx_s.at[d], fx_r.at[1 - d], xdev(d))

    def fxsd_in(d):
        return remote(fxs.at[d], fxsr.at[d], fx_s.at[d], fx_r.at[d], xdev(d))

    def fxrd(d):
        return remote(fxr.at[d], fxrr.at[1 - d], fx_s.at[2 + d], fx_r.at[3 - d], xdev(d))

    def fxrd_in(d):
        return remote(fxr.at[d], fxrr.at[d], fx_s.at[2 + d], fx_r.at[2 + d], xdev(d))

    def last_s(d):
        for i in range(MG):
            fxs[d, i] = z[END * d + i, pl.ds(sc, STRIP), :].astype(BF16)
        fxsd(d).start()

    def last_r(d):
        for i in range(4):
            a = END * d + 2 * i
            fxr[d, i] = jnp.concatenate([z[a, pl.ds(gc, REST), :], z[a + 1, pl.ds(gc, REST), :]], axis=0).astype(BF16)
        fxrd(d).start()

    def last_fold_s(d):
        fxsd_in(d).wait_recv()
        for i in range(MG):
            a = MG + REST * d + i
            z[a, pl.ds(sc, STRIP), :] = z[a, pl.ds(sc, STRIP), :] + fxsr[d, i].astype(F32)

    def last_fold_r(d):
        fxrd_in(d).wait_recv()
        for i in range(4):
            a = MG + REST * d + 2 * i
            v = fxrr[d, i].astype(F32)
            z[a, pl.ds(gc, REST), :] = z[a, pl.ds(gc, REST), :] + v[0:REST]
            z[a + 1, pl.ds(gc, REST), :] = z[a + 1, pl.ds(gc, REST), :] + v[REST:80]

    def last_y(j, p0, n):
        fy(j, p0, n).wait_recv()

        def body(i, c):
            v = fyr_[p0 + i].astype(F32)
            a = MG + 2 * (p0 + i)
            z[a, pl.ds(mc, MG), :] = z[a, pl.ds(mc, MG), :] + v[0:MG]
            z[a + 1, pl.ds(mc, MG), :] = z[a + 1, pl.ds(mc, MG), :] + v[MG:STRIP]
            return c
        lax.fori_loop(0, n, body, 0)

    def add_u(a0, rows):
        def body(i, c):
            u[a0 - MG + i] = u[a0 - MG + i] + om * z[a0 + i, MG:END, :]
            return c
        lax.fori_loop(0, rows, body, 0)

    for j in SIDES:
        dot_s(STRIP + STRIP * j)
        send_fy(j, *FCHUNKS[j])

    def last_ends_s(i, c):
        d = jnp.where(i == 0, first, 1 - first)
        dot_s(TILE * d)
        on_side(d, lambda: last_s(d))
        return c
    lax.fori_loop(0, 2, last_ends_s, 0)

    def last_ends_r(i, c):
        d = jnp.where(i == 0, first, 1 - first)
        dot_r(TILE * d)
        on_side(d, lambda: last_r(d))
        on_side(1 - d, lambda: last_fold_s(1 - d))
        send_fy(3 - d, 20 * (1 - d), 4)
        return c
    lax.fori_loop(0, 2, last_ends_r, 0)
    lax.fori_loop(1, 3, lambda i, c: (dot_r(STRIP * i), c)[1], 0)
    for j in SIDES:
        last_y(j, *FCHUNKS[j])
    add_u(STRIP, 32)
    for d in (order[1], order[0]):
        on_side(d, lambda d=d: last_fold_r(d))
        last_y(2 + d, 20 * d, 4)
        add_u(MG + REST * d, MG)
    for j in SIDES:
        fy(j, *FCHUNKS[j]).wait_send()
        fy(2 + j, 20 * j, 4).wait_send()

        def sent(j=j):
            fxsd(j).wait_send()
            fxrd(j).wait_send()
        on_side(j, sent)


def solution(mesh):
    def local_step(forcing, u_init, diffusivity, local_solve, relax_omega):
        any_spec = pl.BlockSpec(memory_space=pltpu.HBM)
        dma = pltpu.SemaphoreType.DMA
        return pl.pallas_call(
            kernel,
            out_shape=jax.ShapeDtypeStruct((TILE, TILE, RHS), F32),
            in_specs=[pl.BlockSpec(memory_space=pltpu.SMEM)] + [any_spec] * 4,
            out_specs=pl.BlockSpec(memory_space=pltpu.VMEM),
            scratch_shapes=[
                pltpu.VMEM((EXT, STRIP, WIN), BF16),
                pltpu.VMEM((EXT, REST, WIN), BF16),
                pltpu.VMEM((EXT, EXT, RHS), BF16),
                pltpu.VMEM((EXT, EXT, RHS), F32),
                pltpu.VMEM((EXT, EXT, RHS), F32),
                pltpu.VMEM((49, EXT, 128), F32),
                pltpu.VMEM((TILE, EXT, 128), F32),
                pltpu.VMEM((TILE, TILE), F32),
                pltpu.VMEM((3, TILE, TILE), F32),
                pltpu.VMEM((128, 128), F32),
                pltpu.VMEM((YLEN, MG, RHS), F32),
                pltpu.VMEM((YLEN, MG, RHS), F32),
                pltpu.VMEM((2, 9, STRIP, RHS), F32),
                pltpu.VMEM((2, 9, REST, RHS), F32),
                pltpu.VMEM((24, STRIP, RHS), BF16),
                pltpu.VMEM((24, STRIP, RHS), BF16),
                pltpu.VMEM((2, MG, TILE, RHS), BF16),
                pltpu.VMEM((2, MG, TILE, RHS), BF16),
                pltpu.VMEM((2, 4, STRIP, RHS), BF16),
                pltpu.VMEM((6, MG, RHS), F32),
                pltpu.VMEM((6, MG, RHS), F32),
                pltpu.VMEM((24, STRIP, RHS), BF16),
                pltpu.VMEM((24, STRIP, RHS), BF16),
                pltpu.VMEM((2, MG, STRIP, RHS), BF16),
                pltpu.VMEM((2, MG, STRIP, RHS), BF16),
                pltpu.VMEM((2, 4, 80, RHS), BF16),
                pltpu.VMEM((2, 4, 80, RHS), BF16),
                dma((5,)), dma((5,)), dma((2,)), dma((2,)), dma((2,)), dma((2,)),
                dma((3,)), dma((3,)), dma((2,)), dma((2,)), dma((2,)), dma((2,)),
                dma((6,)), dma((6,)), dma((4,)), dma((4,)), dma((4,)), dma((4,)), dma((4,)), dma((MG,)),
            ],
            compiler_params=pltpu.CompilerParams(
                collective_id=0, has_side_effects=True, vmem_limit_bytes=54_000_000),
            name="schwarz",
        )(relax_omega.reshape(1), forcing, u_init, diffusivity,
          local_solve.reshape(EXT, EXT, WIN))

    field_spec = P('row', 'col', None)
    return jax.shard_map(local_step, mesh=mesh,
                         in_specs=(field_spec, field_spec, P('row', 'col'), P('row', 'col', None, None), P()),
                         out_specs=field_spec, check_vma=False)
```

```python
import functools

import jax
import jax.numpy as jnp
from jax import lax
from jax.experimental import pallas as pl
from jax.experimental.pallas import tpu as pltpu
from jax.sharding import PartitionSpec as P

SWEEPS = 4
TILE = 48
EXT = 64
WIN = EXT * EXT
RHS = 256
MG = 8
STRIP = 16
REST = 40
END = 56
SIDES = (0, 1)
F32 = jnp.float32
BF16 = jnp.bfloat16
MESH = pl.DeviceIdType.MESH

CHUNKS = ((16, 16, 0), (40, 8, 18), (32, 8, 27))
SIDE_OFF = 36
YLEN = 56
RMID = (11, 6)
REARLY = (7, 4)
FCHUNKS = ((4, MG), (12, MG))

def kernel(omega, f_hbm, u_hbm, kap_hbm, m_hbm, u,
           ms, mr, w, z, r, wx, wy, kown, krecv, kfull,
           ys, yr, xrs, xrr, rsy, rry, rsx, rrx, rrd, ues, uer,
           fys, fyr_, fxs, fxsr, fxr, fxrr,
           yz_s, yz_r, xs_s, xs_r, xr_s, xr_r, ry_s, ry_r, rx_s, rx_r, rd_s, rd_r,
           ie_s, ie_r, fy_s, fy_r, fx_s, fx_r, lsem, msem):
    col = lax.axis_index("col")
    row = lax.axis_index("row")
    has_up = row > 0
    has_dn = row < 3
    ydev = (1 - col, row)
    has = (has_up, has_dn)
    first = jnp.where(row < 2, 1, 0)
    order = (first, 1 - first)

    def xdev(d):
        return (col, row - 1 + 2 * d)

    def ddev(d):
        return (1 - col, row - 1 + 2 * d)

    def on_side(d, fn):
        there = jnp.where(d == 0, row, 3 - row) > 0
        pl.when(there)(fn)

    def off_side(d, fn):
        there = jnp.where(d == 0, row, 3 - row) > 0
        pl.when(jnp.logical_not(there))(fn)

    hc = pl.multiple_of(END - END * col, MG)
    mc = pl.multiple_of(TILE - REST * col, MG)
    oc = pl.multiple_of(END * col, MG)
    sc = pl.multiple_of(TILE - TILE * col, STRIP)
    rc = pl.multiple_of(STRIP * col, STRIP)
    gc = pl.multiple_of(MG + MG * col, MG)
    cd = pl.multiple_of(REST - 32 * col, MG)
    ci = pl.multiple_of(MG + STRIP * col, MG)
    es = 55 - 47 * col
    er = END - 49 * col

    def remote(src, dst, ss, rs, dev):
        return pltpu.make_async_remote_copy(src_ref=src, dst_ref=dst, send_sem=ss, recv_sem=rs,
                                            device_id=dev, device_id_type=MESH)

    inner = (pl.ds(MG, TILE), pl.ds(MG, TILE))
    cp_k = pltpu.make_async_copy(kap_hbm, kown, lsem.at[0])
    cp_z = pltpu.make_async_copy(u_hbm, z.at[inner], lsem.at[1])
    cp_r = pltpu.make_async_copy(f_hbm, r.at[inner], lsem.at[2])
    cp_u = pltpu.make_async_copy(u_hbm, u, lsem.at[3])
    for cp in (cp_k, cp_z, cp_r):
        cp.start()

    def load_s(i):
        return pltpu.make_async_copy(m_hbm.at[pl.ds(STRIP * i, STRIP), pl.ds(sc, STRIP)], ms.at[pl.ds(STRIP * i, STRIP)], msem.at[i])

    def load_r(i):
        return pltpu.make_async_copy(m_hbm.at[pl.ds(STRIP * i, STRIP), pl.ds(gc, REST)], mr.at[pl.ds(STRIP * i, STRIP)], msem.at[4 + i])

    for ref in (z, r):
        ref[0:MG] = jnp.zeros((MG, EXT, RHS), F32)
        ref[END:EXT] = jnp.zeros((MG, EXT, RHS), F32)
        ref[MG:END, 0:MG] = jnp.zeros((TILE, MG, RHS), F32)
        ref[MG:END, END:EXT] = jnp.zeros((TILE, MG, RHS), F32)
    kfull[...] = jnp.zeros_like(kfull)
    ys[...] = jnp.zeros_like(ys)

    bar = pltpu.get_barrier_semaphore()
    pl.semaphore_signal(bar, inc=1, device_id=ydev, device_id_type=MESH)
    for d in SIDES:
        @pl.when(has[d])
        def _(d=d):
            pl.semaphore_signal(bar, inc=1, device_id=xdev(d), device_id_type=MESH)
            pl.semaphore_signal(bar, inc=1, device_id=ddev(d), device_id_type=MESH)
    n_sides = has_up.astype(jnp.int32) + has_dn.astype(jnp.int32)
    pl.semaphore_wait(bar, 1 + 2 * n_sides)

    cp_k.wait()
    k_y = remote(kown, krecv.at[2], ie_s.at[0], ie_r.at[0], ydev)
    k_y.start()
    k_x = [remote(kown, krecv.at[1 - d], ie_s.at[1 + d], ie_r.at[2 - d], xdev(d)) for d in SIDES]
    u_x = [remote(z.at[MG if d == 0 else 55, pl.ds(MG, TILE)], z.at[END if d == 0 else 7, pl.ds(MG, TILE)],
                  ie_s.at[3 + d], ie_r.at[4 - d], xdev(d)) for d in SIDES]
    k_in = [remote(kown, krecv.at[d], ie_s.at[1 + d], ie_r.at[1 + d], xdev(d)) for d in SIDES]
    u_in = [remote(z.at[MG if d == 0 else 55, pl.ds(MG, TILE)], z.at[7 if d == 0 else END, pl.ds(MG, TILE)],
                   ie_s.at[3 + d], ie_r.at[3 + d], xdev(d)) for d in SIDES]
    for d in SIDES:
        on_side(d, lambda d=d: k_x[d].start())
    cp_z.wait()
    for k in range(TILE):
        ues[k // MG, k % MG, :] = z[MG + k, pl.ds(es, 1), :][0]
    u_y = remote(ues, uer, ie_s.at[5], ie_r.at[5], ydev)
    u_y.start()
    for d in SIDES:
        on_side(d, lambda d=d: u_x[d].start())
    cp_r.wait()
    for i in range(4):
        load_s(i).start()
    for i in range(4):
        load_r(i).start()
    cp_u.start()

    kfull[MG:END, MG:END] = kown[...]
    for d in SIDES:
        @pl.when(has[d])
        def _(d=d):
            k_in[d].wait_recv()
            src = 47 if d == 0 else 0
            dst = 7 if d == 0 else END
            kfull[dst:dst + 1, MG:END] = krecv[d, src:src + 1, :]
    k_y.wait_recv()

    @pl.when(col == 0)
    def _():
        kfull[MG:END, END:57] = krecv[2, :, 0:1]

    @pl.when(col == 1)
    def _():
        kfull[MG:END, 7:MG] = krecv[2, :, 47:TILE]

    kt = kfull[...].T
    prev = jnp.broadcast_to(kt[0:EXT, 7:MG], (EXT, 128))
    for a in range(MG, 57):
        here = jnp.broadcast_to(kt[0:EXT, a:a + 1], (EXT, 128))
        wx[a - MG] = 0.5 * (prev + here)
        if a < END:
            wy[a - MG] = 0.5 * (pltpu.roll(here, 1, 0) + here)
        prev = here

    def both(v):
        return jnp.concatenate([v, v], axis=1)

    def update(a0, rows, c0, n, om, add_u):
        def body(i, carry):
            a = a0 + i
            wide = z[a, pl.ds(c0 - MG, n + STRIP), :]
            fy = both(wy[a - MG, pl.ds(c0 - MG, n + STRIP), :]) * (wide - pltpu.roll(wide, 1, 0))
            fyr = pltpu.roll(fy, n + 15, 0)
            mid = wide[MG:MG + n]
            az = (both(wx[a - MG, pl.ds(c0, n), :]) * (mid - z[a - 1, pl.ds(c0, n), :])
                  + both(wx[a - 7, pl.ds(c0, n), :]) * (mid - z[a + 1, pl.ds(c0, n), :])
                  + fy[MG:MG + n] - fyr[MG:MG + n])
            r[a, pl.ds(c0, n), :] = r[a, pl.ds(c0, n), :] - om * az
            if add_u:
                u[a - MG, pl.ds(c0 - MG, n), :] = u[a - MG, pl.ds(c0 - MG, n), :] + om * mid
            return carry
        lax.fori_loop(0, rows, body, 0)

    def ry(p0, n, j):
        return remote(rsy.at[pl.ds(p0, n)], rry.at[pl.ds(p0, n)], ry_s.at[j], ry_r.at[j], ydev)

    def ry_mid():
        return ry(*RMID, 2)

    def ry_early():
        return ry(*REARLY, 3)

    def ry_side(d):
        return ry(17 * d, 7, d)

    def rx(d):
        return remote(rsx.at[d], rrx.at[1 - d], rx_s.at[d], rx_r.at[1 - d], xdev(d))

    def rx_in(d):
        return remote(rsx.at[d], rrx.at[d], rx_s.at[d], rx_r.at[d], xdev(d))

    def rd(d):
        return remote(rsy.at[pl.ds(20 * d, 4)], rrd.at[1 - d], rd_s.at[d], rd_r.at[1 - d], ddev(d))

    def rd_forward(d):
        return remote(rry.at[pl.ds(20 * d, 4)], rrd.at[1 - d], rd_s.at[d], rd_r.at[1 - d], xdev(d))

    def same_chip(d):
        return lax.rem(row + d, 2) == 1

    def rd_in(d):
        return remote(rsy.at[pl.ds(20 * d, 4)], rrd.at[d], rd_s.at[d], rd_r.at[d], ddev(d))

    def pack_ry(p0, n):
        for q in range(n):
            a = MG + 2 * (p0 + q)
            rsy[p0 + q] = jnp.concatenate([r[a, pl.ds(mc, MG), :], r[a + 1, pl.ds(mc, MG), :]], axis=0).astype(BF16)

    def send_ry_side(d):
        pack_ry(17 * d, 7)
        on_side(d, lambda: pl.when(jnp.logical_not(same_chip(d)))(lambda: rd(d).start()))
        ry_side(d).start()

    def send_ry_mid():
        pack_ry(*RMID)
        ry_mid().start()

    def send_ry_early():
        pack_ry(*REARLY)
        ry_early().start()

    def send_rx(d):
        for i in range(MG):
            rsx[d, i] = r[MG + REST * d + i, MG:END, :].astype(BF16)
        on_side(d, lambda: rx(d).start())

    def to_w(a0, rows, c0, n):
        def body(i, carry):
            w[a0 + i, pl.ds(c0, n), :] = r[a0 + i, pl.ds(c0, n), :].astype(BF16)
            return carry
        lax.fori_loop(0, rows, body, 0)

    def unpack_ry(p0, n):
        def body(i, carry):
            v = rry[p0 + i].astype(F32)
            a = MG + 2 * (p0 + i)
            r[a, pl.ds(hc, MG), :] = v[0:MG]
            r[a + 1, pl.ds(hc, MG), :] = v[MG:STRIP]
            w[a, pl.ds(sc, STRIP), :] = r[a, pl.ds(sc, STRIP), :].astype(BF16)
            w[a + 1, pl.ds(sc, STRIP), :] = r[a + 1, pl.ds(sc, STRIP), :].astype(BF16)
            return carry
        lax.fori_loop(0, n, body, 0)

    def recv_r():
        to_w(MG, TILE, rc, TILE)
        ry_early().wait_recv()
        unpack_ry(*REARLY)
        for d in (order[1], order[0]):
            ry_side(d).wait_recv()
            on_side(d, lambda d=d: pl.when(same_chip(d))(lambda: rd_forward(d).start()))
            unpack_ry(17 * d, 7)
        for d in (order[1], order[0]):
            def side(d=d):
                rx_in(d).wait_recv()
                rd_in(d).wait_recv()
                for i in range(MG):
                    r[END * d + i, MG:END, :] = rrx[d, i].astype(F32)
                for q in range(4):
                    v = rrd[d, q].astype(F32)
                    r[END * d + 2 * q, pl.ds(hc, MG), :] = v[0:MG]
                    r[END * d + 2 * q + 1, pl.ds(hc, MG), :] = v[MG:STRIP]
                to_w(END * d, MG, 0, EXT)
            on_side(d, side)
        ry_mid().wait_recv()
        unpack_ry(*RMID)
        ry_mid().wait_send()
        ry_early().wait_send()
        for d in SIDES:
            ry_side(d).wait_send()

            def sent(d=d):
                rx(d).wait_send()
                rd(d).wait_send()
            on_side(d, sent)

    for d in SIDES:
        @pl.when(has[d])
        def _(d=d):
            u_in[d].wait_recv()
    u_y.wait_recv()
    for k in range(TILE):
        z[MG + k, pl.ds(er, 1), :] = uer[k // MG, k % MG, :][None]
    for d in SIDES:
        update(MG + 34 * d, 14, cd, STRIP, 1.0, False)
    for d in SIDES:
        send_ry_side(d)
    update(22, 20, cd, STRIP, 1.0, False)
    send_ry_early()
    send_ry_mid()
    update(MG, MG, ci, 32, 1.0, False)
    update(TILE, MG, ci, 32, 1.0, False)
    for d in SIDES:
        send_rx(d)
        off_side(d, lambda d=d: to_w(END * d, MG, 0, EXT))
    update(STRIP, 32, ci, 32, 1.0, False)
    recv_r()
    k_y.wait_send()
    u_y.wait_send()
    for d in SIDES:
        @pl.when(has[d])
        def _(d=d):
            k_x[d].wait_send()
            u_x[d].wait_send()
    cp_u.wait()

    om = omega[0]

    def dot_s(a0):
        lhs = ms[pl.ds(a0, STRIP)].reshape(RHS, WIN)
        z[pl.ds(a0, STRIP), pl.ds(sc, STRIP), :] = jnp.dot(
            lhs, w[...].reshape(WIN, RHS), preferred_element_type=F32).reshape(STRIP, STRIP, RHS)

    def dot_r(a0):
        lhs = mr[pl.ds(a0, STRIP)].reshape(640, WIN)
        z[pl.ds(a0, STRIP), pl.ds(gc, REST), :] = jnp.dot(
            lhs, w[...].reshape(WIN, RHS), preferred_element_type=F32).reshape(STRIP, REST, RHS)

    def yz(j, off, length):
        return remote(ys.at[pl.ds(off, length)], yr.at[pl.ds(off, length)], yz_s.at[j], yz_r.at[j], ydev)

    def yz_mid(j):
        return yz(j, CHUNKS[j][2], CHUNKS[j][1] + pl.cdiv(CHUNKS[j][1], MG))

    def yz_side(d):
        return yz(3 + d, SIDE_OFF + 10 * d, 10)

    def pack_y(a0, n, off, e0, ne):
        for k in range(n):
            ys[off + k] = z[a0 + k, pl.ds(hc, MG), :]
        for k in range(ne):
            ys[off + n + k // MG, k % MG, :] = z[e0 + k, pl.ds(es, 1), :][0]

    def add_y(a0, n, off, e0, ne):
        for k in range(n):
            z[a0 + k, pl.ds(mc, MG), :] = z[a0 + k, pl.ds(mc, MG), :] + yr[off + k]
        for k in range(ne):
            z[e0 + k, pl.ds(er, 1), :] = z[e0 + k, pl.ds(er, 1), :] + yr[off + n + k // MG, k % MG, :][None]

    def side_rows(d):
        return 7 + 41 * d, 9, SIDE_OFF + 10 * d, MG + REST * d, MG

    def send_y(j):
        pack_y(*CHUNKS[j], *CHUNKS[j][:2])
        yz_mid(j).start()

    def send_y_side(d):
        pack_y(*side_rows(d))
        yz_side(d).start()

    def recv_y(j):
        yz_mid(j).wait_recv()
        add_y(*CHUNKS[j], *CHUNKS[j][:2])

    def recv_y_side(d):
        yz_side(d).wait_recv()
        add_y(*side_rows(d))

    def xs(d):
        return remote(z.at[pl.ds(55 * d, 9), pl.ds(sc, STRIP)], xrs.at[1 - d], xs_s.at[d], xs_r.at[1 - d], xdev(d))

    def xs_in(d):
        return remote(z.at[pl.ds(55 * d, 9), pl.ds(sc, STRIP)], xrs.at[d], xs_s.at[d], xs_r.at[d], xdev(d))

    def xr(d):
        return remote(z.at[pl.ds(55 * d, 9), pl.ds(gc, REST)], xrr.at[1 - d], xr_s.at[d], xr_r.at[1 - d], xdev(d))

    def xr_in(d):
        return remote(z.at[pl.ds(55 * d, 9), pl.ds(gc, REST)], xrr.at[d], xr_s.at[d], xr_r.at[d], xdev(d))

    def fold_s(d):
        def side():
            xs(d).wait_send()
            xs_in(d).wait_recv()
            for k in range(9):
                a = 7 + 41 * d + k
                z[a, pl.ds(sc, STRIP), :] = z[a, pl.ds(sc, STRIP), :] + xrs[d, k]
        on_side(d, side)

    def fold_r(d):
        def side():
            xr(d).wait_send()
            xr_in(d).wait_recv()
            for k in range(9):
                a = 7 + 41 * d + k
                z[a, pl.ds(gc, REST), :] = z[a, pl.ds(gc, REST), :] + xrr[d, k]
        on_side(d, side)

    def no_row_s(d):
        z[7 + 49 * d, pl.ds(sc, STRIP), :] = jnp.zeros((STRIP, RHS), F32)

    def no_row_r(d):
        z[7 + 49 * d, pl.ds(gc, REST), :] = jnp.zeros((REST, RHS), F32)

    def sweep(s, carry):
        @pl.when(s == 0)
        def _():
            for i in range(4):
                load_s(i).wait()
        dot_s(STRIP)
        send_y(0)
        dot_s(32)
        send_y(1)

        def ends_s(i, c):
            d = jnp.where(i == 0, first, 1 - first)
            dot_s(TILE * d)
            on_side(d, lambda: xs(d).start())
            off_side(d, lambda: no_row_s(d))
            return c
        lax.fori_loop(0, 2, ends_s, 0)

        @pl.when(s == 0)
        def _():
            for i in range(4):
                load_r(i).wait()
        def ends_r(i, c):
            d = jnp.where(i == 0, first, 1 - first)
            dot_r(TILE * d)
            on_side(d, lambda: xr(d).start())
            off_side(d, lambda: no_row_r(d))
            fold_s(1 - d)
            send_y_side(1 - d)
            return c
        lax.fori_loop(0, 2, ends_r, 0)
        send_y(2)
        lax.fori_loop(1, 3, lambda i, c: (dot_r(STRIP * i), c)[1], 0)
        recv_y(0)
        update(22, MG, cd, STRIP, om, True)
        send_ry_early()
        recv_y(1)

        def ends_u(i, c):
            d = jnp.where(i == 0, 1 - first, first)
            fold_r(d)
            update(MG + 39 * d, 9, ci, 32, om, True)
            recv_y_side(d)
            update(MG + 34 * d, 14, cd, STRIP, om, True)
            send_ry_side(d)
            send_rx(d)
            return c
        lax.fori_loop(0, 2, ends_u, 0)
        update(17, 30, ci, 32, om, True)
        recv_y(2)
        update(30, 12, cd, STRIP, om, True)
        send_ry_mid()
        recv_r()
        for j in range(3):
            yz_mid(j).wait_send()
        for d in SIDES:
            yz_side(d).wait_send()
        return carry

    lax.fori_loop(0, SWEEPS - 1, sweep, 0)

    def fy(j, p0, n):
        return remote(fys.at[pl.ds(p0, n)], fyr_.at[pl.ds(p0, n)], fy_s.at[j], fy_r.at[j], ydev)

    def send_fy(j, p0, n):
        for q in range(n):
            a = MG + 2 * (p0 + q)
            fys[p0 + q] = jnp.concatenate([z[a, pl.ds(hc, MG), :], z[a + 1, pl.ds(hc, MG), :]], axis=0).astype(BF16)
        fy(j, p0, n).start()

    def fxsd(d):
        return remote(fxs.at[d], fxsr.at[1 - d], fx_s.at[d], fx_r.at[1 - d], xdev(d))

    def fxsd_in(d):
        return remote(fxs.at[d], fxsr.at[d], fx_s.at[d], fx_r.at[d], xdev(d))

    def fxrd(d):
        return remote(fxr.at[d], fxrr.at[1 - d], fx_s.at[2 + d], fx_r.at[3 - d], xdev(d))

    def fxrd_in(d):
        return remote(fxr.at[d], fxrr.at[d], fx_s.at[2 + d], fx_r.at[2 + d], xdev(d))

    def last_s(d):
        for i in range(MG):
            fxs[d, i] = z[END * d + i, pl.ds(sc, STRIP), :].astype(BF16)
        fxsd(d).start()

    def last_r(d):
        for i in range(4):
            a = END * d + 2 * i
            fxr[d, i] = jnp.concatenate([z[a, pl.ds(gc, REST), :], z[a + 1, pl.ds(gc, REST), :]], axis=0).astype(BF16)
        fxrd(d).start()

    def last_fold_s(d):
        fxsd_in(d).wait_recv()
        for i in range(MG):
            a = MG + REST * d + i
            z[a, pl.ds(sc, STRIP), :] = z[a, pl.ds(sc, STRIP), :] + fxsr[d, i].astype(F32)

    def last_fold_r(d):
        fxrd_in(d).wait_recv()
        for i in range(4):
            a = MG + REST * d + 2 * i
            v = fxrr[d, i].astype(F32)
            z[a, pl.ds(gc, REST), :] = z[a, pl.ds(gc, REST), :] + v[0:REST]
            z[a + 1, pl.ds(gc, REST), :] = z[a + 1, pl.ds(gc, REST), :] + v[REST:80]

    def last_y(j, p0, n):
        fy(j, p0, n).wait_recv()

        def body(i, c):
            v = fyr_[p0 + i].astype(F32)
            a = MG + 2 * (p0 + i)
            z[a, pl.ds(mc, MG), :] = z[a, pl.ds(mc, MG), :] + v[0:MG]
            z[a + 1, pl.ds(mc, MG), :] = z[a + 1, pl.ds(mc, MG), :] + v[MG:STRIP]
            return c
        lax.fori_loop(0, n, body, 0)

    def add_u(a0, rows):
        def body(i, c):
            u[a0 - MG + i] = u[a0 - MG + i] + om * z[a0 + i, MG:END, :]
            return c
        lax.fori_loop(0, rows, body, 0)

    for j in SIDES:
        dot_s(STRIP + STRIP * j)
        send_fy(j, *FCHUNKS[j])

    def last_ends_s(i, c):
        d = jnp.where(i == 0, first, 1 - first)
        dot_s(TILE * d)
        on_side(d, lambda: last_s(d))
        return c
    lax.fori_loop(0, 2, last_ends_s, 0)

    def last_ends_r(i, c):
        d = jnp.where(i == 0, first, 1 - first)
        dot_r(TILE * d)
        on_side(d, lambda: last_r(d))
        on_side(1 - d, lambda: last_fold_s(1 - d))
        send_fy(3 - d, 20 * (1 - d), 4)
        return c
    lax.fori_loop(0, 2, last_ends_r, 0)
    lax.fori_loop(1, 3, lambda i, c: (dot_r(STRIP * i), c)[1], 0)
    for j in SIDES:
        last_y(j, *FCHUNKS[j])
    add_u(STRIP, 32)
    for d in (order[1], order[0]):
        on_side(d, lambda d=d: last_fold_r(d))
        last_y(2 + d, 20 * d, 4)
        add_u(MG + REST * d, MG)
    for j in SIDES:
        fy(j, *FCHUNKS[j]).wait_send()
        fy(2 + j, 20 * j, 4).wait_send()

        def sent(j=j):
            fxsd(j).wait_send()
            fxrd(j).wait_send()
        on_side(j, sent)


def solution(mesh):
    def local_step(forcing, u_init, diffusivity, local_solve, relax_omega):
        any_spec = pl.BlockSpec(memory_space=pltpu.HBM)
        dma = pltpu.SemaphoreType.DMA
        return pl.pallas_call(
            kernel,
            out_shape=jax.ShapeDtypeStruct((TILE, TILE, RHS), F32),
            in_specs=[pl.BlockSpec(memory_space=pltpu.SMEM)] + [any_spec] * 4,
            out_specs=pl.BlockSpec(memory_space=pltpu.VMEM),
            scratch_shapes=[
                pltpu.VMEM((EXT, STRIP, WIN), BF16),
                pltpu.VMEM((EXT, REST, WIN), BF16),
                pltpu.VMEM((EXT, EXT, RHS), BF16),
                pltpu.VMEM((EXT, EXT, RHS), F32),
                pltpu.VMEM((EXT, EXT, RHS), F32),
                pltpu.VMEM((49, EXT, 128), F32),
                pltpu.VMEM((TILE, EXT, 128), F32),
                pltpu.VMEM((TILE, TILE), F32),
                pltpu.VMEM((3, TILE, TILE), F32),
                pltpu.VMEM((128, 128), F32),
                pltpu.VMEM((YLEN, MG, RHS), F32),
                pltpu.VMEM((YLEN, MG, RHS), F32),
                pltpu.VMEM((2, 9, STRIP, RHS), F32),
                pltpu.VMEM((2, 9, REST, RHS), F32),
                pltpu.VMEM((24, STRIP, RHS), BF16),
                pltpu.VMEM((24, STRIP, RHS), BF16),
                pltpu.VMEM((2, MG, TILE, RHS), BF16),
                pltpu.VMEM((2, MG, TILE, RHS), BF16),
                pltpu.VMEM((2, 4, STRIP, RHS), BF16),
                pltpu.VMEM((6, MG, RHS), F32),
                pltpu.VMEM((6, MG, RHS), F32),
                pltpu.VMEM((24, STRIP, RHS), BF16),
                pltpu.VMEM((24, STRIP, RHS), BF16),
                pltpu.VMEM((2, MG, STRIP, RHS), BF16),
                pltpu.VMEM((2, MG, STRIP, RHS), BF16),
                pltpu.VMEM((2, 4, 80, RHS), BF16),
                pltpu.VMEM((2, 4, 80, RHS), BF16),
                dma((5,)), dma((5,)), dma((2,)), dma((2,)), dma((2,)), dma((2,)),
                dma((4,)), dma((4,)), dma((2,)), dma((2,)), dma((2,)), dma((2,)),
                dma((6,)), dma((6,)), dma((4,)), dma((4,)), dma((4,)), dma((4,)), dma((4,)), dma((MG,)),
            ],
            compiler_params=pltpu.CompilerParams(
                collective_id=0, has_side_effects=True, vmem_limit_bytes=54_000_000),
            name="schwarz",
        )(relax_omega.reshape(1), forcing, u_init, diffusivity,
          local_solve.reshape(EXT, EXT, WIN))

    field_spec = P('row', 'col', None)
    return jax.shard_map(local_step, mesh=mesh,
                         in_specs=(field_spec, field_spec, P('row', 'col'), P('row', 'col', None, None), P()),
                         out_specs=field_spec, check_vma=False)
```

```python
import functools

import jax
import jax.numpy as jnp
from jax import lax
from jax.experimental import pallas as pl
from jax.experimental.pallas import tpu as pltpu
from jax.sharding import PartitionSpec as P

SWEEPS = 4
TILE = 48
EXT = 64
WIN = EXT * EXT
RHS = 256
MG = 8
STRIP = 16
REST = 40
END = 56
SIDES = (0, 1)
F32 = jnp.float32
BF16 = jnp.bfloat16
MESH = pl.DeviceIdType.MESH

CHUNKS = ((16, 16, 0), (40, 8, 18), (32, 8, 27))
SIDE_OFF = 36
YLEN = 56
RMID = (11, 6)
REARLY = (7, 4)
FCHUNKS = ((4, MG), (12, MG))

def kernel(omega, f_hbm, u_hbm, kown, m_hbm, u,
           ms, mr, w, z, r, wx, wy, krecv, kfull,
           ys, yr, xrs, xrr, rsy, rry, rsx, rrx, rrd, rdb, ues, uer, pcs, pcr,
           fys, fyr_, fxs, fxsr, fxr, fxrr,
           yz_s, yz_r, xs_s, xs_r, xr_s, xr_r, ry_s, ry_r, rx_s, rx_r, rd_s, rd_r,
           ie_s, ie_r, fy_s, fy_r, fx_s, fx_r, lsem, msem):
    col = lax.axis_index("col")
    row = lax.axis_index("row")
    has_up = row > 0
    has_dn = row < 3
    ydev = (1 - col, row)
    has = (has_up, has_dn)
    first = jnp.where(row < 2, 1, 0)
    order = (first, 1 - first)

    def xdev(d):
        return (col, row - 1 + 2 * d)

    def ddev(d):
        return (1 - col, row - 1 + 2 * d)

    def on_side(d, fn):
        there = jnp.where(d == 0, row, 3 - row) > 0
        pl.when(there)(fn)

    def off_side(d, fn):
        there = jnp.where(d == 0, row, 3 - row) > 0
        pl.when(jnp.logical_not(there))(fn)

    hc = pl.multiple_of(END - END * col, MG)
    mc = pl.multiple_of(TILE - REST * col, MG)
    oc = pl.multiple_of(END * col, MG)
    sc = pl.multiple_of(TILE - TILE * col, STRIP)
    rc = pl.multiple_of(STRIP * col, STRIP)
    gc = pl.multiple_of(MG + MG * col, MG)
    cd = pl.multiple_of(REST - 32 * col, MG)
    ci = pl.multiple_of(MG + STRIP * col, MG)
    es = 55 - 47 * col
    er = END - 49 * col
    face = END - TILE * col

    def remote(src, dst, ss, rs, dev):
        return pltpu.make_async_remote_copy(src_ref=src, dst_ref=dst, send_sem=ss, recv_sem=rs,
                                            device_id=dev, device_id_type=MESH)

    inner = (pl.ds(MG, TILE), pl.ds(MG, TILE))
    cp_z = pltpu.make_async_copy(u_hbm, z.at[inner], lsem.at[1])
    cp_r = pltpu.make_async_copy(f_hbm, r.at[inner], lsem.at[2])
    cp_u = pltpu.make_async_copy(u_hbm, u, lsem.at[3])
    for cp in (cp_z, cp_r):
        cp.start()

    def load_s(i):
        return pltpu.make_async_copy(m_hbm.at[pl.ds(STRIP * i, STRIP), pl.ds(sc, STRIP)], ms.at[pl.ds(STRIP * i, STRIP)], msem.at[i])

    def load_r(i):
        return pltpu.make_async_copy(m_hbm.at[pl.ds(STRIP * i, STRIP), pl.ds(gc, REST)], mr.at[pl.ds(STRIP * i, STRIP)], msem.at[4 + i])

    for a in (7, END):
        z[a] = jnp.zeros((EXT, RHS), F32)
    bar = pltpu.get_barrier_semaphore()
    pl.semaphore_signal(bar, inc=1, device_id=ydev, device_id_type=MESH)
    for d in SIDES:
        def greet(d=d):
            pl.semaphore_signal(bar, inc=1, device_id=xdev(d), device_id_type=MESH)
            pl.semaphore_signal(bar, inc=1, device_id=ddev(d), device_id_type=MESH)
        on_side(d, greet)
    r[7] = jnp.zeros((EXT, RHS), F32)
    r[END] = jnp.zeros((EXT, RHS), F32)
    for ref in (z, r):
        ref[0:7] = jnp.zeros((7, EXT, RHS), F32)
        ref[57:EXT] = jnp.zeros((7, EXT, RHS), F32)
        ref[MG:END, 0:MG] = jnp.zeros((TILE, MG, RHS), F32)
        ref[MG:END, END:EXT] = jnp.zeros((TILE, MG, RHS), F32)

    kfull[...] = jnp.zeros_like(kfull)
    kfull[MG:END, MG:END] = kown[...]
    kt = kfull[...].T
    prev = jnp.broadcast_to(kt[0:EXT, 7:MG], (EXT, 128))
    for a in range(MG, 57):
        here = jnp.broadcast_to(kt[0:EXT, a:a + 1], (EXT, 128))
        wx[a - MG] = 0.5 * (prev + here)
        if a < END:
            wy[a - MG] = 0.5 * (pltpu.roll(here, 1, 0) + here)
        prev = here
    for k in range(TILE):
        wy[k, pl.ds(face, 1), :] = jnp.zeros((1, 128), F32)
    n_sides = has_up.astype(jnp.int32) + has_dn.astype(jnp.int32)
    pl.semaphore_wait(bar, 1 + 2 * n_sides)

    k_y = remote(kown, krecv.at[2], ie_s.at[0], ie_r.at[0], ydev)
    k_y.start()
    k_x = [remote(kown, krecv.at[1 - d], ie_s.at[1 + d], ie_r.at[2 - d], xdev(d)) for d in SIDES]
    u_x = [remote(z.at[MG if d == 0 else 55, pl.ds(MG, TILE)], z.at[END if d == 0 else 7, pl.ds(MG, TILE)],
                  ie_s.at[3 + d], ie_r.at[4 - d], xdev(d)) for d in SIDES]
    k_in = [remote(kown, krecv.at[d], ie_s.at[1 + d], ie_r.at[1 + d], xdev(d)) for d in SIDES]
    u_in = [remote(z.at[MG if d == 0 else 55, pl.ds(MG, TILE)], z.at[7 if d == 0 else END, pl.ds(MG, TILE)],
                   ie_s.at[3 + d], ie_r.at[3 + d], xdev(d)) for d in SIDES]
    for d in SIDES:
        on_side(d, lambda d=d: k_x[d].start())
    cp_z.wait()
    for k in range(TILE):
        ues[k // MG, k % MG, :] = z[MG + k, pl.ds(es, 1), :][0]
    u_y = remote(ues, uer, ie_s.at[5], ie_r.at[5], ydev)
    u_y.start()
    for d in SIDES:
        on_side(d, lambda d=d: u_x[d].start())
    cp_r.wait()
    for i in range(4):
        load_s(i).start()
    load_r(3 * first).start()
    load_r(3 - 3 * first).start()
    for i in (1, 2):
        load_r(i).start()
    cp_u.start()

    def both(v):
        return jnp.concatenate([v, v], axis=1)

    def update(a0, rows, c0, n, om, add_u):
        def body(i, carry):
            a = a0 + i
            wide = z[a, pl.ds(c0 - MG, n + STRIP), :]
            fy = both(wy[a - MG, pl.ds(c0 - MG, n + STRIP), :]) * (wide - pltpu.roll(wide, 1, 0))
            fyr = pltpu.roll(fy, n + 15, 0)
            mid = wide[MG:MG + n]
            az = (both(wx[a - MG, pl.ds(c0, n), :]) * (mid - z[a - 1, pl.ds(c0, n), :])
                  + both(wx[a - 7, pl.ds(c0, n), :]) * (mid - z[a + 1, pl.ds(c0, n), :])
                  + fy[MG:MG + n] - fyr[MG:MG + n])
            r[a, pl.ds(c0, n), :] = r[a, pl.ds(c0, n), :] - om * az
            if add_u:
                u[a - MG, pl.ds(c0 - MG, n), :] = u[a - MG, pl.ds(c0 - MG, n), :] + om * mid
            return carry
        lax.fori_loop(0, rows, body, 0)

    def ry(p0, n, j):
        return remote(rsy.at[pl.ds(p0, n)], rry.at[pl.ds(p0, n)], ry_s.at[j], ry_r.at[j], ydev)

    def ry_mid():
        return ry(*RMID, 2)

    def ry_early():
        return ry(*REARLY, 3)

    def ry_side(d):
        return ry(17 * d, 7, d)

    def rx(d):
        return remote(rsx.at[d], rrx.at[1 - d], rx_s.at[d], rx_r.at[1 - d], xdev(d))

    def rx_in(d):
        return remote(rsx.at[d], rrx.at[d], rx_s.at[d], rx_r.at[d], xdev(d))

    def rd(d):
        return remote(rsy.at[pl.ds(20 * d, 4)], rrd.at[1 - d], rd_s.at[d], rd_r.at[1 - d], ddev(d))

    def rd_forward(d):
        return remote(rry.at[pl.ds(20 * d, 4)], rrd.at[1 - d], rd_s.at[d], rd_r.at[1 - d], xdev(d))

    def same_chip(d):
        return lax.rem(row + d, 2) == 1

    def rd_in(d):
        return remote(rsy.at[pl.ds(20 * d, 4)], rrd.at[d], rd_s.at[d], rd_r.at[d], ddev(d))

    def pack_ry(p0, n):
        for q in range(n):
            a = MG + 2 * (p0 + q)
            rsy[p0 + q] = jnp.concatenate([r[a, pl.ds(mc, MG), :], r[a + 1, pl.ds(mc, MG), :]], axis=0).astype(BF16)

    def send_ry_side(d):
        pack_ry(17 * d, 7)
        on_side(d, lambda: pl.when(jnp.logical_not(same_chip(d)))(lambda: rd(d).start()))
        ry_side(d).start()

    def send_ry_mid():
        pack_ry(*RMID)
        ry_mid().start()

    def send_ry_early():
        pack_ry(*REARLY)
        ry_early().start()

    def send_rx(d):
        for i in range(MG):
            rsx[d, i] = r[MG + REST * d + i, MG:END, :].astype(BF16)
        on_side(d, lambda: rx(d).start())

    def to_w(a0, rows, c0, n):
        def body(i, carry):
            w[a0 + i, pl.ds(c0, n), :] = r[a0 + i, pl.ds(c0, n), :].astype(BF16)
            return carry
        lax.fori_loop(0, rows, body, 0)

    def unpack_ry(p0, n):
        def body(i, carry):
            v = rry[p0 + i].astype(F32)
            a = MG + 2 * (p0 + i)
            r[a, pl.ds(hc, MG), :] = v[0:MG]
            r[a + 1, pl.ds(hc, MG), :] = v[MG:STRIP]
            w[a, pl.ds(sc, STRIP), :] = r[a, pl.ds(sc, STRIP), :].astype(BF16)
            w[a + 1, pl.ds(sc, STRIP), :] = r[a + 1, pl.ds(sc, STRIP), :].astype(BF16)
            return carry
        lax.fori_loop(0, n, body, 0)

    def recv_side(d):
        rx_in(d).wait_recv()
        rd_in(d).wait_recv()
        for i in range(MG):
            r[END * d + i, MG:END, :] = rrx[d, i].astype(F32)
        for q in range(4):
            v = rrd[d, q].astype(F32)
            r[END * d + 2 * q, pl.ds(hc, MG), :] = v[0:MG]
            r[END * d + 2 * q + 1, pl.ds(hc, MG), :] = v[MG:STRIP]
        to_w(END * d, MG, 0, EXT)

    def recv_r():
        to_w(MG, TILE, rc, TILE)
        ry_early().wait_recv()
        unpack_ry(*REARLY)
        for d in (order[1], order[0]):
            ry_side(d).wait_recv()
            on_side(d, lambda d=d: pl.when(same_chip(d))(lambda: rd_forward(d).start()))
            unpack_ry(17 * d, 7)
        for d in (order[1], order[0]):
            on_side(d, lambda d=d: recv_side(d))
        ry_mid().wait_recv()
        unpack_ry(*RMID)
        ry_mid().wait_send()
        ry_early().wait_send()
        for d in SIDES:
            ry_side(d).wait_send()

            def sent(d=d):
                rx(d).wait_send()
                rd(d).wait_send()
            on_side(d, sent)

    update(9, 46, cd, STRIP, 1.0, False)
    pack_ry(1, 22)
    ry(1, 22, 2).start()
    update(9, 46, ci, 32, 1.0, False)
    for d in SIDES:
        def edge(d=d):
            k_in[d].wait_recv()
            kfull[7 + 49 * d:MG + 49 * d, MG:END] = krecv[d, 47 - 47 * d:TILE - 47 * d, :]
            u_in[d].wait_recv()
        on_side(d, edge)
    kt = kfull[...].T
    for d in SIDES:
        a = MG + TILE * d
        wx[TILE * d] = 0.5 * (jnp.broadcast_to(kt[0:EXT, a - 1:a], (EXT, 128))
                              + jnp.broadcast_to(kt[0:EXT, a:a + 1], (EXT, 128)))
    for d in SIDES:
        update(MG + 47 * d, 1, cd, STRIP, 1.0, False)
        pack_ry(23 * d, 1)
        ry(23 * d, 1, d).start()
    for k in range(TILE):
        pcs[k // MG, k % MG, :] = r[MG + k, pl.ds(es, 1), :][0]
    p_y = remote(pcs, pcr, ie_s.at[6], ie_r.at[6], ydev)
    p_y.start()
    for d in SIDES:
        update(MG + 47 * d, 1, ci, 32, 1.0, False)
    k_y.wait_recv()
    u_y.wait_recv()

    def lane(ref, i):
        return jnp.broadcast_to(ref[:, i:i + 1], (TILE, 128))

    k_nb = krecv[2]
    k_me = kown[...]
    wf = 0.5 * (jnp.where(col == 0, lane(k_me, 47), lane(k_me, 0))
                + jnp.where(col == 0, lane(k_nb, 0), lane(k_nb, 47)))
    flux = both(wf) * (ues[...].reshape(TILE, RHS) - uer[...].reshape(TILE, RHS))
    mine = pcs[...].reshape(TILE, RHS) - flux
    for k in range(TILE):
        wy[k, pl.ds(face, 1), :] = wf[k:k + 1]
        r[MG + k, pl.ds(es, 1), :] = mine[k:k + 1]

    def corner(d):
        return remote(rdb.at[d], rrd.at[1 - d], rd_s.at[d], rd_r.at[1 - d], ddev(d))

    for d in SIDES:
        for q in range(4):
            a = MG + REST * d + 2 * q
            rdb[d, q] = jnp.concatenate([r[a, pl.ds(mc, MG), :], r[a + 1, pl.ds(mc, MG), :]], axis=0).astype(BF16)
        on_side(d, lambda d=d: corner(d).start())
        send_rx(d)
        off_side(d, lambda d=d: to_w(END * d, MG, 0, EXT))
    to_w(MG, TILE, rc, TILE)
    for d in SIDES:
        ry(23 * d, 1, d).wait_recv()
        unpack_ry(23 * d, 1)
    ry(1, 22, 2).wait_recv()
    unpack_ry(1, 22)
    p_y.wait_recv()
    theirs = pcr[...].reshape(TILE, RHS) + flux
    for k in range(TILE):
        r[MG + k, pl.ds(er, 1), :] = theirs[k:k + 1]
    to_w(MG, TILE, sc, STRIP)
    for d in (order[1], order[0]):
        on_side(d, lambda d=d: recv_side(d))
    ry(1, 22, 2).wait_send()
    for d in SIDES:
        ry(23 * d, 1, d).wait_send()

        def sent(d=d):
            k_x[d].wait_send()
            u_x[d].wait_send()
            rx(d).wait_send()
            corner(d).wait_send()
        on_side(d, sent)
    k_y.wait_send()
    u_y.wait_send()
    p_y.wait_send()

    om = omega[0]

    def dot_s(a0):
        lhs = ms[pl.ds(a0, STRIP)].reshape(RHS, WIN)
        z[pl.ds(a0, STRIP), pl.ds(sc, STRIP), :] = jnp.dot(
            lhs, w[...].reshape(WIN, RHS), preferred_element_type=F32).reshape(STRIP, STRIP, RHS)

    def dot_r(a0):
        lhs = mr[pl.ds(a0, STRIP)].reshape(640, WIN)
        z[pl.ds(a0, STRIP), pl.ds(gc, REST), :] = jnp.dot(
            lhs, w[...].reshape(WIN, RHS), preferred_element_type=F32).reshape(STRIP, REST, RHS)

    def yz(j, off, length):
        return remote(ys.at[pl.ds(off, length)], yr.at[pl.ds(off, length)], yz_s.at[j], yz_r.at[j], ydev)

    def yz_mid(j):
        return yz(j, CHUNKS[j][2], CHUNKS[j][1] + pl.cdiv(CHUNKS[j][1], MG))

    def yz_side(d):
        return yz(3 + d, SIDE_OFF + 10 * d, 10)

    def pack_y(a0, n, off, e0, ne):
        for k in range(n):
            ys[off + k] = z[a0 + k, pl.ds(hc, MG), :]
        for k in range(ne):
            ys[off + n + k // MG, k % MG, :] = z[e0 + k, pl.ds(es, 1), :][0]

    def add_y(a0, n, off, e0, ne):
        for k in range(n):
            z[a0 + k, pl.ds(mc, MG), :] = z[a0 + k, pl.ds(mc, MG), :] + yr[off + k]
        for k in range(ne):
            z[e0 + k, pl.ds(er, 1), :] = z[e0 + k, pl.ds(er, 1), :] + yr[off + n + k // MG, k % MG, :][None]

    def side_rows(d):
        return 7 + 41 * d, 9, SIDE_OFF + 10 * d, MG + REST * d, MG

    def send_y(j):
        pack_y(*CHUNKS[j], *CHUNKS[j][:2])
        yz_mid(j).start()

    def send_y_side(d):
        pack_y(*side_rows(d))
        yz_side(d).start()

    def recv_y(j):
        yz_mid(j).wait_recv()
        add_y(*CHUNKS[j], *CHUNKS[j][:2])

    def recv_y_side(d):
        yz_side(d).wait_recv()
        add_y(*side_rows(d))

    def xs(d):
        return remote(z.at[pl.ds(55 * d, 9), pl.ds(sc, STRIP)], xrs.at[1 - d], xs_s.at[d], xs_r.at[1 - d], xdev(d))

    def xs_in(d):
        return remote(z.at[pl.ds(55 * d, 9), pl.ds(sc, STRIP)], xrs.at[d], xs_s.at[d], xs_r.at[d], xdev(d))

    def xr(d):
        return remote(z.at[pl.ds(55 * d, 9), pl.ds(gc, REST)], xrr.at[1 - d], xr_s.at[d], xr_r.at[1 - d], xdev(d))

    def xr_in(d):
        return remote(z.at[pl.ds(55 * d, 9), pl.ds(gc, REST)], xrr.at[d], xr_s.at[d], xr_r.at[d], xdev(d))

    def fold_s(d):
        def side():
            xs(d).wait_send()
            xs_in(d).wait_recv()
            for k in range(9):
                a = 7 + 41 * d + k
                z[a, pl.ds(sc, STRIP), :] = z[a, pl.ds(sc, STRIP), :] + xrs[d, k]
        on_side(d, side)

    def fold_r(d):
        def side():
            xr(d).wait_send()
            xr_in(d).wait_recv()
            for k in range(9):
                a = 7 + 41 * d + k
                z[a, pl.ds(gc, REST), :] = z[a, pl.ds(gc, REST), :] + xrr[d, k]
        on_side(d, side)

    def no_row_s(d):
        z[7 + 49 * d, pl.ds(sc, STRIP), :] = jnp.zeros((STRIP, RHS), F32)

    def no_row_r(d):
        z[7 + 49 * d, pl.ds(gc, REST), :] = jnp.zeros((REST, RHS), F32)

    def sweep(s, carry):
        @pl.when(s == 0)
        def _():
            for i in range(4):
                load_s(i).wait()
        dot_s(STRIP)
        send_y(0)
        dot_s(32)
        send_y(1)

        def ends_s(i, c):
            d = jnp.where(i == 0, first, 1 - first)
            dot_s(TILE * d)
            on_side(d, lambda: xs(d).start())
            off_side(d, lambda: no_row_s(d))
            return c
        lax.fori_loop(0, 2, ends_s, 0)

        def ends_r(i, c):
            d = jnp.where(i == 0, first, 1 - first)
            pl.when(s == 0)(lambda: load_r(3 * d).wait())
            dot_r(TILE * d)
            on_side(d, lambda: xr(d).start())
            off_side(d, lambda: no_row_r(d))
            fold_s(1 - d)
            send_y_side(1 - d)
            return c
        lax.fori_loop(0, 2, ends_r, 0)
        send_y(2)

        def mid_r(i, c):
            pl.when(s == 0)(lambda: load_r(i).wait())
            dot_r(STRIP * i)
            return c
        lax.fori_loop(1, 3, mid_r, 0)
        pl.when(s == 0)(lambda: cp_u.wait())
        recv_y(0)
        update(22, MG, cd, STRIP, om, True)
        send_ry_early()
        recv_y(1)

        def ends_u(i, c):
            d = jnp.where(i == 0, 1 - first, first)
            fold_r(d)
            update(MG + 39 * d, 9, ci, 32, om, True)
            recv_y_side(d)
            update(MG + 34 * d, 14, cd, STRIP, om, True)
            send_ry_side(d)
            send_rx(d)
            return c
        lax.fori_loop(0, 2, ends_u, 0)
        update(17, 30, ci, 32, om, True)
        recv_y(2)
        update(30, 12, cd, STRIP, om, True)
        send_ry_mid()
        recv_r()
        for j in range(3):
            yz_mid(j).wait_send()
        for d in SIDES:
            yz_side(d).wait_send()
        return carry

    lax.fori_loop(0, SWEEPS - 1, sweep, 0)

    def fy(j, p0, n):
        return remote(fys.at[pl.ds(p0, n)], fyr_.at[pl.ds(p0, n)], fy_s.at[j], fy_r.at[j], ydev)

    def send_fy(j, p0, n):
        for q in range(n):
            a = MG + 2 * (p0 + q)
            fys[p0 + q] = jnp.concatenate([z[a, pl.ds(hc, MG), :], z[a + 1, pl.ds(hc, MG), :]], axis=0).astype(BF16)
        fy(j, p0, n).start()

    def fxsd(d):
        return remote(fxs.at[d], fxsr.at[1 - d], fx_s.at[d], fx_r.at[1 - d], xdev(d))

    def fxsd_in(d):
        return remote(fxs.at[d], fxsr.at[d], fx_s.at[d], fx_r.at[d], xdev(d))

    def fxrd(d):
        return remote(fxr.at[d], fxrr.at[1 - d], fx_s.at[2 + d], fx_r.at[3 - d], xdev(d))

    def fxrd_in(d):
        return remote(fxr.at[d], fxrr.at[d], fx_s.at[2 + d], fx_r.at[2 + d], xdev(d))

    def last_s(d):
        for i in range(MG):
            fxs[d, i] = z[END * d + i, pl.ds(sc, STRIP), :].astype(BF16)
        fxsd(d).start()

    def last_r(d):
        for i in range(4):
            a = END * d + 2 * i
            fxr[d, i] = jnp.concatenate([z[a, pl.ds(gc, REST), :], z[a + 1, pl.ds(gc, REST), :]], axis=0).astype(BF16)
        fxrd(d).start()

    def last_fold_s(d):
        fxsd_in(d).wait_recv()
        for i in range(MG):
            a = MG + REST * d + i
            z[a, pl.ds(sc, STRIP), :] = z[a, pl.ds(sc, STRIP), :] + fxsr[d, i].astype(F32)

    def last_fold_r(d):
        fxrd_in(d).wait_recv()
        for i in range(4):
            a = MG + REST * d + 2 * i
            v = fxrr[d, i].astype(F32)
            z[a, pl.ds(gc, REST), :] = z[a, pl.ds(gc, REST), :] + v[0:REST]
            z[a + 1, pl.ds(gc, REST), :] = z[a + 1, pl.ds(gc, REST), :] + v[REST:80]

    def last_y(j, p0, n):
        fy(j, p0, n).wait_recv()

        def body(i, c):
            v = fyr_[p0 + i].astype(F32)
            a = MG + 2 * (p0 + i)
            z[a, pl.ds(mc, MG), :] = z[a, pl.ds(mc, MG), :] + v[0:MG]
            z[a + 1, pl.ds(mc, MG), :] = z[a + 1, pl.ds(mc, MG), :] + v[MG:STRIP]
            return c
        lax.fori_loop(0, n, body, 0)

    def add_u(a0, rows):
        def body(i, c):
            u[a0 - MG + i] = u[a0 - MG + i] + om * z[a0 + i, MG:END, :]
            return c
        lax.fori_loop(0, rows, body, 0)

    for j in SIDES:
        dot_s(STRIP + STRIP * j)
        send_fy(j, *FCHUNKS[j])

    def last_ends_s(i, c):
        d = jnp.where(i == 0, first, 1 - first)
        dot_s(TILE * d)
        on_side(d, lambda: last_s(d))
        return c
    lax.fori_loop(0, 2, last_ends_s, 0)

    def last_ends_r(i, c):
        d = jnp.where(i == 0, first, 1 - first)
        dot_r(TILE * d)
        on_side(d, lambda: last_r(d))
        on_side(1 - d, lambda: last_fold_s(1 - d))
        send_fy(3 - d, 20 * (1 - d), 4)
        return c
    lax.fori_loop(0, 2, last_ends_r, 0)
    lax.fori_loop(1, 3, lambda i, c: (dot_r(STRIP * i), c)[1], 0)
    for j in SIDES:
        last_y(j, *FCHUNKS[j])
    add_u(STRIP, 32)
    for d in (order[1], order[0]):
        on_side(d, lambda d=d: last_fold_r(d))
        last_y(2 + d, 20 * d, 4)
        add_u(MG + REST * d, MG)
    for j in SIDES:
        fy(j, *FCHUNKS[j]).wait_send()
        fy(2 + j, 20 * j, 4).wait_send()

        def sent(j=j):
            fxsd(j).wait_send()
            fxrd(j).wait_send()
        on_side(j, sent)


def solution(mesh):
    def local_step(forcing, u_init, diffusivity, local_solve, relax_omega):
        any_spec = pl.BlockSpec(memory_space=pltpu.HBM)
        dma = pltpu.SemaphoreType.DMA
        return pl.pallas_call(
            kernel,
            out_shape=jax.ShapeDtypeStruct((TILE, TILE, RHS), F32),
            in_specs=[pl.BlockSpec(memory_space=pltpu.SMEM), any_spec, any_spec,
                      pl.BlockSpec(memory_space=pltpu.VMEM), any_spec],
            out_specs=pl.BlockSpec(memory_space=pltpu.VMEM),
            scratch_shapes=[
                pltpu.VMEM((EXT, STRIP, WIN), BF16),
                pltpu.VMEM((EXT, REST, WIN), BF16),
                pltpu.VMEM((EXT, EXT, RHS), BF16),
                pltpu.VMEM((EXT, EXT, RHS), F32),
                pltpu.VMEM((EXT, EXT, RHS), F32),
                pltpu.VMEM((49, EXT, 128), F32),
                pltpu.VMEM((TILE, EXT, 128), F32),
                pltpu.VMEM((3, TILE, TILE), F32),
                pltpu.VMEM((128, 128), F32),
                pltpu.VMEM((YLEN, MG, RHS), F32),
                pltpu.VMEM((YLEN, MG, RHS), F32),
                pltpu.VMEM((2, 9, STRIP, RHS), F32),
                pltpu.VMEM((2, 9, REST, RHS), F32),
                pltpu.VMEM((24, STRIP, RHS), BF16),
                pltpu.VMEM((24, STRIP, RHS), BF16),
                pltpu.VMEM((2, MG, TILE, RHS), BF16),
                pltpu.VMEM((2, MG, TILE, RHS), BF16),
                pltpu.VMEM((2, 4, STRIP, RHS), BF16),
                pltpu.VMEM((2, 4, STRIP, RHS), BF16),
                pltpu.VMEM((6, MG, RHS), F32),
                pltpu.VMEM((6, MG, RHS), F32),
                pltpu.VMEM((6, MG, RHS), F32),
                pltpu.VMEM((6, MG, RHS), F32),
                pltpu.VMEM((24, STRIP, RHS), BF16),
                pltpu.VMEM((24, STRIP, RHS), BF16),
                pltpu.VMEM((2, MG, STRIP, RHS), BF16),
                pltpu.VMEM((2, MG, STRIP, RHS), BF16),
                pltpu.VMEM((2, 4, 80, RHS), BF16),
                pltpu.VMEM((2, 4, 80, RHS), BF16),
                dma((5,)), dma((5,)), dma((2,)), dma((2,)), dma((2,)), dma((2,)),
                dma((4,)), dma((4,)), dma((2,)), dma((2,)), dma((2,)), dma((2,)),
                dma((7,)), dma((7,)), dma((4,)), dma((4,)), dma((4,)), dma((4,)), dma((4,)), dma((MG,)),
            ],
            compiler_params=pltpu.CompilerParams(
                collective_id=0, has_side_effects=True, vmem_limit_bytes=54_000_000),
            name="schwarz",
        )(relax_omega.reshape(1), forcing, u_init, diffusivity,
          local_solve.reshape(EXT, EXT, WIN))

    field_spec = P('row', 'col', None)
    return jax.shard_map(local_step, mesh=mesh,
                         in_specs=(field_spec, field_spec, P('row', 'col'), P('row', 'col', None, None), P()),
                         out_specs=field_spec, check_vma=False)
```

```python
import functools

import jax
import jax.numpy as jnp
from jax import lax
from jax.experimental import pallas as pl
from jax.experimental.pallas import tpu as pltpu
from jax.sharding import PartitionSpec as P

SWEEPS = 4
TILE = 48
EXT = 64
WIN = EXT * EXT
RHS = 256
MG = 8
STRIP = 16
REST = 40
END = 56
END_ROWS = 640
LATE = 768
LANES = 128
GROUP = 1024
SIDES = (0, 1)
F32 = jnp.float32
BF16 = jnp.bfloat16
MESH = pl.DeviceIdType.MESH

CHUNKS = ((16, 16, 0), (40, 8, 18), (32, 8, 27))
SIDE_OFF = 36
YLEN = 56
RMID = (11, 6)
REARLY = (7, 4)
FCHUNKS = ((4, MG), (12, MG))

def kernel(omega, f_hbm, u_hbm, kown, m_hbm, u,
           ms, mr, w, z, r, wx, wy, krecv, kfull,
           ys, yr, xrs, xrr, rsy, rry, rsx, rrx, rrd, rdb, ues, uer, pcs, pcr,
           fys, fyr_, fxs, fxsr, fxr, fxrr, msl, wl, psel,
           yz_s, yz_r, xs_s, xs_r, xr_s, xr_r, ry_s, ry_r, rx_s, rx_r, rd_s, rd_r,
           ie_s, ie_r, fy_s, fy_r, fx_s, fx_r, lsem, msem):
    col = lax.axis_index("col")
    row = lax.axis_index("row")
    has_up = row > 0
    has_dn = row < 3
    ydev = (1 - col, row)
    has = (has_up, has_dn)
    first = jnp.where(row < 2, 1, 0)
    order = (first, 1 - first)

    def xdev(d):
        return (col, row - 1 + 2 * d)

    def ddev(d):
        return (1 - col, row - 1 + 2 * d)

    def on_side(d, fn):
        there = jnp.where(d == 0, row, 3 - row) > 0
        pl.when(there)(fn)

    def off_side(d, fn):
        there = jnp.where(d == 0, row, 3 - row) > 0
        pl.when(jnp.logical_not(there))(fn)

    hc = pl.multiple_of(END - END * col, MG)
    mc = pl.multiple_of(TILE - REST * col, MG)
    oc = pl.multiple_of(END * col, MG)
    sc = pl.multiple_of(TILE - TILE * col, STRIP)
    rc = pl.multiple_of(STRIP * col, STRIP)
    gc = pl.multiple_of(MG + MG * col, MG)
    cd = pl.multiple_of(REST - 32 * col, MG)
    ci = pl.multiple_of(MG + STRIP * col, MG)
    es = 55 - 47 * col
    er = END - 49 * col
    face = END - TILE * col

    def remote(src, dst, ss, rs, dev):
        return pltpu.make_async_remote_copy(src_ref=src, dst_ref=dst, send_sem=ss, recv_sem=rs,
                                            device_id=dev, device_id_type=MESH)

    inner = (pl.ds(MG, TILE), pl.ds(MG, TILE))
    cp_z = pltpu.make_async_copy(u_hbm, z.at[inner], lsem.at[1])
    cp_r = pltpu.make_async_copy(f_hbm, r.at[inner], lsem.at[2])
    cp_u = pltpu.make_async_copy(u_hbm, u, lsem.at[3])
    for cp in (cp_z, cp_r):
        cp.start()

    def load_s(i):
        return pltpu.make_async_copy(m_hbm.at[pl.ds(STRIP * i, STRIP), pl.ds(sc, STRIP)], ms.at[pl.ds(STRIP * i, STRIP)], msem.at[i])

    def load_r(i):
        return pltpu.make_async_copy(m_hbm.at[pl.ds(STRIP * i, STRIP), pl.ds(gc, REST)], mr.at[pl.ds(STRIP * i, STRIP)], msem.at[4 + i])

    for a in (7, END):
        z[a] = jnp.zeros((EXT, RHS), F32)
    bar = pltpu.get_barrier_semaphore()
    pl.semaphore_signal(bar, inc=1, device_id=ydev, device_id_type=MESH)
    for d in SIDES:
        def greet(d=d):
            pl.semaphore_signal(bar, inc=1, device_id=xdev(d), device_id_type=MESH)
            pl.semaphore_signal(bar, inc=1, device_id=ddev(d), device_id_type=MESH)
        on_side(d, greet)
    r[7] = jnp.zeros((EXT, RHS), F32)
    r[END] = jnp.zeros((EXT, RHS), F32)
    for ref in (z, r):
        ref[0:7] = jnp.zeros((7, EXT, RHS), F32)
        ref[57:EXT] = jnp.zeros((7, EXT, RHS), F32)
        ref[MG:END, 0:MG] = jnp.zeros((TILE, MG, RHS), F32)
        ref[MG:END, END:EXT] = jnp.zeros((TILE, MG, RHS), F32)

    kfull[...] = jnp.zeros_like(kfull)
    kfull[MG:END, MG:END] = kown[...]
    kt = kfull[...].T
    prev = jnp.broadcast_to(kt[0:EXT, 7:MG], (EXT, LANES))
    for a in range(MG, 57):
        here = jnp.broadcast_to(kt[0:EXT, a:a + 1], (EXT, LANES))
        wx[a - MG] = 0.5 * (prev + here)
        if a < END:
            wy[a - MG] = 0.5 * (pltpu.roll(here, 1, 0) + here)
        prev = here
    for k in range(TILE):
        wy[k, pl.ds(face, 1), :] = jnp.zeros((1, LANES), F32)
    n_sides = has_up.astype(jnp.int32) + has_dn.astype(jnp.int32)
    pl.semaphore_wait(bar, 1 + 2 * n_sides)

    k_y = remote(kown, krecv.at[2], ie_s.at[0], ie_r.at[0], ydev)
    k_y.start()
    k_x = [remote(kown, krecv.at[1 - d], ie_s.at[1 + d], ie_r.at[2 - d], xdev(d)) for d in SIDES]
    u_x = [remote(z.at[MG if d == 0 else 55, pl.ds(MG, TILE)], z.at[END if d == 0 else 7, pl.ds(MG, TILE)],
                  ie_s.at[3 + d], ie_r.at[4 - d], xdev(d)) for d in SIDES]
    k_in = [remote(kown, krecv.at[d], ie_s.at[1 + d], ie_r.at[1 + d], xdev(d)) for d in SIDES]
    u_in = [remote(z.at[MG if d == 0 else 55, pl.ds(MG, TILE)], z.at[7 if d == 0 else END, pl.ds(MG, TILE)],
                   ie_s.at[3 + d], ie_r.at[3 + d], xdev(d)) for d in SIDES]
    for d in SIDES:
        on_side(d, lambda d=d: k_x[d].start())
    cp_z.wait()
    for k in range(TILE):
        ues[k // MG, k % MG, :] = z[MG + k, pl.ds(es, 1), :][0]
    u_y = remote(ues, uer, ie_s.at[5], ie_r.at[5], ydev)
    u_y.start()
    for d in SIDES:
        on_side(d, lambda d=d: u_x[d].start())
    cp_r.wait()
    for i in range(4):
        load_s(i).start()
    load_r(3 * first).start()
    load_r(3 - 3 * first).start()
    for i in (1, 2):
        load_r(i).start()
    cp_u.start()

    def both(v):
        return jnp.concatenate([v, v], axis=1)

    def update(a0, rows, c0, n, om, add_u):
        def body(i, carry):
            a = a0 + i
            wide = z[a, pl.ds(c0 - MG, n + STRIP), :]
            fy = both(wy[a - MG, pl.ds(c0 - MG, n + STRIP), :]) * (wide - pltpu.roll(wide, 1, 0))
            fyr = pltpu.roll(fy, n + 15, 0)
            mid = wide[MG:MG + n]
            az = (both(wx[a - MG, pl.ds(c0, n), :]) * (mid - z[a - 1, pl.ds(c0, n), :])
                  + both(wx[a - 7, pl.ds(c0, n), :]) * (mid - z[a + 1, pl.ds(c0, n), :])
                  + fy[MG:MG + n] - fyr[MG:MG + n])
            r[a, pl.ds(c0, n), :] = r[a, pl.ds(c0, n), :] - om * az
            if add_u:
                u[a - MG, pl.ds(c0 - MG, n), :] = u[a - MG, pl.ds(c0 - MG, n), :] + om * mid
            return carry
        lax.fori_loop(0, rows, body, 0)

    lo, hi = MG * EXT, END * EXT

    def pack_late(lhs, dst, row0, rows):
        for g in range(3):
            cols = lhs[:, lo + GROUP * g:lo + GROUP * (g + 1)]
            dst[pl.ds(row0, rows), RHS * g:RHS * (g + 1)] = jnp.dot(
                cols, psel[...], preferred_element_type=F32).astype(BF16)

    def pack_matrix():
        k = lax.broadcasted_iota(jnp.int32, (GROUP, RHS), 0)
        n = lax.broadcasted_iota(jnp.int32, (GROUP, RHS), 1)
        hit = ((k >> 6) == (n >> 4)) & ((k & 63) == sc + (n & 15))
        psel[...] = jnp.where(hit, 1.0, 0.0).astype(BF16)

        def strip(i, c):
            load_s(i).wait()
            pack_late(ms[pl.ds(STRIP * i, STRIP)].reshape(RHS, WIN), msl, pl.multiple_of(RHS * i, RHS), RHS)
            return c
        lax.fori_loop(0, 4, strip, 0)

    def early_s():
        w[MG:END, pl.ds(sc, STRIP), :] = jnp.zeros((TILE, STRIP, RHS), BF16)

        def strip(i, c):
            lhs = ms[pl.ds(STRIP * i, STRIP)].reshape(RHS, WIN)[:, lo:hi]
            z[pl.ds(STRIP * i, STRIP), pl.ds(sc, STRIP), :] = jnp.dot(
                lhs, w[MG:END].reshape(hi - lo, RHS), preferred_element_type=F32).reshape(STRIP, STRIP, RHS)
            return c
        lax.fori_loop(0, 4, strip, 0)

    def late(lhs, packed):
        cells = jnp.concatenate([w[0:MG].reshape(lo, RHS), w[END:EXT].reshape(lo, RHS),
                                 wl[...].reshape(LATE, RHS)], axis=0)
        return jnp.dot(jnp.concatenate([lhs[:, 0:lo], lhs[:, hi:WIN], packed], axis=1), cells,
                       preferred_element_type=F32)

    def dot_s(a0):
        part = late(ms[pl.ds(a0, STRIP)].reshape(RHS, WIN), msl[pl.ds(pl.multiple_of(a0 * STRIP, RHS), RHS), :])
        here = (pl.ds(a0, STRIP), pl.ds(sc, STRIP))
        z[here] = z[here] + part.reshape(STRIP, STRIP, RHS)

    def dot_r(a0):
        lhs = mr[pl.ds(a0, STRIP)].reshape(END_ROWS, WIN)
        z[pl.ds(a0, STRIP), pl.ds(gc, REST), :] = jnp.dot(
            lhs, w[...].reshape(WIN, RHS), preferred_element_type=F32).reshape(STRIP, REST, RHS)

    def ry(p0, n, j):
        return remote(rsy.at[pl.ds(p0, n)], rry.at[pl.ds(p0, n)], ry_s.at[j], ry_r.at[j], ydev)

    def ry_mid():
        return ry(*RMID, 2)

    def ry_early():
        return ry(*REARLY, 3)

    def ry_side(d):
        return ry(17 * d, 7, d)

    def rx(d):
        return remote(rsx.at[d], rrx.at[1 - d], rx_s.at[d], rx_r.at[1 - d], xdev(d))

    def rx_in(d):
        return remote(rsx.at[d], rrx.at[d], rx_s.at[d], rx_r.at[d], xdev(d))

    def rd(d):
        return remote(rsy.at[pl.ds(20 * d, 4)], rrd.at[1 - d], rd_s.at[d], rd_r.at[1 - d], ddev(d))

    def rd_forward(d):
        return remote(rry.at[pl.ds(20 * d, 4)], rrd.at[1 - d], rd_s.at[d], rd_r.at[1 - d], xdev(d))

    def same_chip(d):
        return lax.rem(row + d, 2) == 1

    def rd_in(d):
        return remote(rsy.at[pl.ds(20 * d, 4)], rrd.at[d], rd_s.at[d], rd_r.at[d], ddev(d))

    def pack_ry(p0, n):
        for q in range(n):
            a = MG + 2 * (p0 + q)
            rsy[p0 + q] = jnp.concatenate([r[a, pl.ds(mc, MG), :], r[a + 1, pl.ds(mc, MG), :]], axis=0).astype(BF16)

    def send_ry_side(d):
        pack_ry(17 * d, 7)
        on_side(d, lambda: pl.when(jnp.logical_not(same_chip(d)))(lambda: rd(d).start()))
        ry_side(d).start()

    def send_ry_mid():
        pack_ry(*RMID)
        ry_mid().start()

    def send_ry_early():
        pack_ry(*REARLY)
        ry_early().start()

    def send_rx(d):
        for i in range(MG):
            rsx[d, i] = r[MG + REST * d + i, MG:END, :].astype(BF16)
        on_side(d, lambda: rx(d).start())

    def to_w(a0, rows, c0, n):
        def body(i, carry):
            w[a0 + i, pl.ds(c0, n), :] = r[a0 + i, pl.ds(c0, n), :].astype(BF16)
            return carry
        lax.fori_loop(0, rows, body, 0)

    def to_strip(a):
        cells = r[a, pl.ds(sc, STRIP), :].astype(BF16)
        w[a, pl.ds(sc, STRIP), :] = cells
        wl[a - MG] = cells

    def unpack_ry(p0, n):
        def body(i, carry):
            v = rry[p0 + i].astype(F32)
            a = MG + 2 * (p0 + i)
            r[a, pl.ds(hc, MG), :] = v[0:MG]
            r[a + 1, pl.ds(hc, MG), :] = v[MG:STRIP]
            to_strip(a)
            to_strip(a + 1)
            return carry
        lax.fori_loop(0, n, body, 0)

    def recv_side(d):
        rx_in(d).wait_recv()
        rd_in(d).wait_recv()
        for i in range(MG):
            r[END * d + i, MG:END, :] = rrx[d, i].astype(F32)
        for q in range(4):
            v = rrd[d, q].astype(F32)
            r[END * d + 2 * q, pl.ds(hc, MG), :] = v[0:MG]
            r[END * d + 2 * q + 1, pl.ds(hc, MG), :] = v[MG:STRIP]
        to_w(END * d, MG, 0, EXT)

    def recv_r():
        to_w(MG, TILE, rc, TILE)
        early_s()
        ry_early().wait_recv()
        unpack_ry(*REARLY)
        for d in (order[1], order[0]):
            ry_side(d).wait_recv()
            on_side(d, lambda d=d: pl.when(same_chip(d))(lambda: rd_forward(d).start()))
            unpack_ry(17 * d, 7)
        for d in (order[1], order[0]):
            on_side(d, lambda d=d: recv_side(d))
        ry_mid().wait_recv()
        unpack_ry(*RMID)
        ry_mid().wait_send()
        ry_early().wait_send()
        for d in SIDES:
            ry_side(d).wait_send()

            def sent(d=d):
                rx(d).wait_send()
                rd(d).wait_send()
            on_side(d, sent)

    update(9, 46, cd, STRIP, 1.0, False)
    pack_ry(1, 22)
    ry(1, 22, 2).start()
    update(9, 46, ci, 32, 1.0, False)
    for d in SIDES:
        def edge(d=d):
            k_in[d].wait_recv()
            kfull[7 + 49 * d:MG + 49 * d, MG:END] = krecv[d, 47 - 47 * d:TILE - 47 * d, :]
            u_in[d].wait_recv()
        on_side(d, edge)
    kt = kfull[...].T
    for d in SIDES:
        a = MG + TILE * d
        wx[TILE * d] = 0.5 * (jnp.broadcast_to(kt[0:EXT, a - 1:a], (EXT, LANES))
                              + jnp.broadcast_to(kt[0:EXT, a:a + 1], (EXT, LANES)))
    for d in SIDES:
        update(MG + 47 * d, 1, cd, STRIP, 1.0, False)
        pack_ry(23 * d, 1)
        ry(23 * d, 1, d).start()
    for k in range(TILE):
        pcs[k // MG, k % MG, :] = r[MG + k, pl.ds(es, 1), :][0]
    p_y = remote(pcs, pcr, ie_s.at[6], ie_r.at[6], ydev)
    p_y.start()
    for d in SIDES:
        update(MG + 47 * d, 1, ci, 32, 1.0, False)
    k_y.wait_recv()
    u_y.wait_recv()

    def lane(ref, i):
        return jnp.broadcast_to(ref[:, i:i + 1], (TILE, LANES))

    k_nb = krecv[2]
    k_me = kown[...]
    wf = 0.5 * (jnp.where(col == 0, lane(k_me, 47), lane(k_me, 0))
                + jnp.where(col == 0, lane(k_nb, 0), lane(k_nb, 47)))
    flux = both(wf) * (ues[...].reshape(TILE, RHS) - uer[...].reshape(TILE, RHS))
    mine = pcs[...].reshape(TILE, RHS) - flux
    for k in range(TILE):
        wy[k, pl.ds(face, 1), :] = wf[k:k + 1]
        r[MG + k, pl.ds(es, 1), :] = mine[k:k + 1]

    def corner(d):
        return remote(rdb.at[d], rrd.at[1 - d], rd_s.at[d], rd_r.at[1 - d], ddev(d))

    for d in SIDES:
        for q in range(4):
            a = MG + REST * d + 2 * q
            rdb[d, q] = jnp.concatenate([r[a, pl.ds(mc, MG), :], r[a + 1, pl.ds(mc, MG), :]], axis=0).astype(BF16)
        on_side(d, lambda d=d: corner(d).start())
        send_rx(d)
        off_side(d, lambda d=d: to_w(END * d, MG, 0, EXT))
    to_w(MG, TILE, rc, TILE)
    pack_matrix()
    for d in SIDES:
        on_side(d, lambda d=d: u_x[d].wait_send())
    early_s()
    for d in SIDES:
        ry(23 * d, 1, d).wait_recv()
        unpack_ry(23 * d, 1)
    ry(1, 22, 2).wait_recv()
    unpack_ry(1, 22)
    p_y.wait_recv()
    theirs = pcr[...].reshape(TILE, RHS) + flux
    for k in range(TILE):
        r[MG + k, pl.ds(er, 1), :] = theirs[k:k + 1]

    def strip_row(i, c):
        to_strip(MG + i)
        return c
    lax.fori_loop(0, TILE, strip_row, 0)
    for d in (order[1], order[0]):
        on_side(d, lambda d=d: recv_side(d))
    ry(1, 22, 2).wait_send()
    for d in SIDES:
        ry(23 * d, 1, d).wait_send()

        def sent(d=d):
            k_x[d].wait_send()
            rx(d).wait_send()
            corner(d).wait_send()
        on_side(d, sent)
    k_y.wait_send()
    u_y.wait_send()
    p_y.wait_send()

    om = omega[0]

    def yz(j, off, length):
        return remote(ys.at[pl.ds(off, length)], yr.at[pl.ds(off, length)], yz_s.at[j], yz_r.at[j], ydev)

    def yz_mid(j):
        return yz(j, CHUNKS[j][2], CHUNKS[j][1] + pl.cdiv(CHUNKS[j][1], MG))

    def yz_side(d):
        return yz(3 + d, SIDE_OFF + 10 * d, 10)

    def pack_y(a0, n, off, e0, ne):
        for k in range(n):
            ys[off + k] = z[a0 + k, pl.ds(hc, MG), :]
        for k in range(ne):
            ys[off + n + k // MG, k % MG, :] = z[e0 + k, pl.ds(es, 1), :][0]

    def add_y(a0, n, off, e0, ne):
        for k in range(n):
            z[a0 + k, pl.ds(mc, MG), :] = z[a0 + k, pl.ds(mc, MG), :] + yr[off + k]
        for k in range(ne):
            z[e0 + k, pl.ds(er, 1), :] = z[e0 + k, pl.ds(er, 1), :] + yr[off + n + k // MG, k % MG, :][None]

    def side_rows(d):
        return 7 + 41 * d, 9, SIDE_OFF + 10 * d, MG + REST * d, MG

    def send_y(j):
        pack_y(*CHUNKS[j], *CHUNKS[j][:2])
        yz_mid(j).start()

    def send_y_side(d):
        pack_y(*side_rows(d))
        yz_side(d).start()

    def recv_y(j):
        yz_mid(j).wait_recv()
        add_y(*CHUNKS[j], *CHUNKS[j][:2])

    def recv_y_side(d):
        yz_side(d).wait_recv()
        add_y(*side_rows(d))

    def xs(d):
        return remote(z.at[pl.ds(55 * d, 9), pl.ds(sc, STRIP)], xrs.at[1 - d], xs_s.at[d], xs_r.at[1 - d], xdev(d))

    def xs_in(d):
        return remote(z.at[pl.ds(55 * d, 9), pl.ds(sc, STRIP)], xrs.at[d], xs_s.at[d], xs_r.at[d], xdev(d))

    def xr(d):
        return remote(z.at[pl.ds(55 * d, 9), pl.ds(gc, REST)], xrr.at[1 - d], xr_s.at[d], xr_r.at[1 - d], xdev(d))

    def xr_in(d):
        return remote(z.at[pl.ds(55 * d, 9), pl.ds(gc, REST)], xrr.at[d], xr_s.at[d], xr_r.at[d], xdev(d))

    def fold_s(d):
        def side():
            xs(d).wait_send()
            xs_in(d).wait_recv()
            for k in range(9):
                a = 7 + 41 * d + k
                z[a, pl.ds(sc, STRIP), :] = z[a, pl.ds(sc, STRIP), :] + xrs[d, k]
        on_side(d, side)

    def fold_r(d):
        def side():
            xr(d).wait_send()
            xr_in(d).wait_recv()
            for k in range(9):
                a = 7 + 41 * d + k
                z[a, pl.ds(gc, REST), :] = z[a, pl.ds(gc, REST), :] + xrr[d, k]
        on_side(d, side)

    def no_row_s(d):
        z[7 + 49 * d, pl.ds(sc, STRIP), :] = jnp.zeros((STRIP, RHS), F32)

    def no_row_r(d):
        z[7 + 49 * d, pl.ds(gc, REST), :] = jnp.zeros((REST, RHS), F32)

    def sweep(s, carry):
        dot_s(STRIP)
        send_y(0)
        dot_s(32)
        send_y(1)

        def ends_s(i, c):
            d = jnp.where(i == 0, first, 1 - first)
            dot_s(TILE * d)
            on_side(d, lambda: xs(d).start())
            off_side(d, lambda: no_row_s(d))
            return c
        lax.fori_loop(0, 2, ends_s, 0)

        def ends_r(i, c):
            d = jnp.where(i == 0, first, 1 - first)
            pl.when(s == 0)(lambda: load_r(3 * d).wait())
            dot_r(TILE * d)
            on_side(d, lambda: xr(d).start())
            off_side(d, lambda: no_row_r(d))
            fold_s(1 - d)
            send_y_side(1 - d)
            return c
        lax.fori_loop(0, 2, ends_r, 0)
        send_y(2)

        def mid_r(i, c):
            pl.when(s == 0)(lambda: load_r(i).wait())
            dot_r(STRIP * i)
            return c
        lax.fori_loop(1, 3, mid_r, 0)
        pl.when(s == 0)(lambda: cp_u.wait())
        recv_y(0)
        update(22, MG, cd, STRIP, om, True)
        send_ry_early()
        recv_y(1)

        def ends_u(i, c):
            d = jnp.where(i == 0, 1 - first, first)
            fold_r(d)
            update(MG + 39 * d, 9, ci, 32, om, True)
            recv_y_side(d)
            update(MG + 34 * d, 14, cd, STRIP, om, True)
            send_ry_side(d)
            send_rx(d)
            return c
        lax.fori_loop(0, 2, ends_u, 0)
        update(17, 30, ci, 32, om, True)
        recv_y(2)
        update(30, 12, cd, STRIP, om, True)
        send_ry_mid()
        recv_r()
        for j in range(3):
            yz_mid(j).wait_send()
        for d in SIDES:
            yz_side(d).wait_send()
        return carry

    lax.fori_loop(0, SWEEPS - 1, sweep, 0)

    def fy(j, p0, n):
        return remote(fys.at[pl.ds(p0, n)], fyr_.at[pl.ds(p0, n)], fy_s.at[j], fy_r.at[j], ydev)

    def send_fy(j, p0, n):
        for q in range(n):
            a = MG + 2 * (p0 + q)
            fys[p0 + q] = jnp.concatenate([z[a, pl.ds(hc, MG), :], z[a + 1, pl.ds(hc, MG), :]], axis=0).astype(BF16)
        fy(j, p0, n).start()

    def fxsd(d):
        return remote(fxs.at[d], fxsr.at[1 - d], fx_s.at[d], fx_r.at[1 - d], xdev(d))

    def fxsd_in(d):
        return remote(fxs.at[d], fxsr.at[d], fx_s.at[d], fx_r.at[d], xdev(d))

    def fxrd(d):
        return remote(fxr.at[d], fxrr.at[1 - d], fx_s.at[2 + d], fx_r.at[3 - d], xdev(d))

    def fxrd_in(d):
        return remote(fxr.at[d], fxrr.at[d], fx_s.at[2 + d], fx_r.at[2 + d], xdev(d))

    def last_s(d):
        for i in range(MG):
            fxs[d, i] = z[END * d + i, pl.ds(sc, STRIP), :].astype(BF16)
        fxsd(d).start()

    def last_r(d):
        for i in range(4):
            a = END * d + 2 * i
            fxr[d, i] = jnp.concatenate([z[a, pl.ds(gc, REST), :], z[a + 1, pl.ds(gc, REST), :]], axis=0).astype(BF16)
        fxrd(d).start()

    def last_fold_s(d):
        fxsd_in(d).wait_recv()
        for i in range(MG):
            a = MG + REST * d + i
            z[a, pl.ds(sc, STRIP), :] = z[a, pl.ds(sc, STRIP), :] + fxsr[d, i].astype(F32)

    def last_fold_r(d):
        fxrd_in(d).wait_recv()
        for i in range(4):
            a = MG + REST * d + 2 * i
            v = fxrr[d, i].astype(F32)
            z[a, pl.ds(gc, REST), :] = z[a, pl.ds(gc, REST), :] + v[0:REST]
            z[a + 1, pl.ds(gc, REST), :] = z[a + 1, pl.ds(gc, REST), :] + v[REST:80]

    def last_y(j, p0, n):
        fy(j, p0, n).wait_recv()

        def body(i, c):
            v = fyr_[p0 + i].astype(F32)
            a = MG + 2 * (p0 + i)
            z[a, pl.ds(mc, MG), :] = z[a, pl.ds(mc, MG), :] + v[0:MG]
            z[a + 1, pl.ds(mc, MG), :] = z[a + 1, pl.ds(mc, MG), :] + v[MG:STRIP]
            return c
        lax.fori_loop(0, n, body, 0)

    def add_u(a0, rows):
        def body(i, c):
            u[a0 - MG + i] = u[a0 - MG + i] + om * z[a0 + i, MG:END, :]
            return c
        lax.fori_loop(0, rows, body, 0)

    for j in SIDES:
        dot_s(STRIP + STRIP * j)
        send_fy(j, *FCHUNKS[j])

    def last_ends_s(i, c):
        d = jnp.where(i == 0, first, 1 - first)
        dot_s(TILE * d)
        on_side(d, lambda: last_s(d))
        return c
    lax.fori_loop(0, 2, last_ends_s, 0)

    def last_ends_r(i, c):
        d = jnp.where(i == 0, first, 1 - first)
        dot_r(TILE * d)
        on_side(d, lambda: last_r(d))
        on_side(1 - d, lambda: last_fold_s(1 - d))
        send_fy(3 - d, 20 * (1 - d), 4)
        return c
    lax.fori_loop(0, 2, last_ends_r, 0)
    lax.fori_loop(1, 3, lambda i, c: (dot_r(STRIP * i), c)[1], 0)
    for j in SIDES:
        last_y(j, *FCHUNKS[j])
    add_u(STRIP, 32)
    for d in (order[1], order[0]):
        on_side(d, lambda d=d: last_fold_r(d))
        last_y(2 + d, 20 * d, 4)
        add_u(MG + REST * d, MG)
    for j in SIDES:
        fy(j, *FCHUNKS[j]).wait_send()
        fy(2 + j, 20 * j, 4).wait_send()

        def sent(j=j):
            fxsd(j).wait_send()
            fxrd(j).wait_send()
        on_side(j, sent)


def solution(mesh):
    def local_step(forcing, u_init, diffusivity, local_solve, relax_omega):
        any_spec = pl.BlockSpec(memory_space=pltpu.HBM)
        dma = pltpu.SemaphoreType.DMA
        return pl.pallas_call(
            kernel,
            out_shape=jax.ShapeDtypeStruct((TILE, TILE, RHS), F32),
            in_specs=[pl.BlockSpec(memory_space=pltpu.SMEM), any_spec, any_spec,
                      pl.BlockSpec(memory_space=pltpu.VMEM), any_spec],
            out_specs=pl.BlockSpec(memory_space=pltpu.VMEM),
            scratch_shapes=[
                pltpu.VMEM((EXT, STRIP, WIN), BF16),
                pltpu.VMEM((EXT, REST, WIN), BF16),
                pltpu.VMEM((EXT, EXT, RHS), BF16),
                pltpu.VMEM((EXT, EXT, RHS), F32),
                pltpu.VMEM((EXT, EXT, RHS), F32),
                pltpu.VMEM((49, EXT, LANES), F32),
                pltpu.VMEM((TILE, EXT, LANES), F32),
                pltpu.VMEM((3, TILE, TILE), F32),
                pltpu.VMEM((LANES, LANES), F32),
                pltpu.VMEM((YLEN, MG, RHS), F32),
                pltpu.VMEM((YLEN, MG, RHS), F32),
                pltpu.VMEM((2, 9, STRIP, RHS), F32),
                pltpu.VMEM((2, 9, REST, RHS), F32),
                pltpu.VMEM((24, STRIP, RHS), BF16),
                pltpu.VMEM((24, STRIP, RHS), BF16),
                pltpu.VMEM((2, MG, TILE, RHS), BF16),
                pltpu.VMEM((2, MG, TILE, RHS), BF16),
                pltpu.VMEM((2, 4, STRIP, RHS), BF16),
                pltpu.VMEM((2, 4, STRIP, RHS), BF16),
                pltpu.VMEM((6, MG, RHS), F32),
                pltpu.VMEM((6, MG, RHS), F32),
                pltpu.VMEM((6, MG, RHS), F32),
                pltpu.VMEM((6, MG, RHS), F32),
                pltpu.VMEM((24, STRIP, RHS), BF16),
                pltpu.VMEM((24, STRIP, RHS), BF16),
                pltpu.VMEM((2, MG, STRIP, RHS), BF16),
                pltpu.VMEM((2, MG, STRIP, RHS), BF16),
                pltpu.VMEM((2, 4, 80, RHS), BF16),
                pltpu.VMEM((2, 4, 80, RHS), BF16),
                pltpu.VMEM((GROUP, LATE), BF16),
                pltpu.VMEM((TILE, STRIP, RHS), BF16),
                pltpu.VMEM((GROUP, RHS), BF16),
                dma((5,)), dma((5,)), dma((2,)), dma((2,)), dma((2,)), dma((2,)),
                dma((4,)), dma((4,)), dma((2,)), dma((2,)), dma((2,)), dma((2,)),
                dma((7,)), dma((7,)), dma((4,)), dma((4,)), dma((4,)), dma((4,)), dma((4,)), dma((MG,)),
            ],
            compiler_params=pltpu.CompilerParams(
                collective_id=0, has_side_effects=True, vmem_limit_bytes=53_000_000),
            name="schwarz",
        )(relax_omega.reshape(1), forcing, u_init, diffusivity,
          local_solve.reshape(EXT, EXT, WIN))

    field_spec = P('row', 'col', None)
    return jax.shard_map(local_step, mesh=mesh,
                         in_specs=(field_spec, field_spec, P('row', 'col'), P('row', 'col', None, None), P()),
                         out_specs=field_spec, check_vma=False)
```

```python
import functools

import jax
import jax.numpy as jnp
from jax import lax
from jax.experimental import pallas as pl
from jax.experimental.pallas import tpu as pltpu
from jax.sharding import PartitionSpec as P

SWEEPS = 4
TILE = 48
EXT = 64
WIN = EXT * EXT
RHS = 256
MG = 8
STRIP = 16
REST = 40
END = 56
END_ROWS = 640
LATE = 768
LANES = 128
GROUP = 1024
SIDES = (0, 1)
F32 = jnp.float32
BF16 = jnp.bfloat16
MESH = pl.DeviceIdType.MESH

CHUNKS = ((16, 16, 0), (40, 8, 18), (32, 8, 27))
SIDE_OFF = 36
YLEN = 56
RMID = (11, 6)
REARLY = (7, 4)
FCHUNKS = ((4, MG), (12, MG))

def kernel(omega, f_hbm, u_hbm, kap_hbm, m_hbm, u,
           ms, mr, w, z, r, wx, wy, kown, krecv, kfull,
           ys, yr, xrs, xrr, rsy, rry, rsx, rrx, rrd, rdb, ues, uer, pcs, pcr,
           fys, fyr_, fxs, fxsr, fxr, fxrr, msl, wl, psel,
           yz_s, yz_r, xs_s, xs_r, xr_s, xr_r, ry_s, ry_r, rx_s, rx_r, rd_s, rd_r,
           ie_s, ie_r, fy_s, fy_r, fx_s, fx_r, lsem, msem):
    col = lax.axis_index("col")
    row = lax.axis_index("row")
    has_up = row > 0
    has_dn = row < 3
    ydev = (1 - col, row)
    has = (has_up, has_dn)
    first = jnp.where(row < 2, 1, 0)
    order = (first, 1 - first)

    def xdev(d):
        return (col, row - 1 + 2 * d)

    def ddev(d):
        return (1 - col, row - 1 + 2 * d)

    def on_side(d, fn):
        there = jnp.where(d == 0, row, 3 - row) > 0
        pl.when(there)(fn)

    def off_side(d, fn):
        there = jnp.where(d == 0, row, 3 - row) > 0
        pl.when(jnp.logical_not(there))(fn)

    hc = pl.multiple_of(END - END * col, MG)
    mc = pl.multiple_of(TILE - REST * col, MG)
    oc = pl.multiple_of(END * col, MG)
    sc = pl.multiple_of(TILE - TILE * col, STRIP)
    rc = pl.multiple_of(STRIP * col, STRIP)
    gc = pl.multiple_of(MG + MG * col, MG)
    cd = pl.multiple_of(REST - 32 * col, MG)
    ci = pl.multiple_of(MG + STRIP * col, MG)
    es = 55 - 47 * col
    er = END - 49 * col
    face = END - TILE * col

    def remote(src, dst, ss, rs, dev):
        return pltpu.make_async_remote_copy(src_ref=src, dst_ref=dst, send_sem=ss, recv_sem=rs,
                                            device_id=dev, device_id_type=MESH)

    inner = (pl.ds(MG, TILE), pl.ds(MG, TILE))
    cp_z = pltpu.make_async_copy(u_hbm, z.at[inner], lsem.at[1])
    cp_r = pltpu.make_async_copy(f_hbm, r.at[inner], lsem.at[2])
    cp_u = pltpu.make_async_copy(u_hbm, u, lsem.at[3])
    cp_k = pltpu.make_async_copy(kap_hbm, kown, lsem.at[0])
    for cp in (cp_k, cp_z, cp_r):
        cp.start()

    def load_s(i):
        return pltpu.make_async_copy(m_hbm.at[pl.ds(STRIP * i, STRIP), pl.ds(sc, STRIP)], ms.at[pl.ds(STRIP * i, STRIP)], msem.at[i])

    def load_r(i):
        return pltpu.make_async_copy(m_hbm.at[pl.ds(STRIP * i, STRIP), pl.ds(gc, REST)], mr.at[pl.ds(STRIP * i, STRIP)], msem.at[4 + i])

    for a in (7, END):
        z[a] = jnp.zeros((EXT, RHS), F32)
    bar = pltpu.get_barrier_semaphore()
    pl.semaphore_signal(bar, inc=1, device_id=ydev, device_id_type=MESH)
    for d in SIDES:
        def greet(d=d):
            pl.semaphore_signal(bar, inc=1, device_id=xdev(d), device_id_type=MESH)
            pl.semaphore_signal(bar, inc=1, device_id=ddev(d), device_id_type=MESH)
        on_side(d, greet)
    r[7] = jnp.zeros((EXT, RHS), F32)
    r[END] = jnp.zeros((EXT, RHS), F32)
    for ref in (z, r):
        ref[0:7] = jnp.zeros((7, EXT, RHS), F32)
        ref[57:EXT] = jnp.zeros((7, EXT, RHS), F32)
        ref[MG:END, 0:MG] = jnp.zeros((TILE, MG, RHS), F32)
        ref[MG:END, END:EXT] = jnp.zeros((TILE, MG, RHS), F32)

    kfull[...] = jnp.zeros_like(kfull)
    cp_k.wait()
    kfull[MG:END, MG:END] = kown[...]
    kt = kfull[...].T
    prev = jnp.broadcast_to(kt[0:EXT, 7:MG], (EXT, LANES))
    for a in range(MG, 57):
        here = jnp.broadcast_to(kt[0:EXT, a:a + 1], (EXT, LANES))
        wx[a - MG] = 0.5 * (prev + here)
        if a < END:
            wy[a - MG] = 0.5 * (pltpu.roll(here, 1, 0) + here)
        prev = here
    for k in range(TILE):
        wy[k, pl.ds(face, 1), :] = jnp.zeros((1, LANES), F32)
    n_sides = has_up.astype(jnp.int32) + has_dn.astype(jnp.int32)
    pl.semaphore_wait(bar, 1 + 2 * n_sides)

    k_y = remote(kown, krecv.at[2], ie_s.at[0], ie_r.at[0], ydev)
    k_y.start()
    k_x = [remote(kown, krecv.at[1 - d], ie_s.at[1 + d], ie_r.at[2 - d], xdev(d)) for d in SIDES]
    u_x = [remote(z.at[MG if d == 0 else 55, pl.ds(MG, TILE)], z.at[END if d == 0 else 7, pl.ds(MG, TILE)],
                  ie_s.at[3 + d], ie_r.at[4 - d], xdev(d)) for d in SIDES]
    k_in = [remote(kown, krecv.at[d], ie_s.at[1 + d], ie_r.at[1 + d], xdev(d)) for d in SIDES]
    u_in = [remote(z.at[MG if d == 0 else 55, pl.ds(MG, TILE)], z.at[7 if d == 0 else END, pl.ds(MG, TILE)],
                   ie_s.at[3 + d], ie_r.at[3 + d], xdev(d)) for d in SIDES]
    for d in SIDES:
        on_side(d, lambda d=d: k_x[d].start())
    cp_z.wait()
    for k in range(TILE):
        ues[k // MG, k % MG, :] = z[MG + k, pl.ds(es, 1), :][0]
    u_y = remote(ues, uer, ie_s.at[5], ie_r.at[5], ydev)
    u_y.start()
    for d in SIDES:
        on_side(d, lambda d=d: u_x[d].start())
    cp_r.wait()
    for i in range(4):
        load_s(i).start()
    load_r(3 * first).start()
    load_r(3 - 3 * first).start()
    for i in (1, 2):
        load_r(i).start()
    cp_u.start()

    def both(v):
        return jnp.concatenate([v, v], axis=1)

    def update(a0, rows, c0, n, om, add_u):
        def body(i, carry):
            a = a0 + i
            wide = z[a, pl.ds(c0 - MG, n + STRIP), :]
            fy = both(wy[a - MG, pl.ds(c0 - MG, n + STRIP), :]) * (wide - pltpu.roll(wide, 1, 0))
            fyr = pltpu.roll(fy, n + 15, 0)
            mid = wide[MG:MG + n]
            az = (both(wx[a - MG, pl.ds(c0, n), :]) * (mid - z[a - 1, pl.ds(c0, n), :])
                  + both(wx[a - 7, pl.ds(c0, n), :]) * (mid - z[a + 1, pl.ds(c0, n), :])
                  + fy[MG:MG + n] - fyr[MG:MG + n])
            r[a, pl.ds(c0, n), :] = r[a, pl.ds(c0, n), :] - om * az
            if add_u:
                u[a - MG, pl.ds(c0 - MG, n), :] = u[a - MG, pl.ds(c0 - MG, n), :] + om * mid
            return carry
        lax.fori_loop(0, rows, body, 0)

    lo, hi = MG * EXT, END * EXT

    def pack_late(lhs, dst, row0, rows):
        for g in range(3):
            cols = lhs[:, lo + GROUP * g:lo + GROUP * (g + 1)]
            dst[pl.ds(row0, rows), RHS * g:RHS * (g + 1)] = jnp.dot(
                cols, psel[...], preferred_element_type=F32).astype(BF16)

    def pack_matrix():
        k = lax.broadcasted_iota(jnp.int32, (GROUP, RHS), 0)
        n = lax.broadcasted_iota(jnp.int32, (GROUP, RHS), 1)
        hit = ((k >> 6) == (n >> 4)) & ((k & 63) == sc + (n & 15))
        psel[...] = jnp.where(hit, 1.0, 0.0).astype(BF16)

        def strip(i, c):
            load_s(i).wait()
            pack_late(ms[pl.ds(STRIP * i, STRIP)].reshape(RHS, WIN), msl, pl.multiple_of(RHS * i, RHS), RHS)
            return c
        lax.fori_loop(0, 4, strip, 0)

    def early_s():
        w[MG:END, pl.ds(sc, STRIP), :] = jnp.zeros((TILE, STRIP, RHS), BF16)

        def strip(i, c):
            lhs = ms[pl.ds(STRIP * i, STRIP)].reshape(RHS, WIN)[:, lo:hi]
            z[pl.ds(STRIP * i, STRIP), pl.ds(sc, STRIP), :] = jnp.dot(
                lhs, w[MG:END].reshape(hi - lo, RHS), preferred_element_type=F32).reshape(STRIP, STRIP, RHS)
            return c
        lax.fori_loop(0, 4, strip, 0)

    def late(lhs, packed):
        cells = jnp.concatenate([w[0:MG].reshape(lo, RHS), w[END:EXT].reshape(lo, RHS),
                                 wl[...].reshape(LATE, RHS)], axis=0)
        return jnp.dot(jnp.concatenate([lhs[:, 0:lo], lhs[:, hi:WIN], packed], axis=1), cells,
                       preferred_element_type=F32)

    def dot_s(a0):
        part = late(ms[pl.ds(a0, STRIP)].reshape(RHS, WIN), msl[pl.ds(pl.multiple_of(a0 * STRIP, RHS), RHS), :])
        here = (pl.ds(a0, STRIP), pl.ds(sc, STRIP))
        z[here] = z[here] + part.reshape(STRIP, STRIP, RHS)

    def dot_r(a0):
        lhs = mr[pl.ds(a0, STRIP)].reshape(END_ROWS, WIN)
        z[pl.ds(a0, STRIP), pl.ds(gc, REST), :] = jnp.dot(
            lhs, w[...].reshape(WIN, RHS), preferred_element_type=F32).reshape(STRIP, REST, RHS)

    def ry(p0, n, j):
        return remote(rsy.at[pl.ds(p0, n)], rry.at[pl.ds(p0, n)], ry_s.at[j], ry_r.at[j], ydev)

    def ry_mid():
        return ry(*RMID, 2)

    def ry_early():
        return ry(*REARLY, 3)

    def ry_side(d):
        return ry(17 * d, 7, d)

    def rx(d):
        return remote(rsx.at[d], rrx.at[1 - d], rx_s.at[d], rx_r.at[1 - d], xdev(d))

    def rx_in(d):
        return remote(rsx.at[d], rrx.at[d], rx_s.at[d], rx_r.at[d], xdev(d))

    def rd(d):
        return remote(rsy.at[pl.ds(20 * d, 4)], rrd.at[1 - d], rd_s.at[d], rd_r.at[1 - d], ddev(d))

    def rd_forward(d):
        return remote(rry.at[pl.ds(20 * d, 4)], rrd.at[1 - d], rd_s.at[d], rd_r.at[1 - d], xdev(d))

    def same_chip(d):
        return lax.rem(row + d, 2) == 1

    def rd_in(d):
        return remote(rsy.at[pl.ds(20 * d, 4)], rrd.at[d], rd_s.at[d], rd_r.at[d], ddev(d))

    def pack_ry(p0, n):
        for q in range(n):
            a = MG + 2 * (p0 + q)
            rsy[p0 + q] = jnp.concatenate([r[a, pl.ds(mc, MG), :], r[a + 1, pl.ds(mc, MG), :]], axis=0).astype(BF16)

    def send_ry_side(d):
        pack_ry(17 * d, 7)
        on_side(d, lambda: pl.when(jnp.logical_not(same_chip(d)))(lambda: rd(d).start()))
        ry_side(d).start()

    def send_ry_mid():
        pack_ry(*RMID)
        ry_mid().start()

    def send_ry_early():
        pack_ry(*REARLY)
        ry_early().start()

    def send_rx(d):
        for i in range(MG):
            rsx[d, i] = r[MG + REST * d + i, MG:END, :].astype(BF16)
        on_side(d, lambda: rx(d).start())

    def to_w(a0, rows, c0, n):
        def body(i, carry):
            w[a0 + i, pl.ds(c0, n), :] = r[a0 + i, pl.ds(c0, n), :].astype(BF16)
            return carry
        lax.fori_loop(0, rows, body, 0)

    def to_strip(a):
        cells = r[a, pl.ds(sc, STRIP), :].astype(BF16)
        w[a, pl.ds(sc, STRIP), :] = cells
        wl[a - MG] = cells

    def unpack_ry(p0, n):
        def body(i, carry):
            v = rry[p0 + i].astype(F32)
            a = MG + 2 * (p0 + i)
            r[a, pl.ds(hc, MG), :] = v[0:MG]
            r[a + 1, pl.ds(hc, MG), :] = v[MG:STRIP]
            to_strip(a)
            to_strip(a + 1)
            return carry
        lax.fori_loop(0, n, body, 0)

    def recv_side(d):
        rx_in(d).wait_recv()
        rd_in(d).wait_recv()
        for i in range(MG):
            r[END * d + i, MG:END, :] = rrx[d, i].astype(F32)
        for q in range(4):
            v = rrd[d, q].astype(F32)
            r[END * d + 2 * q, pl.ds(hc, MG), :] = v[0:MG]
            r[END * d + 2 * q + 1, pl.ds(hc, MG), :] = v[MG:STRIP]
        to_w(END * d, MG, 0, EXT)

    def recv_r():
        to_w(MG, TILE, rc, TILE)
        early_s()
        ry_early().wait_recv()
        unpack_ry(*REARLY)
        for d in (order[1], order[0]):
            ry_side(d).wait_recv()
            on_side(d, lambda d=d: pl.when(same_chip(d))(lambda: rd_forward(d).start()))
            unpack_ry(17 * d, 7)
        for d in (order[1], order[0]):
            on_side(d, lambda d=d: recv_side(d))
        ry_mid().wait_recv()
        unpack_ry(*RMID)
        ry_mid().wait_send()
        ry_early().wait_send()
        for d in SIDES:
            ry_side(d).wait_send()

            def sent(d=d):
                rx(d).wait_send()
                rd(d).wait_send()
            on_side(d, sent)

    update(9, 46, cd, STRIP, 1.0, False)
    pack_ry(1, 22)
    ry(1, 22, 2).start()
    update(9, 46, ci, 32, 1.0, False)
    for d in SIDES:
        def edge(d=d):
            k_in[d].wait_recv()
            kfull[7 + 49 * d:MG + 49 * d, MG:END] = krecv[d, 47 - 47 * d:TILE - 47 * d, :]
            u_in[d].wait_recv()
        on_side(d, edge)
    kt = kfull[...].T
    for d in SIDES:
        a = MG + TILE * d
        wx[TILE * d] = 0.5 * (jnp.broadcast_to(kt[0:EXT, a - 1:a], (EXT, LANES))
                              + jnp.broadcast_to(kt[0:EXT, a:a + 1], (EXT, LANES)))
    for d in SIDES:
        update(MG + 47 * d, 1, cd, STRIP, 1.0, False)
        pack_ry(23 * d, 1)
        ry(23 * d, 1, d).start()
    for k in range(TILE):
        pcs[k // MG, k % MG, :] = r[MG + k, pl.ds(es, 1), :][0]
    p_y = remote(pcs, pcr, ie_s.at[6], ie_r.at[6], ydev)
    p_y.start()
    for d in SIDES:
        update(MG + 47 * d, 1, ci, 32, 1.0, False)
    k_y.wait_recv()
    u_y.wait_recv()

    def lane(ref, i):
        return jnp.broadcast_to(ref[:, i:i + 1], (TILE, LANES))

    k_nb = krecv[2]
    k_me = kown[...]
    wf = 0.5 * (jnp.where(col == 0, lane(k_me, 47), lane(k_me, 0))
                + jnp.where(col == 0, lane(k_nb, 0), lane(k_nb, 47)))
    flux = both(wf) * (ues[...].reshape(TILE, RHS) - uer[...].reshape(TILE, RHS))
    mine = pcs[...].reshape(TILE, RHS) - flux
    for k in range(TILE):
        wy[k, pl.ds(face, 1), :] = wf[k:k + 1]
        r[MG + k, pl.ds(es, 1), :] = mine[k:k + 1]

    def corner(d):
        return remote(rdb.at[d], rrd.at[1 - d], rd_s.at[d], rd_r.at[1 - d], ddev(d))

    for d in SIDES:
        for q in range(4):
            a = MG + REST * d + 2 * q
            rdb[d, q] = jnp.concatenate([r[a, pl.ds(mc, MG), :], r[a + 1, pl.ds(mc, MG), :]], axis=0).astype(BF16)
        on_side(d, lambda d=d: corner(d).start())
        send_rx(d)
        off_side(d, lambda d=d: to_w(END * d, MG, 0, EXT))
    to_w(MG, TILE, rc, TILE)
    pack_matrix()
    for d in SIDES:
        on_side(d, lambda d=d: u_x[d].wait_send())
    early_s()
    for d in SIDES:
        ry(23 * d, 1, d).wait_recv()
        unpack_ry(23 * d, 1)
    ry(1, 22, 2).wait_recv()
    unpack_ry(1, 22)
    p_y.wait_recv()
    theirs = pcr[...].reshape(TILE, RHS) + flux
    for k in range(TILE):
        r[MG + k, pl.ds(er, 1), :] = theirs[k:k + 1]

    def strip_row(i, c):
        to_strip(MG + i)
        return c
    lax.fori_loop(0, TILE, strip_row, 0)
    for d in (order[1], order[0]):
        on_side(d, lambda d=d: recv_side(d))
    ry(1, 22, 2).wait_send()
    for d in SIDES:
        ry(23 * d, 1, d).wait_send()

        def sent(d=d):
            k_x[d].wait_send()
            rx(d).wait_send()
            corner(d).wait_send()
        on_side(d, sent)
    k_y.wait_send()
    u_y.wait_send()
    p_y.wait_send()

    om = omega[0]

    def yz(j, off, length):
        return remote(ys.at[pl.ds(off, length)], yr.at[pl.ds(off, length)], yz_s.at[j], yz_r.at[j], ydev)

    def yz_mid(j):
        return yz(j, CHUNKS[j][2], CHUNKS[j][1] + pl.cdiv(CHUNKS[j][1], MG))

    def yz_side(d):
        return yz(3 + d, SIDE_OFF + 10 * d, 10)

    def pack_y(a0, n, off, e0, ne):
        for k in range(n):
            ys[off + k] = z[a0 + k, pl.ds(hc, MG), :]
        for k in range(ne):
            ys[off + n + k // MG, k % MG, :] = z[e0 + k, pl.ds(es, 1), :][0]

    def add_y(a0, n, off, e0, ne):
        for k in range(n):
            z[a0 + k, pl.ds(mc, MG), :] = z[a0 + k, pl.ds(mc, MG), :] + yr[off + k]
        for k in range(ne):
            z[e0 + k, pl.ds(er, 1), :] = z[e0 + k, pl.ds(er, 1), :] + yr[off + n + k // MG, k % MG, :][None]

    def side_rows(d):
        return 7 + 41 * d, 9, SIDE_OFF + 10 * d, MG + REST * d, MG

    def send_y(j):
        pack_y(*CHUNKS[j], *CHUNKS[j][:2])
        yz_mid(j).start()

    def send_y_side(d):
        pack_y(*side_rows(d))
        yz_side(d).start()

    def recv_y(j):
        yz_mid(j).wait_recv()
        add_y(*CHUNKS[j], *CHUNKS[j][:2])

    def recv_y_side(d):
        yz_side(d).wait_recv()
        add_y(*side_rows(d))

    def xs(d):
        return remote(z.at[pl.ds(55 * d, 9), pl.ds(sc, STRIP)], xrs.at[1 - d], xs_s.at[d], xs_r.at[1 - d], xdev(d))

    def xs_in(d):
        return remote(z.at[pl.ds(55 * d, 9), pl.ds(sc, STRIP)], xrs.at[d], xs_s.at[d], xs_r.at[d], xdev(d))

    def xr(d):
        return remote(z.at[pl.ds(55 * d, 9), pl.ds(gc, REST)], xrr.at[1 - d], xr_s.at[d], xr_r.at[1 - d], xdev(d))

    def xr_in(d):
        return remote(z.at[pl.ds(55 * d, 9), pl.ds(gc, REST)], xrr.at[d], xr_s.at[d], xr_r.at[d], xdev(d))

    def fold_s(d):
        def side():
            xs(d).wait_send()
            xs_in(d).wait_recv()
            for k in range(9):
                a = 7 + 41 * d + k
                z[a, pl.ds(sc, STRIP), :] = z[a, pl.ds(sc, STRIP), :] + xrs[d, k]
        on_side(d, side)

    def fold_r(d):
        def side():
            xr(d).wait_send()
            xr_in(d).wait_recv()
            for k in range(9):
                a = 7 + 41 * d + k
                z[a, pl.ds(gc, REST), :] = z[a, pl.ds(gc, REST), :] + xrr[d, k]
        on_side(d, side)

    def no_row_s(d):
        z[7 + 49 * d, pl.ds(sc, STRIP), :] = jnp.zeros((STRIP, RHS), F32)

    def no_row_r(d):
        z[7 + 49 * d, pl.ds(gc, REST), :] = jnp.zeros((REST, RHS), F32)

    def sweep(s, carry):
        dot_s(STRIP)
        send_y(0)
        dot_s(32)
        send_y(1)

        def ends_s(i, c):
            d = jnp.where(i == 0, first, 1 - first)
            dot_s(TILE * d)
            on_side(d, lambda: xs(d).start())
            off_side(d, lambda: no_row_s(d))
            return c
        lax.fori_loop(0, 2, ends_s, 0)

        def ends_r(i, c):
            d = jnp.where(i == 0, first, 1 - first)
            pl.when(s == 0)(lambda: load_r(3 * d).wait())
            dot_r(TILE * d)
            on_side(d, lambda: xr(d).start())
            off_side(d, lambda: no_row_r(d))
            fold_s(1 - d)
            send_y_side(1 - d)
            return c
        lax.fori_loop(0, 2, ends_r, 0)
        send_y(2)

        def mid_r(i, c):
            pl.when(s == 0)(lambda: load_r(i).wait())
            dot_r(STRIP * i)
            return c
        lax.fori_loop(1, 3, mid_r, 0)
        pl.when(s == 0)(lambda: cp_u.wait())
        recv_y(0)
        update(22, MG, cd, STRIP, om, True)
        send_ry_early()
        recv_y(1)

        def ends_u(i, c):
            d = jnp.where(i == 0, 1 - first, first)
            fold_r(d)
            update(MG + 39 * d, 9, ci, 32, om, True)
            recv_y_side(d)
            update(MG + 34 * d, 14, cd, STRIP, om, True)
            send_ry_side(d)
            send_rx(d)
            return c
        lax.fori_loop(0, 2, ends_u, 0)
        update(17, 30, ci, 32, om, True)
        recv_y(2)
        update(30, 12, cd, STRIP, om, True)
        send_ry_mid()
        recv_r()
        for j in range(3):
            yz_mid(j).wait_send()
        for d in SIDES:
            yz_side(d).wait_send()
        return carry

    lax.fori_loop(0, SWEEPS - 1, sweep, 0)

    def fy(j, p0, n):
        return remote(fys.at[pl.ds(p0, n)], fyr_.at[pl.ds(p0, n)], fy_s.at[j], fy_r.at[j], ydev)

    def send_fy(j, p0, n):
        for q in range(n):
            a = MG + 2 * (p0 + q)
            fys[p0 + q] = jnp.concatenate([z[a, pl.ds(hc, MG), :], z[a + 1, pl.ds(hc, MG), :]], axis=0).astype(BF16)
        fy(j, p0, n).start()

    def fxsd(d):
        return remote(fxs.at[d], fxsr.at[1 - d], fx_s.at[d], fx_r.at[1 - d], xdev(d))

    def fxsd_in(d):
        return remote(fxs.at[d], fxsr.at[d], fx_s.at[d], fx_r.at[d], xdev(d))

    def fxrd(d):
        return remote(fxr.at[d], fxrr.at[1 - d], fx_s.at[2 + d], fx_r.at[3 - d], xdev(d))

    def fxrd_in(d):
        return remote(fxr.at[d], fxrr.at[d], fx_s.at[2 + d], fx_r.at[2 + d], xdev(d))

    def last_s(d):
        for i in range(MG):
            fxs[d, i] = z[END * d + i, pl.ds(sc, STRIP), :].astype(BF16)
        fxsd(d).start()

    def last_r(d):
        for i in range(4):
            a = END * d + 2 * i
            fxr[d, i] = jnp.concatenate([z[a, pl.ds(gc, REST), :], z[a + 1, pl.ds(gc, REST), :]], axis=0).astype(BF16)
        fxrd(d).start()

    def last_fold_s(d):
        fxsd_in(d).wait_recv()
        for i in range(MG):
            a = MG + REST * d + i
            z[a, pl.ds(sc, STRIP), :] = z[a, pl.ds(sc, STRIP), :] + fxsr[d, i].astype(F32)

    def last_fold_r(d):
        fxrd_in(d).wait_recv()
        for i in range(4):
            a = MG + REST * d + 2 * i
            v = fxrr[d, i].astype(F32)
            z[a, pl.ds(gc, REST), :] = z[a, pl.ds(gc, REST), :] + v[0:REST]
            z[a + 1, pl.ds(gc, REST), :] = z[a + 1, pl.ds(gc, REST), :] + v[REST:80]

    def last_y(j, p0, n):
        fy(j, p0, n).wait_recv()

        def body(i, c):
            v = fyr_[p0 + i].astype(F32)
            a = MG + 2 * (p0 + i)
            z[a, pl.ds(mc, MG), :] = z[a, pl.ds(mc, MG), :] + v[0:MG]
            z[a + 1, pl.ds(mc, MG), :] = z[a + 1, pl.ds(mc, MG), :] + v[MG:STRIP]
            return c
        lax.fori_loop(0, n, body, 0)

    def add_u(a0, rows):
        def body(i, c):
            u[a0 - MG + i] = u[a0 - MG + i] + om * z[a0 + i, MG:END, :]
            return c
        lax.fori_loop(0, rows, body, 0)

    for j in SIDES:
        dot_s(STRIP + STRIP * j)
        send_fy(j, *FCHUNKS[j])

    def last_ends_s(i, c):
        d = jnp.where(i == 0, first, 1 - first)
        dot_s(TILE * d)
        on_side(d, lambda: last_s(d))
        return c
    lax.fori_loop(0, 2, last_ends_s, 0)

    def last_ends_r(i, c):
        d = jnp.where(i == 0, first, 1 - first)
        dot_r(TILE * d)
        on_side(d, lambda: last_r(d))
        on_side(1 - d, lambda: last_fold_s(1 - d))
        send_fy(3 - d, 20 * (1 - d), 4)
        return c
    lax.fori_loop(0, 2, last_ends_r, 0)
    lax.fori_loop(1, 3, lambda i, c: (dot_r(STRIP * i), c)[1], 0)
    for j in SIDES:
        last_y(j, *FCHUNKS[j])
    add_u(STRIP, 32)
    for d in (order[1], order[0]):
        on_side(d, lambda d=d: last_fold_r(d))
        last_y(2 + d, 20 * d, 4)
        add_u(MG + REST * d, MG)
    for j in SIDES:
        fy(j, *FCHUNKS[j]).wait_send()
        fy(2 + j, 20 * j, 4).wait_send()

        def sent(j=j):
            fxsd(j).wait_send()
            fxrd(j).wait_send()
        on_side(j, sent)


def solution(mesh):
    def local_step(forcing, u_init, diffusivity, local_solve, relax_omega):
        any_spec = pl.BlockSpec(memory_space=pltpu.HBM)
        dma = pltpu.SemaphoreType.DMA
        return pl.pallas_call(
            kernel,
            out_shape=jax.ShapeDtypeStruct((TILE, TILE, RHS), F32),
            in_specs=[pl.BlockSpec(memory_space=pltpu.SMEM), any_spec, any_spec,
                      any_spec, any_spec],
            out_specs=pl.BlockSpec(memory_space=pltpu.VMEM),
            scratch_shapes=[
                pltpu.VMEM((EXT, STRIP, WIN), BF16),
                pltpu.VMEM((EXT, REST, WIN), BF16),
                pltpu.VMEM((EXT, EXT, RHS), BF16),
                pltpu.VMEM((EXT, EXT, RHS), F32),
                pltpu.VMEM((EXT, EXT, RHS), F32),
                pltpu.VMEM((49, EXT, LANES), F32),
                pltpu.VMEM((TILE, EXT, LANES), F32),
                pltpu.VMEM((TILE, TILE), F32),
                pltpu.VMEM((3, TILE, TILE), F32),
                pltpu.VMEM((LANES, LANES), F32),
                pltpu.VMEM((YLEN, MG, RHS), F32),
                pltpu.VMEM((YLEN, MG, RHS), F32),
                pltpu.VMEM((2, 9, STRIP, RHS), F32),
                pltpu.VMEM((2, 9, REST, RHS), F32),
                pltpu.VMEM((24, STRIP, RHS), BF16),
                pltpu.VMEM((24, STRIP, RHS), BF16),
                pltpu.VMEM((2, MG, TILE, RHS), BF16),
                pltpu.VMEM((2, MG, TILE, RHS), BF16),
                pltpu.VMEM((2, 4, STRIP, RHS), BF16),
                pltpu.VMEM((2, 4, STRIP, RHS), BF16),
                pltpu.VMEM((6, MG, RHS), F32),
                pltpu.VMEM((6, MG, RHS), F32),
                pltpu.VMEM((6, MG, RHS), F32),
                pltpu.VMEM((6, MG, RHS), F32),
                pltpu.VMEM((24, STRIP, RHS), BF16),
                pltpu.VMEM((24, STRIP, RHS), BF16),
                pltpu.VMEM((2, MG, STRIP, RHS), BF16),
                pltpu.VMEM((2, MG, STRIP, RHS), BF16),
                pltpu.VMEM((2, 4, 80, RHS), BF16),
                pltpu.VMEM((2, 4, 80, RHS), BF16),
                pltpu.VMEM((GROUP, LATE), BF16),
                pltpu.VMEM((TILE, STRIP, RHS), BF16),
                pltpu.VMEM((GROUP, RHS), BF16),
                dma((5,)), dma((5,)), dma((2,)), dma((2,)), dma((2,)), dma((2,)),
                dma((4,)), dma((4,)), dma((2,)), dma((2,)), dma((2,)), dma((2,)),
                dma((7,)), dma((7,)), dma((4,)), dma((4,)), dma((4,)), dma((4,)), dma((4,)), dma((MG,)),
            ],
            compiler_params=pltpu.CompilerParams(
                collective_id=0, has_side_effects=True, vmem_limit_bytes=53_000_000),
            name="schwarz",
        )(relax_omega.reshape(1), forcing, u_init,
          pltpu.with_memory_space_constraint(diffusivity, pltpu.HBM),
          local_solve.reshape(EXT, EXT, WIN))

    field_spec = P('row', 'col', None)
    return jax.shard_map(local_step, mesh=mesh,
                         in_specs=(field_spec, field_spec, P('row', 'col'), P('row', 'col', None, None), P()),
                         out_specs=field_spec, check_vma=False)
```

```python
import functools

import jax
import jax.numpy as jnp
from jax import lax
from jax.experimental import pallas as pl
from jax.experimental.pallas import tpu as pltpu
from jax.sharding import PartitionSpec as P

SWEEPS = 4
TILE = 48
EXT = 64
WIN = EXT * EXT
RHS = 256
MG = 8
STRIP = 16
REST = 40
END = 56
END_ROWS = 640
LATE = 768
LANES = 128
GROUP = 1024
SIDES = (0, 1)
F32 = jnp.float32
BF16 = jnp.bfloat16
MESH = pl.DeviceIdType.MESH

CHUNKS = ((16, 16, 0), (40, 8, 18), (32, 8, 27))
SIDE_OFF = 36
YLEN = 56
RMID = (11, 6)
REARLY = (7, 4)
FCHUNKS = ((4, MG), (12, MG))

def kernel(omega, f_hbm, u_hbm, kap_hbm, m_hbm, u,
           ms, mr, w, z, r, wx, wy, kown, krecv, kfull,
           ys, yr, xrs, xrr, rsy, rry, rsx, rrx, rrd, rdb, ues, uer, pcs, pcr,
           fys, fyr_, fxs, fxsr, fxr, fxrr, msl, wl, psel,
           yz_s, yz_r, xs_s, xs_r, xr_s, xr_r, ry_s, ry_r, rx_s, rx_r, rd_s, rd_r,
           ie_s, ie_r, fy_s, fy_r, fx_s, fx_r, lsem, msem):
    col = lax.axis_index("col")
    row = lax.axis_index("row")
    has_up = row > 0
    has_dn = row < 3
    ydev = (1 - col, row)
    has = (has_up, has_dn)
    first = jnp.where(row < 2, 1, 0)
    order = (first, 1 - first)

    def xdev(d):
        return (col, row - 1 + 2 * d)

    def ddev(d):
        return (1 - col, row - 1 + 2 * d)

    def on_side(d, fn):
        there = jnp.where(d == 0, row, 3 - row) > 0
        pl.when(there)(fn)

    def off_side(d, fn):
        there = jnp.where(d == 0, row, 3 - row) > 0
        pl.when(jnp.logical_not(there))(fn)

    hc = pl.multiple_of(END - END * col, MG)
    mc = pl.multiple_of(TILE - REST * col, MG)
    oc = pl.multiple_of(END * col, MG)
    sc = pl.multiple_of(TILE - TILE * col, STRIP)
    rc = pl.multiple_of(STRIP * col, STRIP)
    gc = pl.multiple_of(MG + MG * col, MG)
    cd = pl.multiple_of(REST - 32 * col, MG)
    ci = pl.multiple_of(MG + STRIP * col, MG)
    es = 55 - 47 * col
    er = END - 49 * col
    face = END - TILE * col

    def remote(src, dst, ss, rs, dev):
        return pltpu.make_async_remote_copy(src_ref=src, dst_ref=dst, send_sem=ss, recv_sem=rs,
                                            device_id=dev, device_id_type=MESH)

    inner = (pl.ds(MG, TILE), pl.ds(MG, TILE))
    cp_z = pltpu.make_async_copy(u_hbm, z.at[inner], lsem.at[1])
    cp_r = pltpu.make_async_copy(f_hbm, r.at[inner], lsem.at[2])
    cp_u = pltpu.make_async_copy(u_hbm, u, lsem.at[3])
    cp_k = pltpu.make_async_copy(kap_hbm, kown, lsem.at[0])
    for cp in (cp_k, cp_z, cp_r):
        cp.start()

    def load_s(i):
        return pltpu.make_async_copy(m_hbm.at[pl.ds(STRIP * i, STRIP), pl.ds(sc, STRIP)], ms.at[pl.ds(STRIP * i, STRIP)], msem.at[i])

    def load_r(i):
        return pltpu.make_async_copy(m_hbm.at[pl.ds(STRIP * i, STRIP), pl.ds(gc, REST)], mr.at[pl.ds(STRIP * i, STRIP)], msem.at[4 + i])

    for a in (7, END):
        z[a] = jnp.zeros((EXT, RHS), F32)
    bar = pltpu.get_barrier_semaphore()
    pl.semaphore_signal(bar, inc=1, device_id=ydev, device_id_type=MESH)
    for d in SIDES:
        def greet(d=d):
            pl.semaphore_signal(bar, inc=1, device_id=xdev(d), device_id_type=MESH)
            pl.semaphore_signal(bar, inc=1, device_id=ddev(d), device_id_type=MESH)
        on_side(d, greet)
    r[7] = jnp.zeros((EXT, RHS), F32)
    r[END] = jnp.zeros((EXT, RHS), F32)
    for ref in (z, r):
        ref[0:7] = jnp.zeros((7, EXT, RHS), F32)
        ref[57:EXT] = jnp.zeros((7, EXT, RHS), F32)
        ref[MG:END, 0:MG] = jnp.zeros((TILE, MG, RHS), F32)
        ref[MG:END, END:EXT] = jnp.zeros((TILE, MG, RHS), F32)

    kfull[...] = jnp.zeros_like(kfull)
    cp_k.wait()
    kfull[MG:END, MG:END] = kown[...]
    kt = kfull[...].T
    prev = jnp.broadcast_to(kt[0:EXT, 7:MG], (EXT, LANES))
    for a in range(MG, 57):
        here = jnp.broadcast_to(kt[0:EXT, a:a + 1], (EXT, LANES))
        wx[a - MG] = 0.5 * (prev + here)
        if a < END:
            wy[a - MG] = 0.5 * (pltpu.roll(here, 1, 0) + here)
        prev = here
    for k in range(TILE):
        wy[k, pl.ds(face, 1), :] = jnp.zeros((1, LANES), F32)
    n_sides = has_up.astype(jnp.int32) + has_dn.astype(jnp.int32)
    pl.semaphore_wait(bar, 1 + 2 * n_sides)

    k_y = remote(kown, krecv.at[2], ie_s.at[0], ie_r.at[0], ydev)
    k_y.start()
    k_x = [remote(kown, krecv.at[1 - d], ie_s.at[1 + d], ie_r.at[2 - d], xdev(d)) for d in SIDES]
    u_x = [remote(z.at[MG if d == 0 else 55, pl.ds(MG, TILE)], z.at[END if d == 0 else 7, pl.ds(MG, TILE)],
                  ie_s.at[3 + d], ie_r.at[4 - d], xdev(d)) for d in SIDES]
    k_in = [remote(kown, krecv.at[d], ie_s.at[1 + d], ie_r.at[1 + d], xdev(d)) for d in SIDES]
    u_in = [remote(z.at[MG if d == 0 else 55, pl.ds(MG, TILE)], z.at[7 if d == 0 else END, pl.ds(MG, TILE)],
                   ie_s.at[3 + d], ie_r.at[3 + d], xdev(d)) for d in SIDES]
    for d in SIDES:
        on_side(d, lambda d=d: k_x[d].start())
    cp_z.wait()
    for k in range(TILE):
        ues[k // MG, k % MG, :] = z[MG + k, pl.ds(es, 1), :][0]
    u_y = remote(ues, uer, ie_s.at[5], ie_r.at[5], ydev)
    u_y.start()
    for d in SIDES:
        on_side(d, lambda d=d: u_x[d].start())
    cp_r.wait()
    for i in range(4):
        load_s(i).start()
    load_r(3 * first).start()
    load_r(3 - 3 * first).start()
    for i in (1, 2):
        load_r(i).start()
    cp_u.start()

    def both(v):
        return jnp.concatenate([v, v], axis=1)

    def update(a0, rows, c0, n, om, add_u):
        def body(i, carry):
            a = a0 + i
            wide = z[a, pl.ds(c0 - MG, n + STRIP), :]
            fy = both(wy[a - MG, pl.ds(c0 - MG, n + STRIP), :]) * (wide - pltpu.roll(wide, 1, 0))
            fyr = pltpu.roll(fy, n + 15, 0)
            mid = wide[MG:MG + n]
            az = (both(wx[a - MG, pl.ds(c0, n), :]) * (mid - z[a - 1, pl.ds(c0, n), :])
                  + both(wx[a - 7, pl.ds(c0, n), :]) * (mid - z[a + 1, pl.ds(c0, n), :])
                  + fy[MG:MG + n] - fyr[MG:MG + n])
            r[a, pl.ds(c0, n), :] = r[a, pl.ds(c0, n), :] - om * az
            if add_u:
                u[a - MG, pl.ds(c0 - MG, n), :] = u[a - MG, pl.ds(c0 - MG, n), :] + om * mid
            return carry
        lax.fori_loop(0, rows, body, 0)

    lo, hi = MG * EXT, END * EXT

    def pack_late(lhs, dst, row0, rows):
        for g in range(3):
            cols = lhs[:, lo + GROUP * g:lo + GROUP * (g + 1)]
            dst[pl.ds(row0, rows), RHS * g:RHS * (g + 1)] = jnp.dot(
                cols, psel[...], preferred_element_type=F32).astype(BF16)

    def pack_matrix():
        k = lax.broadcasted_iota(jnp.int32, (GROUP, RHS), 0)
        n = lax.broadcasted_iota(jnp.int32, (GROUP, RHS), 1)
        hit = ((k >> 6) == (n >> 4)) & ((k & 63) == sc + (n & 15))
        psel[...] = jnp.where(hit, 1.0, 0.0).astype(BF16)

        def strip(i, c):
            load_s(i).wait()
            pack_late(ms[pl.ds(STRIP * i, STRIP)].reshape(RHS, WIN), msl, pl.multiple_of(RHS * i, RHS), RHS)
            return c
        lax.fori_loop(0, 4, strip, 0)

    def early_s():
        w[MG:END, pl.ds(sc, STRIP), :] = jnp.zeros((TILE, STRIP, RHS), BF16)

        def strip(i, c):
            lhs = ms[pl.ds(STRIP * i, STRIP)].reshape(RHS, WIN)[:, lo:hi]
            z[pl.ds(STRIP * i, STRIP), pl.ds(sc, STRIP), :] = jnp.dot(
                lhs, w[MG:END].reshape(hi - lo, RHS), preferred_element_type=F32).reshape(STRIP, STRIP, RHS)
            return c
        lax.fori_loop(0, 4, strip, 0)

    def late(lhs, packed):
        cells = jnp.concatenate([w[0:MG].reshape(lo, RHS), w[END:EXT].reshape(lo, RHS),
                                 wl[...].reshape(LATE, RHS)], axis=0)
        return jnp.dot(jnp.concatenate([lhs[:, 0:lo], lhs[:, hi:WIN], packed], axis=1), cells,
                       preferred_element_type=F32)

    def dot_s(a0):
        part = late(ms[pl.ds(a0, STRIP)].reshape(RHS, WIN), msl[pl.ds(pl.multiple_of(a0 * STRIP, RHS), RHS), :])
        here = (pl.ds(a0, STRIP), pl.ds(sc, STRIP))
        z[here] = z[here] + part.reshape(STRIP, STRIP, RHS)

    def dot_r(a0):
        lhs = mr[pl.ds(a0, STRIP)].reshape(END_ROWS, WIN)
        z[pl.ds(a0, STRIP), pl.ds(gc, REST), :] = jnp.dot(
            lhs, w[...].reshape(WIN, RHS), preferred_element_type=F32).reshape(STRIP, REST, RHS)

    def ry(p0, n, j):
        return remote(rsy.at[pl.ds(p0, n)], rry.at[pl.ds(p0, n)], ry_s.at[j], ry_r.at[j], ydev)

    def ry_mid():
        return ry(*RMID, 2)

    def ry_early():
        return ry(*REARLY, 3)

    def ry_side(d):
        return ry(17 * d, 7, d)

    def rx(d):
        return remote(rsx.at[d], rrx.at[1 - d], rx_s.at[d], rx_r.at[1 - d], xdev(d))

    def rx_in(d):
        return remote(rsx.at[d], rrx.at[d], rx_s.at[d], rx_r.at[d], xdev(d))

    def rd(d):
        return remote(rsy.at[pl.ds(20 * d, 4)], rrd.at[1 - d], rd_s.at[d], rd_r.at[1 - d], ddev(d))

    def rd_forward(d):
        return remote(rry.at[pl.ds(20 * d, 4)], rrd.at[1 - d], rd_s.at[d], rd_r.at[1 - d], xdev(d))

    def same_chip(d):
        return lax.rem(row + d, 2) == 1

    def rd_in(d):
        return remote(rsy.at[pl.ds(20 * d, 4)], rrd.at[d], rd_s.at[d], rd_r.at[d], ddev(d))

    def pack_ry(p0, n):
        for q in range(n):
            a = MG + 2 * (p0 + q)
            rsy[p0 + q] = jnp.concatenate([r[a, pl.ds(mc, MG), :], r[a + 1, pl.ds(mc, MG), :]], axis=0).astype(BF16)

    def send_ry_side(d):
        pack_ry(17 * d, 7)
        on_side(d, lambda: pl.when(jnp.logical_not(same_chip(d)))(lambda: rd(d).start()))
        ry_side(d).start()

    def send_ry_mid():
        pack_ry(*RMID)
        ry_mid().start()

    def send_ry_early():
        pack_ry(*REARLY)
        ry_early().start()

    def send_rx(d):
        for i in range(MG):
            rsx[d, i] = r[MG + REST * d + i, MG:END, :].astype(BF16)
        on_side(d, lambda: rx(d).start())

    def to_w(a0, rows, c0, n):
        def body(i, carry):
            w[a0 + i, pl.ds(c0, n), :] = r[a0 + i, pl.ds(c0, n), :].astype(BF16)
            return carry
        lax.fori_loop(0, rows, body, 0)

    def to_strip(a):
        cells = r[a, pl.ds(sc, STRIP), :].astype(BF16)
        w[a, pl.ds(sc, STRIP), :] = cells
        wl[a - MG] = cells

    def unpack_ry(p0, n):
        def body(i, carry):
            v = rry[p0 + i].astype(F32)
            a = MG + 2 * (p0 + i)
            r[a, pl.ds(hc, MG), :] = v[0:MG]
            r[a + 1, pl.ds(hc, MG), :] = v[MG:STRIP]
            to_strip(a)
            to_strip(a + 1)
            return carry
        lax.fori_loop(0, n, body, 0)

    def recv_side(d):
        rx_in(d).wait_recv()
        rd_in(d).wait_recv()
        for i in range(MG):
            r[END * d + i, MG:END, :] = rrx[d, i].astype(F32)
        for q in range(4):
            v = rrd[d, q].astype(F32)
            r[END * d + 2 * q, pl.ds(hc, MG), :] = v[0:MG]
            r[END * d + 2 * q + 1, pl.ds(hc, MG), :] = v[MG:STRIP]
        to_w(END * d, MG, 0, EXT)

    def recv_r():
        to_w(MG, TILE, rc, TILE)
        early_s()
        ry_early().wait_recv()
        unpack_ry(*REARLY)
        for d in (order[1], order[0]):
            ry_side(d).wait_recv()
            on_side(d, lambda d=d: pl.when(same_chip(d))(lambda: rd_forward(d).start()))
            unpack_ry(17 * d, 7)
        for d in (order[1], order[0]):
            on_side(d, lambda d=d: recv_side(d))
        ry_mid().wait_recv()
        unpack_ry(*RMID)
        ry_mid().wait_send()
        ry_early().wait_send()
        for d in SIDES:
            ry_side(d).wait_send()

            def sent(d=d):
                rx(d).wait_send()
                rd(d).wait_send()
            on_side(d, sent)

    update(9, 46, cd, STRIP, 1.0, False)
    pack_ry(1, 22)
    ry(1, 22, 2).start()
    update(9, 46, ci, 32, 1.0, False)
    for d in SIDES:
        def edge(d=d):
            k_in[d].wait_recv()
            kfull[7 + 49 * d:MG + 49 * d, MG:END] = krecv[d, 47 - 47 * d:TILE - 47 * d, :]
            u_in[d].wait_recv()
        on_side(d, edge)
    kt = kfull[...].T
    for d in SIDES:
        a = MG + TILE * d
        wx[TILE * d] = 0.5 * (jnp.broadcast_to(kt[0:EXT, a - 1:a], (EXT, LANES))
                              + jnp.broadcast_to(kt[0:EXT, a:a + 1], (EXT, LANES)))
    for d in SIDES:
        update(MG + 47 * d, 1, cd, STRIP, 1.0, False)
        pack_ry(23 * d, 1)
        ry(23 * d, 1, d).start()
    for k in range(TILE):
        pcs[k // MG, k % MG, :] = r[MG + k, pl.ds(es, 1), :][0]
    p_y = remote(pcs, pcr, ie_s.at[6], ie_r.at[6], ydev)
    p_y.start()
    for d in SIDES:
        update(MG + 47 * d, 1, ci, 32, 1.0, False)
    k_y.wait_recv()
    u_y.wait_recv()

    def lane(ref, i):
        return jnp.broadcast_to(ref[:, i:i + 1], (TILE, LANES))

    k_nb = krecv[2]
    k_me = kown[...]
    wf = 0.5 * (jnp.where(col == 0, lane(k_me, 47), lane(k_me, 0))
                + jnp.where(col == 0, lane(k_nb, 0), lane(k_nb, 47)))
    flux = both(wf) * (ues[...].reshape(TILE, RHS) - uer[...].reshape(TILE, RHS))
    mine = pcs[...].reshape(TILE, RHS) - flux
    for k in range(TILE):
        wy[k, pl.ds(face, 1), :] = wf[k:k + 1]
        r[MG + k, pl.ds(es, 1), :] = mine[k:k + 1]

    def corner(d):
        return remote(rdb.at[d], rrd.at[1 - d], rd_s.at[d], rd_r.at[1 - d], ddev(d))

    for d in SIDES:
        for q in range(4):
            a = MG + REST * d + 2 * q
            rdb[d, q] = jnp.concatenate([r[a, pl.ds(mc, MG), :], r[a + 1, pl.ds(mc, MG), :]], axis=0).astype(BF16)
        on_side(d, lambda d=d: corner(d).start())
        send_rx(d)
        off_side(d, lambda d=d: to_w(END * d, MG, 0, EXT))
    to_w(MG, TILE, rc, TILE)
    pack_matrix()
    for d in SIDES:
        on_side(d, lambda d=d: u_x[d].wait_send())
    early_s()
    for d in SIDES:
        ry(23 * d, 1, d).wait_recv()
        unpack_ry(23 * d, 1)
    ry(1, 22, 2).wait_recv()
    unpack_ry(1, 22)
    p_y.wait_recv()
    theirs = pcr[...].reshape(TILE, RHS) + flux
    for k in range(TILE):
        r[MG + k, pl.ds(er, 1), :] = theirs[k:k + 1]

    def strip_row(i, c):
        to_strip(MG + i)
        return c
    lax.fori_loop(0, TILE, strip_row, 0)
    for d in (order[1], order[0]):
        on_side(d, lambda d=d: recv_side(d))
    ry(1, 22, 2).wait_send()
    for d in SIDES:
        ry(23 * d, 1, d).wait_send()

        def sent(d=d):
            k_x[d].wait_send()
            rx(d).wait_send()
            corner(d).wait_send()
        on_side(d, sent)
    k_y.wait_send()
    u_y.wait_send()
    p_y.wait_send()

    om = omega[0]

    def yz(j, off, length):
        return remote(ys.at[pl.ds(off, length)], yr.at[pl.ds(off, length)], yz_s.at[j], yz_r.at[j], ydev)

    def yz_mid(j):
        return yz(j, CHUNKS[j][2], CHUNKS[j][1] + pl.cdiv(CHUNKS[j][1], MG))

    def yz_side(d):
        return yz(3 + d, SIDE_OFF + 10 * d, 10)

    def pack_y(a0, n, off, e0, ne):
        for k in range(n):
            ys[off + k] = z[a0 + k, pl.ds(hc, MG), :]
        for k in range(ne):
            ys[off + n + k // MG, k % MG, :] = z[e0 + k, pl.ds(es, 1), :][0]

    def add_y(a0, n, off, e0, ne):
        for k in range(n):
            z[a0 + k, pl.ds(mc, MG), :] = z[a0 + k, pl.ds(mc, MG), :] + yr[off + k]
        for k in range(ne):
            z[e0 + k, pl.ds(er, 1), :] = z[e0 + k, pl.ds(er, 1), :] + yr[off + n + k // MG, k % MG, :][None]

    def side_rows(d):
        return 7 + 41 * d, 9, SIDE_OFF + 10 * d, MG + REST * d, MG

    def send_y(j):
        pack_y(*CHUNKS[j], *CHUNKS[j][:2])
        yz_mid(j).start()

    def send_y_side(d):
        pack_y(*side_rows(d))
        yz_side(d).start()

    def recv_y(j):
        yz_mid(j).wait_recv()
        add_y(*CHUNKS[j], *CHUNKS[j][:2])

    def recv_y_side(d):
        yz_side(d).wait_recv()
        add_y(*side_rows(d))

    def xs(d):
        return remote(z.at[pl.ds(55 * d, 9), pl.ds(sc, STRIP)], xrs.at[1 - d], xs_s.at[d], xs_r.at[1 - d], xdev(d))

    def xs_in(d):
        return remote(z.at[pl.ds(55 * d, 9), pl.ds(sc, STRIP)], xrs.at[d], xs_s.at[d], xs_r.at[d], xdev(d))

    def xr(d):
        return remote(z.at[pl.ds(55 * d, 9), pl.ds(gc, REST)], xrr.at[1 - d], xr_s.at[d], xr_r.at[1 - d], xdev(d))

    def xr_in(d):
        return remote(z.at[pl.ds(55 * d, 9), pl.ds(gc, REST)], xrr.at[d], xr_s.at[d], xr_r.at[d], xdev(d))

    def fold_s(d):
        def side():
            xs(d).wait_send()
            xs_in(d).wait_recv()
            for k in range(9):
                a = 7 + 41 * d + k
                z[a, pl.ds(sc, STRIP), :] = z[a, pl.ds(sc, STRIP), :] + xrs[d, k]
        on_side(d, side)

    def fold_r(d):
        def side():
            xr(d).wait_send()
            xr_in(d).wait_recv()
            for k in range(9):
                a = 7 + 41 * d + k
                z[a, pl.ds(gc, REST), :] = z[a, pl.ds(gc, REST), :] + xrr[d, k]
        on_side(d, side)

    def no_row_s(d):
        z[7 + 49 * d, pl.ds(sc, STRIP), :] = jnp.zeros((STRIP, RHS), F32)

    def no_row_r(d):
        z[7 + 49 * d, pl.ds(gc, REST), :] = jnp.zeros((REST, RHS), F32)

    def sweep(s, carry):
        dot_s(STRIP)
        send_y(0)
        dot_s(32)
        send_y(1)

        def ends_s(i, c):
            d = jnp.where(i == 0, first, 1 - first)
            dot_s(TILE * d)
            on_side(d, lambda: xs(d).start())
            off_side(d, lambda: no_row_s(d))
            return c
        lax.fori_loop(0, 2, ends_s, 0)

        def ends_r(i, c):
            d = jnp.where(i == 0, first, 1 - first)
            pl.when(s == 0)(lambda: load_r(3 * d).wait())
            dot_r(TILE * d)
            on_side(d, lambda: xr(d).start())
            off_side(d, lambda: no_row_r(d))
            fold_s(1 - d)
            send_y_side(1 - d)
            return c
        lax.fori_loop(0, 2, ends_r, 0)
        send_y(2)

        def mid_r(i, c):
            pl.when(s == 0)(lambda: load_r(i).wait())
            dot_r(STRIP * i)
            return c
        lax.fori_loop(1, 3, mid_r, 0)
        pl.when(s == 0)(lambda: cp_u.wait())
        recv_y(0)
        update(22, MG, cd, STRIP, om, True)
        send_ry_early()
        recv_y(1)

        def ends_u(i, c):
            d = jnp.where(i == 0, 1 - first, first)
            fold_r(d)
            update(MG + 39 * d, 9, ci, 32, om, True)
            recv_y_side(d)
            update(MG + 34 * d, 14, cd, STRIP, om, True)
            send_ry_side(d)
            send_rx(d)
            return c
        lax.fori_loop(0, 2, ends_u, 0)
        update(17, 30, ci, 32, om, True)
        recv_y(2)
        update(30, 12, cd, STRIP, om, True)
        send_ry_mid()
        recv_r()
        for j in range(3):
            yz_mid(j).wait_send()
        for d in SIDES:
            yz_side(d).wait_send()
        return carry

    lax.fori_loop(0, SWEEPS - 1, sweep, 0)

    def fy(j, p0, n):
        return remote(fys.at[pl.ds(p0, n)], fyr_.at[pl.ds(p0, n)], fy_s.at[j], fy_r.at[j], ydev)

    def send_fy(j, p0, n):
        for q in range(n):
            a = MG + 2 * (p0 + q)
            fys[p0 + q] = jnp.concatenate([z[a, pl.ds(hc, MG), :], z[a + 1, pl.ds(hc, MG), :]], axis=0).astype(BF16)
        fy(j, p0, n).start()

    def fxsd(d):
        return remote(fxs.at[d], fxsr.at[1 - d], fx_s.at[d], fx_r.at[1 - d], xdev(d))

    def fxsd_in(d):
        return remote(fxs.at[d], fxsr.at[d], fx_s.at[d], fx_r.at[d], xdev(d))

    def fxrd(d):
        return remote(fxr.at[d], fxrr.at[1 - d], fx_s.at[2 + d], fx_r.at[3 - d], xdev(d))

    def fxrd_in(d):
        return remote(fxr.at[d], fxrr.at[d], fx_s.at[2 + d], fx_r.at[2 + d], xdev(d))

    def last_s(d):
        for i in range(MG):
            fxs[d, i] = z[END * d + i, pl.ds(sc, STRIP), :].astype(BF16)
        fxsd(d).start()

    def last_r(d):
        for i in range(4):
            a = END * d + 2 * i
            fxr[d, i] = jnp.concatenate([z[a, pl.ds(gc, REST), :], z[a + 1, pl.ds(gc, REST), :]], axis=0).astype(BF16)
        fxrd(d).start()

    def last_fold_s(d):
        fxsd_in(d).wait_recv()
        for i in range(MG):
            a = MG + REST * d + i
            z[a, pl.ds(sc, STRIP), :] = z[a, pl.ds(sc, STRIP), :] + fxsr[d, i].astype(F32)

    def last_fold_r(d):
        fxrd_in(d).wait_recv()
        for i in range(4):
            a = MG + REST * d + 2 * i
            v = fxrr[d, i].astype(F32)
            z[a, pl.ds(gc, REST), :] = z[a, pl.ds(gc, REST), :] + v[0:REST]
            z[a + 1, pl.ds(gc, REST), :] = z[a + 1, pl.ds(gc, REST), :] + v[REST:80]

    def last_y(j, p0, n):
        fy(j, p0, n).wait_recv()

        def body(i, c):
            v = fyr_[p0 + i].astype(F32)
            a = MG + 2 * (p0 + i)
            z[a, pl.ds(mc, MG), :] = z[a, pl.ds(mc, MG), :] + v[0:MG]
            z[a + 1, pl.ds(mc, MG), :] = z[a + 1, pl.ds(mc, MG), :] + v[MG:STRIP]
            return c
        lax.fori_loop(0, n, body, 0)

    def add_u(a0, rows):
        def body(i, c):
            u[a0 - MG + i] = u[a0 - MG + i] + om * z[a0 + i, MG:END, :]
            return c
        lax.fori_loop(0, rows, body, 0)

    for j in SIDES:
        dot_s(STRIP + STRIP * j)
        send_fy(j, *FCHUNKS[j])

    def last_ends_s(i, c):
        d = jnp.where(i == 0, first, 1 - first)
        dot_s(TILE * d)
        on_side(d, lambda: last_s(d))
        return c
    lax.fori_loop(0, 2, last_ends_s, 0)

    def last_ends_r(i, c):
        d = jnp.where(i == 0, first, 1 - first)
        dot_r(TILE * d)
        on_side(d, lambda: last_r(d))
        on_side(1 - d, lambda: last_fold_s(1 - d))
        send_fy(3 - d, 20 * (1 - d), 4)
        return c
    lax.fori_loop(0, 2, last_ends_r, 0)
    def last_mid(i, c):
        part = jnp.dot(mr[pl.ds(STRIP * i, STRIP)].reshape(END_ROWS, WIN), w[...].reshape(WIN, RHS),
                       preferred_element_type=F32).reshape(STRIP, REST, RHS)
        here = (pl.ds(STRIP * i - MG, STRIP), pl.ds(gc - MG, REST))
        u[here] = u[here] + om * part
        return c
    lax.fori_loop(1, 3, last_mid, 0)
    for j in SIDES:
        last_y(j, *FCHUNKS[j])

    def add_strip(i, c):
        here = pl.ds(mc - MG, MG)
        u[MG + i, here, :] = u[MG + i, here, :] + om * z[STRIP + i, pl.ds(mc, MG), :]
        return c
    lax.fori_loop(0, 32, add_strip, 0)
    for d in (order[1], order[0]):
        on_side(d, lambda d=d: last_fold_r(d))
        last_y(2 + d, 20 * d, 4)
        add_u(MG + REST * d, MG)
    for j in SIDES:
        fy(j, *FCHUNKS[j]).wait_send()
        fy(2 + j, 20 * j, 4).wait_send()

        def sent(j=j):
            fxsd(j).wait_send()
            fxrd(j).wait_send()
        on_side(j, sent)


def solution(mesh):
    def local_step(forcing, u_init, diffusivity, local_solve, relax_omega):
        any_spec = pl.BlockSpec(memory_space=pltpu.HBM)
        dma = pltpu.SemaphoreType.DMA
        return pl.pallas_call(
            kernel,
            out_shape=jax.ShapeDtypeStruct((TILE, TILE, RHS), F32),
            in_specs=[pl.BlockSpec(memory_space=pltpu.SMEM), any_spec, any_spec,
                      any_spec, any_spec],
            out_specs=pl.BlockSpec(memory_space=pltpu.VMEM),
            scratch_shapes=[
                pltpu.VMEM((EXT, STRIP, WIN), BF16),
                pltpu.VMEM((EXT, REST, WIN), BF16),
                pltpu.VMEM((EXT, EXT, RHS), BF16),
                pltpu.VMEM((EXT, EXT, RHS), F32),
                pltpu.VMEM((EXT, EXT, RHS), F32),
                pltpu.VMEM((49, EXT, LANES), F32),
                pltpu.VMEM((TILE, EXT, LANES), F32),
                pltpu.VMEM((TILE, TILE), F32),
                pltpu.VMEM((3, TILE, TILE), F32),
                pltpu.VMEM((LANES, LANES), F32),
                pltpu.VMEM((YLEN, MG, RHS), F32),
                pltpu.VMEM((YLEN, MG, RHS), F32),
                pltpu.VMEM((2, 9, STRIP, RHS), F32),
                pltpu.VMEM((2, 9, REST, RHS), F32),
                pltpu.VMEM((24, STRIP, RHS), BF16),
                pltpu.VMEM((24, STRIP, RHS), BF16),
                pltpu.VMEM((2, MG, TILE, RHS), BF16),
                pltpu.VMEM((2, MG, TILE, RHS), BF16),
                pltpu.VMEM((2, 4, STRIP, RHS), BF16),
                pltpu.VMEM((2, 4, STRIP, RHS), BF16),
                pltpu.VMEM((6, MG, RHS), F32),
                pltpu.VMEM((6, MG, RHS), F32),
                pltpu.VMEM((6, MG, RHS), F32),
                pltpu.VMEM((6, MG, RHS), F32),
                pltpu.VMEM((24, STRIP, RHS), BF16),
                pltpu.VMEM((24, STRIP, RHS), BF16),
                pltpu.VMEM((2, MG, STRIP, RHS), BF16),
                pltpu.VMEM((2, MG, STRIP, RHS), BF16),
                pltpu.VMEM((2, 4, 80, RHS), BF16),
                pltpu.VMEM((2, 4, 80, RHS), BF16),
                pltpu.VMEM((GROUP, LATE), BF16),
                pltpu.VMEM((TILE, STRIP, RHS), BF16),
                pltpu.VMEM((GROUP, RHS), BF16),
                dma((5,)), dma((5,)), dma((2,)), dma((2,)), dma((2,)), dma((2,)),
                dma((4,)), dma((4,)), dma((2,)), dma((2,)), dma((2,)), dma((2,)),
                dma((7,)), dma((7,)), dma((4,)), dma((4,)), dma((4,)), dma((4,)), dma((4,)), dma((MG,)),
            ],
            compiler_params=pltpu.CompilerParams(
                collective_id=0, has_side_effects=True, vmem_limit_bytes=53_000_000),
            name="schwarz",
        )(relax_omega.reshape(1), forcing, u_init,
          pltpu.with_memory_space_constraint(diffusivity, pltpu.HBM),
          local_solve.reshape(EXT, EXT, WIN))

    field_spec = P('row', 'col', None)
    return jax.shard_map(local_step, mesh=mesh,
                         in_specs=(field_spec, field_spec, P('row', 'col'), P('row', 'col', None, None), P()),
                         out_specs=field_spec, check_vma=False)
```
